32 devices in a mesh: grp: 2 (over x), comp: 4 (over z), row: 4 (over y, core).
Axes of the slice: x: 2, y: 2, z: 4, core: 2. Of those that a mesh axis runs over, the one named last changes fastest.
Arguments:
- points: bfloat16 [8192, 512], P(('grp', 'row')), parts along dimension 0
- mu_init: float32 [2, 8192, 256], P(None, ('grp', 'comp')), parts along dimension 1
- logpi_init: float32 [2, 8192], P(None, ('grp', 'comp')), parts along dimension 1
- inv_temp: float32 [3], replicated
Outputs:
- output 1: float32 [2, 8192, 256], P(None, ('grp', 'comp')), parts along dimension 1
- output 2: float32 [2, 8192], P(None, ('grp', 'comp')), parts along dimension 1
- output 3: float32 [2, 8192], P(None, ('grp', 'row')), parts along dimension 1
There are 2 independent parts. The reference program is written for one: setup_inputs(seed, part) draws one part's arguments, and reference() takes and returns one part's arrays. A program takes and returns all parts, laid end to end along the dimension named above; an argument that names none is the same for every part.
All inputs are finite; a program needn't handle non-finite values.
Results may differ from the reference program's by a relative error of at most 0.00106792.
Values are sent between devices in bfloat16 or wider.
A program may use at most 1 GiB of HBM per device.

```python
import jax
import jax.numpy as jnp
from jax import lax

POINTS = 4096
DIM = 512
HALF = 256
COMPS = 4096
SWEEPS = 3
CLUSTERS = 16
BLOCK = 256

EPS_COUNT = 1e-6
PRIOR_ALPHA = 1e-3


def setup_inputs(seed: int = 0, part: int = 0) -> dict:
    base_key = jax.random.key(seed)
    part_key = jax.random.fold_in(base_key, part)
    key_c, key_x, key_j, key_m, key_w = jax.random.split(part_key, 5)
    key_b = jax.random.fold_in(base_key, 1000)
    centers = jax.random.normal(key_c, (2, CLUSTERS, HALF), jnp.float32)
    source = (jnp.arange(POINTS) * CLUSTERS) // POINTS
    noise_x = jax.random.normal(key_x, (2, POINTS, HALF), jnp.float32)
    pts_pair = centers[:, source, :] + 0.7 * noise_x
    points = jnp.transpose(pts_pair, (1, 0, 2)).reshape(POINTS, DIM).astype(jnp.bfloat16)
    pick_ids = jax.random.randint(key_j, (2, COMPS), 0, CLUSTERS)
    noise_m = jax.random.normal(key_m, (2, COMPS, HALF), jnp.float32)
    mu_init = centers[jnp.arange(2)[:, None], pick_ids] + 0.5 * noise_m
    raw_logit = jax.random.normal(key_w, (2, COMPS), jnp.float32)
    logpi_init = raw_logit - jax.nn.logsumexp(raw_logit, axis=1, keepdims=True)
    inv_temp = (0.5 + 1.5 * jax.random.uniform(key_b, (SWEEPS,), jnp.float32)) / HALF
    return {"points": points, "mu_init": mu_init, "logpi_init": logpi_init, "inv_temp": inv_temp}


def reference(points, mu_init, logpi_init, inv_temp):
    x_blocks = points.astype(jnp.float32).reshape(POINTS // BLOCK, BLOCK, 2, HALF)
    x_blocks = jnp.transpose(x_blocks, (0, 2, 1, 3))
    sq_blocks = jnp.sum(x_blocks * x_blocks, axis=3)

    def one_sweep(carry_in, beta_t):
        mean_vecs, log_wts = carry_in
        mu_round = mean_vecs.astype(jnp.bfloat16).astype(jnp.float32)
        mu_sq = jnp.sum(mean_vecs * mean_vecs, axis=2)

        def point_block(acc_pair, block_in):
            x_block, sq_norm = block_in
            cross_dot = jnp.einsum("snh,skh->snk", x_block, mu_round)
            logits = log_wts[:, None, :] - beta_t * (sq_norm[:, :, None] - 2.0 * cross_dot + mu_sq[:, None, :])
            row_max = jnp.max(logits, axis=2)
            shifted = jnp.exp(logits - row_max[:, :, None])
            row_sum = jnp.sum(shifted, axis=2)
            resp_f = shifted / row_sum[:, :, None]
            log_norm = row_max + jnp.log(row_sum)
            resp_round = resp_f.astype(jnp.bfloat16).astype(jnp.float32)
            stat_part = jnp.einsum("snk,snh->skh", resp_round, x_block)
            count_acc, stat_acc = acc_pair
            return (count_acc + jnp.sum(resp_f, axis=1), stat_acc + stat_part), log_norm

        zero_acc = (jnp.zeros((2, COMPS), jnp.float32), jnp.zeros((2, COMPS, HALF), jnp.float32))
        (counts, stat_sum), norm_blocks = lax.scan(point_block, zero_acc, (x_blocks, sq_blocks))
        new_means = stat_sum / (counts[:, :, None] + EPS_COUNT)
        new_logw = jnp.log((counts + PRIOR_ALPHA) / (POINTS + COMPS * PRIOR_ALPHA))
        return (new_means, new_logw), norm_blocks

    (mean_vecs, log_wts), norm_all = lax.scan(one_sweep, (mu_init, logpi_init), inv_temp)
    log_norm = jnp.transpose(norm_all[-1], (1, 0, 2)).reshape(2, POINTS)
    return mean_vecs, log_wts, log_norm
```

```python
import functools

import jax
import jax.numpy as jnp
from jax import lax
from jax.experimental import pallas as pl
from jax.experimental.pallas import tpu as pltpu
from jax.sharding import PartitionSpec as P

EPS_COUNT = 1e-6
PRIOR_ALPHA = 1e-3
LOG2E = 1.4426950408889634
LN2 = 0.6931471805599453
MESH = pl.DeviceIdType.MESH

CORES = 2
TP = 256
NCH = 4


def lse2_parts(parts):
    top = functools.reduce(jnp.maximum, parts)
    total = functools.reduce(jnp.add, [jnp.exp2(p - top) for p in parts])
    return top + jnp.log(total) * LOG2E


def em_kernel(
    comp_size, row_size, sweeps,
    temp_ref, lp_ref, x_hbm, mu_hbm,
    mu_out, lp_out, lse_out,
    xg, mu_own, mub, bcol, e_buf, m_buf, l_buf, s_acc, n_acc, mu_fin, lp_fin, sq_buf,
    pre_buf, bc_src, bc_buf, tot_buf,
    load_sem, y_send, y_recv, z_send, z_recv, sy_send, sy_recv, sz_send, sz_recv, own_send, own_recv,
    pre_send, pre_recv, bc_send, bc_recv, post_send, post_recv,
    fin_send, fin_recv, lpf_send, lpf_recv,
):
    z = lax.axis_index("comp")
    r = lax.axis_index("row")
    y, c = r // CORES, r % CORES
    n_chips = comp_size * row_size // CORES
    y_size = row_size // CORES
    chip = z * y_size + y
    block = x_hbm.shape[0]
    half_dim = x_hbm.shape[1] // 2
    total_pts = block * row_size
    n_own = mub.shape[1]
    total_comp = mu_hbm.shape[1] * comp_size
    tiles = total_pts // TP
    half_tiles = tiles // 2
    half = block // 2
    ch = half // NCH
    sib = {"row": y * CORES + (1 - c)}
    yn = {"row": (1 - y) * CORES + c}
    zpart = z + 1 - 2 * (z % 2)
    zn = {"comp": zpart}

    loads = []
    for s in range(2):
        loads.append(pltpu.make_async_copy(
            x_hbm.at[:, pl.ds(s * half_dim, half_dim)],
            xg.at[s, pl.ds(r * block, block), :], load_sem.at[s]))
        loads.append(pltpu.make_async_copy(
            mu_hbm.at[s, pl.ds(r * n_own, n_own), :], mu_own.at[s], load_sem.at[2 + s]))
    for cp in loads:
        cp.start()

    barrier = pltpu.get_barrier_semaphore()
    pl.semaphore_signal(barrier, inc=1, device_id=sib, device_id_type=MESH)
    for k in range(1, n_chips):
        q = lax.rem(chip + k, n_chips)
        pl.semaphore_signal(
            barrier, inc=1, device_id={"comp": q // y_size, "row": (q % y_size) * CORES + c},
            device_id_type=MESH)
    pl.semaphore_wait(barrier, n_chips)

    def remote(src, dst, send, recv, dev):
        return pltpu.make_async_remote_copy(
            src_ref=src, dst_ref=dst, send_sem=send, recv_sem=recv, device_id=dev, device_id_type=MESH)

    hz = z % 2
    ry = (1 - y) * CORES + c

    def xrows(s, blk, hh, k):
        return xg.at[s, pl.ds(blk * block + hh * half + k * ch, ch), :]

    def y_out(s, k):
        v = xrows(s, r, hz, k)
        return remote(v, v, y_send.at[s, k], y_recv.at[s, k], yn)

    def z_fwd(s, k):
        v = xrows(s, ry, hz, k)
        return remote(v, v, z_send.at[s, k], z_recv.at[s, k], zn)

    def sy_fwd(s, k):
        v = xrows(s, ry, hz, k)
        return remote(v, v, sy_send.at[s, k], sy_recv.at[s, k], sib)

    def sz_fwd(s, k):
        v = xrows(s, ry, 1 - hz, k)
        return remote(v, v, sz_send.at[s, k], sz_recv.at[s, k], sib)

    def own_out(s):
        v = xg.at[s, pl.ds(r * block, block), :]
        return remote(v, v, own_send.at[s], own_recv.at[s], sib)

    for s in range(2):
        loads[2 * s].wait()
        for k in range(NCH):
            y_out(s, k).start()
        own_out(s).start()
    for s in range(2):
        loads[2 * s + 1].wait()

    def col_to_row(col):
        n = col.shape[0]
        eye = lax.broadcasted_iota(jnp.int32, (n, n), 0) == lax.broadcasted_iota(jnp.int32, (n, n), 1)
        return jnp.sum(jnp.where(eye, col, 0.0), axis=0, keepdims=True)

    def row_to_col(row):
        n = row.shape[1]
        eye = lax.broadcasted_iota(jnp.int32, (n, n), 0) == lax.broadcasted_iota(jnp.int32, (n, n), 1)
        return jnp.sum(jnp.where(eye, row, 0.0), axis=1, keepdims=True)

    def set_params(s, mean, logw, t):
        mub[s] = mean.astype(jnp.bfloat16)
        mu_sq = jnp.sum(mean * mean, axis=1, keepdims=True)
        bcol[s] = (logw - temp_ref[t] * mu_sq) * LOG2E

    for s in range(2):
        set_params(s, mu_own[s], row_to_col(lp_ref[s:s + 1, pl.ds(pl.multiple_of(r * n_own, n_own), n_own)]), 0)

    def e_step(s, t):
        scale = temp_ref[t] * (2.0 * LOG2E)
        unroll = 4

        def body(i, _):
            for u in range(unroll):
                tile = i * unroll + u
                x = xg[s, pl.ds(pl.multiple_of(tile * TP, TP), TP), :]
                a = lax.dot_general(mub[s], x, (((1,), (1,)), ((), ())), preferred_element_type=jnp.float32)
                l2 = a * scale + bcol[s]
                m = jnp.max(l2, axis=0, keepdims=True)
                e = jnp.exp2(l2 - m)
                e_buf[s, tile] = e
                rs = jnp.sum(e, axis=0, keepdims=True)
                hh, j = tile // half_tiles, tile % half_tiles
                m_buf[s, hh, pl.ds(j, 1), :] = m
                l_buf[s, hh, pl.ds(j, 1), :] = m + jnp.log(rs) * LOG2E
            return 0

        lax.fori_loop(0, tiles // unroll, body, 0)

    def m_step(s, t):
        idx = 2 * t + s
        unroll = 4
        s_acc[...] = jnp.zeros_like(s_acc)
        n_acc[...] = jnp.zeros_like(n_acc)

        def body(i, _):
            dots, ns = [], []
            for u in range(unroll):
                tile = i * unroll + u
                hh, j = tile // half_tiles, tile % half_tiles
                f = jnp.exp2(m_buf[s, hh, pl.ds(j, 1), :] - tot_buf[idx, hh, pl.ds(j, 1), :])
                resp = e_buf[s, tile] * f
                ns.append(resp[:, :128] + resp[:, 128:])
                x = xg[s, pl.ds(pl.multiple_of(tile * TP, TP), TP), :]
                dots.append(jnp.dot(resp.astype(jnp.bfloat16), x, preferred_element_type=jnp.float32))
            s_acc[...] += functools.reduce(jnp.add, dots)
            n_acc[...] += functools.reduce(jnp.add, ns)
            return 0

        lax.fori_loop(0, tiles // unroll, body, 0)
        cnt = jnp.sum(n_acc[...], axis=1, keepdims=True)
        mean = s_acc[...] / (cnt + EPS_COUNT)
        logw = jnp.log((cnt + PRIOR_ALPHA) / (total_pts + total_comp * PRIOR_ALPHA))
        return mean, logw

    def pre(idx):
        return remote(l_buf.at[idx % 2, 1 - c], pre_buf.at[idx], pre_send.at[idx], pre_recv.at[idx], sib)

    def bcast(idx, k):
        q = lax.rem(chip + k, n_chips)
        return remote(bc_src.at[idx], bc_buf.at[idx, k - 1], bc_send.at[idx, k - 1], bc_recv.at[idx, k - 1],
                      {"comp": q // y_size, "row": (q % y_size) * CORES + c})

    def post(idx):
        v = tot_buf.at[idx, c]
        return remote(v, v, post_send.at[idx], post_recv.at[idx], sib)

    def p2(idx):
        pre(idx).wait()
        bc_src[idx] = lse2_parts([l_buf[idx % 2, c], pre_buf[idx]])
        for k in range(1, n_chips):
            bcast(idx, k).start()

    def p3(idx):
        for k in range(1, n_chips):
            bcast(idx, k).wait()
        tot_buf[idx, c] = lse2_parts([bc_src[idx]] + [bc_buf[idx, k] for k in range(n_chips - 1)])
        post(idx).start()

    for s in range(2):
        own_out(s).wait()
        for k in range(NCH):
            y_out(s, k).wait()
            z_fwd(s, k).start()
            sy_fwd(s, k).start()
        for k in range(NCH):
            z_fwd(s, k).wait()
            sz_fwd(s, k).start()
        for k in range(NCH):
            sy_fwd(s, k).wait()
            sz_fwd(s, k).wait()
        e_step(s, 0)
        pre(s).start()

    ones = jnp.ones((8, half_dim), jnp.bfloat16)
    for s in range(2):
        for j in range(block // TP):
            x = xg[s, pl.ds(pl.multiple_of(r * block + j * TP, TP), TP), :].astype(jnp.float32)
            sq = x * x
            hi = sq.astype(jnp.bfloat16)
            lo = (sq - hi.astype(jnp.float32)).astype(jnp.bfloat16)
            d = functools.partial(lax.dot_general, dimension_numbers=(((1,), (1,)), ((), ())),
                                  preferred_element_type=jnp.float32)
            sq_buf[s, j:j + 1, :] = (d(ones, hi) + d(ones, lo))[0:1]

    def fin(s, d):
        v = mu_fin.at[r, s]
        return remote(v, v, fin_send.at[s, d], fin_recv.at[s, d], sib if d == 0 else yn)

    def fin_fwd(s):
        v = mu_fin.at[ry, s]
        return remote(v, v, fin_send.at[s, 2], fin_recv.at[s, 2], sib)

    def lpf(d):
        v = lp_fin.at[r]
        return remote(v, v, lpf_send.at[d], lpf_recv.at[d], sib if d == 0 else yn)

    def lpf_fwd():
        v = lp_fin.at[ry]
        return remote(v, v, lpf_send.at[2], lpf_recv.at[2], sib)

    p2(0)
    p2(1)
    for t in range(sweeps):
        last = t == sweeps - 1
        for s in range(2):
            idx = 2 * t + s
            p3(idx)
            post(idx).wait()
            mean, logw = m_step(s, t)
            if not last:
                set_params(s, mean, logw, t + 1)
                if s == 1:
                    p2(idx + 1)
                e_step(s, t + 1)
                pre(idx + 2).start()
                if s == 1:
                    p2(idx + 2)
            else:
                mu_fin[r, s] = mean
                lp_fin[r, s:s + 1, :] = col_to_row(logw)
                fin(s, 1).start()
                fin(s, 0).start()
    lpf(1).start()
    lpf(0).start()

    t = sweeps - 1
    blk_tiles = block // TP
    for s in range(2):
        for j in range(blk_tiles):
            tile = r * blk_tiles + j
            row = tot_buf[2 * t + s, tile // half_tiles, pl.ds(tile % half_tiles, 1), :]
            lse_out[s:s + 1, j * TP:(j + 1) * TP] = row * LN2 - temp_ref[t] * sq_buf[s, j:j + 1, :]

    for s in range(2):
        fin(s, 1).wait()
        fin_fwd(s).start()
    lpf(1).wait()
    lpf_fwd().start()
    for s in range(2):
        fin(s, 0).wait()
        fin_fwd(s).wait()
    lpf(0).wait()
    lpf_fwd().wait()
    outs = []
    for q in range(row_size):
        for s in range(2):
            cp = pltpu.make_async_copy(mu_fin.at[q, s], mu_out.at[s, pl.ds(q * n_own, n_own), :],
                                       load_sem.at[4 + 2 * q + s])
            cp.start()
            outs.append(cp)
            lp_out[s:s + 1, q * n_own:(q + 1) * n_own] = lp_fin[q, s:s + 1, :]
    for cp in outs:
        cp.wait()


def solution(mesh):
    comp_size = mesh.shape["comp"]
    row_size = mesh.shape["row"]

    def local_fit(x_local, mu_init, logpi_init, inv_temp):
        block, dim = x_local.shape
        half_dim = dim // 2
        n_local = mu_init.shape[1]
        n_own = n_local // row_size
        total_pts = block * row_size
        tiles = total_pts // TP
        sweeps = inv_temp.shape[0]
        n_chips = comp_size * row_size // CORES
        ni = 2 * sweeps
        ht = tiles // 2
        f32, bf16 = jnp.float32, jnp.bfloat16
        dma = pltpu.SemaphoreType.DMA
        vm = pltpu.VMEM
        scratch = [
            vm((2, total_pts, half_dim), bf16),
            vm((2, n_own, half_dim), f32),
            vm((2, n_own, half_dim), bf16),
            vm((2, n_own, 1), f32),
            vm((2, tiles, n_own, TP), f32),
            vm((2, 2, ht, TP), f32),
            vm((2, 2, ht, TP), f32),
            vm((n_own, half_dim), f32),
            vm((n_own, 128), f32),
            vm((row_size, 2, n_own, half_dim), f32),
            vm((row_size, 2, n_own), f32),
            vm((2, block // TP, TP), f32),
            vm((ni, ht, TP), f32),
            vm((ni, ht, TP), f32),
            vm((ni, n_chips - 1, ht, TP), f32),
            vm((ni, 2, ht, TP), f32),
            dma((4 + 2 * row_size,)),
            dma((2, NCH)), dma((2, NCH)), dma((2, NCH)), dma((2, NCH)),
            dma((2, NCH)), dma((2, NCH)), dma((2, NCH)), dma((2, NCH)),
            dma((2,)), dma((2,)),
            dma((ni,)), dma((ni,)), dma((ni, n_chips - 1)), dma((ni, n_chips - 1)), dma((ni,)), dma((ni,)),
            dma((2, 3)), dma((2, 3)), dma((3,)), dma((3,)),
        ]
        return pl.pallas_call(
            functools.partial(em_kernel, comp_size, row_size, sweeps),
            out_shape=(
                jax.ShapeDtypeStruct((2, n_local, half_dim), f32),
                jax.ShapeDtypeStruct((2, n_local), f32),
                jax.ShapeDtypeStruct((2, block), f32),
            ),
            in_specs=[
                pl.BlockSpec(memory_space=pltpu.SMEM),
                pl.BlockSpec(memory_space=pltpu.VMEM),
                pl.BlockSpec(memory_space=pl.ANY),
                pl.BlockSpec(memory_space=pl.ANY),
            ],
            out_specs=(
                pl.BlockSpec(memory_space=pl.ANY),
                pl.BlockSpec(memory_space=pltpu.VMEM),
                pl.BlockSpec(memory_space=pltpu.VMEM),
            ),
            scratch_shapes=scratch,
            compiler_params=pltpu.CompilerParams(
                collective_id=0, has_side_effects=True, vmem_limit_bytes=56 * 1024 * 1024),
        )(inv_temp, logpi_init, x_local, mu_init)

    return jax.shard_map(
        local_fit,
        mesh=mesh,
        in_specs=(P(("grp", "row"), None), P(None, ("grp", "comp"), None), P(None, ("grp", "comp")), P()),
        out_specs=(P(None, ("grp", "comp"), None), P(None, ("grp", "comp")), P(None, ("grp", "row"))),
        check_vma=False,
    )
```

```python
import functools

import jax
import jax.numpy as jnp
from jax import lax
from jax.experimental import pallas as pl
from jax.experimental.pallas import tpu as pltpu
from jax.sharding import PartitionSpec as P

EPS_COUNT = 1e-6
PRIOR_ALPHA = 1e-3
LOG2E = 1.4426950408889634
LN2 = 0.6931471805599453
MESH = pl.DeviceIdType.MESH

CORES = 2
TP = 256
NCK = 16
ND = 8
NR = NCK - ND
DEPTH = 5
LAG = 5
EU = 4


def lse2_parts(parts):
    top = functools.reduce(jnp.maximum, parts)
    total = functools.reduce(jnp.add, [jnp.exp2(p - top) for p in parts])
    return top + jnp.log(total) * LOG2E


def dot_t(a, b):
    return lax.dot_general(a, b, (((1,), (1,)), ((), ())), preferred_element_type=jnp.float32)


def eye_mask(n):
    return lax.broadcasted_iota(jnp.int32, (n, n), 0) == lax.broadcasted_iota(jnp.int32, (n, n), 1)


def col_to_row(col):
    return jnp.sum(jnp.where(eye_mask(col.shape[0]), col, 0.0), axis=0, keepdims=True)


def row_to_col(row):
    return jnp.sum(jnp.where(eye_mask(row.shape[1]), row, 0.0), axis=1, keepdims=True)


def twice(b):
    return jnp.concatenate([b, b], axis=1)


def em_kernel(
    comp_size, row_size, sweeps,
    temp_ref, lp_ref, x_hbm, mu_hbm,
    mu_out, lp_out, lse_out,
    xg, mu_all, mub, bcol, brow, e_buf, m_buf, l_buf, lq_buf, s_acc, n_acc, mu_fin, lp_fin, sq_buf,
    zl_src, zl_buf, pre_buf, bc_src, bc_buf, tot_buf,
    load_sem, y_send, y_recv, z_send, z_recv, sy_send, sy_recv, sz_send, sz_recv, own_send, own_recv,
    zl_send, zl_recv, ag_send, ag_recv,
    pre_send, pre_recv, bc_send, bc_recv, post_send, post_recv,
    mx_send, mx_recv, br_send, br_recv, fin_send, fin_recv, lpf_send, lpf_recv, out_sem,
):
    z = lax.axis_index("comp")
    r = lax.axis_index("row")
    y, c = r // CORES, r % CORES
    n_chips = comp_size * row_size // CORES
    y_size = row_size // CORES
    chip = z * y_size + y
    block = x_hbm.shape[0]
    half_dim = x_hbm.shape[1] // 2
    total_pts = block * row_size
    n_own = mub.shape[2]
    total_comp = mu_hbm.shape[1] * comp_size
    bt = block // TP
    ch = block // NCK
    rs = y * CORES + (1 - c)
    ry = (1 - y) * CORES + c
    sib = {"row": rs}
    yn = {"row": ry}
    yd = {"row": (1 - y) * CORES + (1 - c)}
    zn = {"comp": z + 1 - 2 * (z % 2)}
    hz = z % 2

    def remote(src, dst, send, recv, dev):
        return pltpu.make_async_remote_copy(
            src_ref=src, dst_ref=dst, send_sem=send, recv_sem=recv, device_id=dev, device_id_type=MESH)

    def same(v, send, recv, dev):
        return remote(v, v, send, recv, dev)

    x_loads = [pltpu.make_async_copy(
        x_hbm.at[:, pl.ds(s * half_dim, half_dim)], xg.at[s, pl.ds(r * block, block), :], load_sem.at[s])
        for s in range(2)]
    mu_loads = [pltpu.make_async_copy(mu_hbm.at[s], mu_all.at[s], load_sem.at[2 + s]) for s in range(2)]
    for cp in x_loads + mu_loads:
        cp.start()

    barrier = pltpu.get_barrier_semaphore()
    for dev in (sib, yd):
        pl.semaphore_signal(barrier, inc=1, device_id=dev, device_id_type=MESH)
    for k in range(1, n_chips):
        q = lax.rem(chip + k, n_chips)
        pl.semaphore_signal(
            barrier, inc=1, device_id={"comp": q // y_size, "row": (q % y_size) * CORES + c},
            device_id_type=MESH)
    pl.semaphore_wait(barrier, n_chips + 1)

    def xrows(s, blk, cid):
        return xg.at[s, pl.ds(pl.multiple_of(blk * block + cid * ch, ch), ch), :]

    def cid_y(k):
        return k + hz * (NCK - 1 - 2 * k)

    def cid_z(k):
        return k + (1 - hz) * (NCK - 1 - 2 * k)

    def y_out(j):
        return same(xrows(j // ND, r, cid_y(j % ND)), y_send.at[j], y_recv.at[j], yn)

    def z_fwd(j):
        return same(xrows(j // ND, ry, cid_y(j % ND)), z_send.at[j], z_recv.at[j], zn)

    def sy_fwd(j):
        return same(xrows(j // ND, ry, cid_y(j % ND)), sy_send.at[j], sy_recv.at[j], sib)

    def sz_fwd(j):
        return same(xrows(j // ND, ry, cid_z(j % ND)), sz_send.at[j], sz_recv.at[j], sib)

    def own_out(s):
        return same(xg.at[s, pl.ds(r * block, block), :], own_send.at[s], own_recv.at[s], sib)

    n_steps = 2 * ND + LAG
    comb_end = 8

    def relay(j):
        @pl.when(j < 2 * ND)
        def _():
            y_out(j).wait()

            @pl.when(j + DEPTH < 2 * ND)
            def _():
                y_out(j + DEPTH).start()

            @pl.when(j % ND < NR)
            def _():
                z_fwd(j).start()

            sy_fwd(j).start()

        jz = j - LAG

        @pl.when(jnp.logical_and(jz >= 0, (jz + ND) % ND < NR))
        def _():
            z_fwd(jz).wait()
            sz_fwd(jz).start()

    def relays(a, b):
        def body(j, _):
            relay(j)
            return 0

        lax.fori_loop(a, b, body, 0)

    x_loads[0].wait()
    for j in range(min(DEPTH, ND)):
        y_out(j).start()
    own_out(0).start()
    x_loads[1].wait()
    own_out(1).start()
    for cp in mu_loads:
        cp.wait()

    def set_params(s, slot, mean, logw, t):
        mub[s, slot] = mean.astype(jnp.bfloat16)
        mu_sq = jnp.sum(mean * mean, axis=1, keepdims=True)
        col = (logw - temp_ref[t] * mu_sq) * LOG2E
        bcol[s, slot] = jnp.broadcast_to(col, (n_own, 128))
        return col

    def x_tile(s, tile):
        return xg[s, pl.ds(pl.multiple_of(tile * TP, TP), TP), :]

    def e_tile(s, slot, t, tile):
        a = dot_t(mub[s, slot], x_tile(s, tile))
        l2 = a * (temp_ref[t] * (2.0 * LOG2E)) + twice(bcol[s, slot])
        m = jnp.max(l2, axis=0, keepdims=True)
        e = jnp.exp2(l2 - m)
        return e, m, m + jnp.log(jnp.sum(e, axis=0, keepdims=True)) * LOG2E

    def e_step(s, t, hook=None):
        def body(i, _):
            for u in range(EU):
                tile = i * EU + u
                b, j = i * (EU // bt) + u // bt, u % bt
                e, m, l = e_tile(s, r, t, tile)
                e_buf[s, tile] = e
                m_buf[s, b, j:j + 1, :] = m
                l_buf[s, b, j:j + 1, :] = l
            if hook is not None:
                hook(i)
            return 0

        lax.fori_loop(0, total_pts // (TP * EU), body, 0)

    def acc_zero():
        s_acc[...] = jnp.zeros_like(s_acc)
        n_acc[...] = jnp.zeros_like(n_acc)

    def acc_block(s, b, resp_of):
        dots, ns = [], []
        for u in range(bt):
            resp = resp_of(u)
            ns.append(resp[:, :128] + resp[:, 128:])
            dots.append(jnp.dot(resp.astype(jnp.bfloat16), x_tile(s, b * bt + u), preferred_element_type=jnp.float32))
        s_acc[...] += functools.reduce(jnp.add, dots)
        n_acc[...] += functools.reduce(jnp.add, ns)

    def m_step(s, t):
        idx = 2 * t + s
        acc_zero()

        def body(b, _):
            def resp_of(u):
                f = jnp.exp2(m_buf[s, b, u:u + 1, :] - tot_buf[idx, b, u:u + 1, :])
                return e_buf[s, b * bt + u] * f

            acc_block(s, b, resp_of)
            return 0

        lax.fori_loop(0, row_size, body, 0)

    def mr_block(s, slot, t, b):
        idx = 2 * t + s

        def resp_of(u):
            a = dot_t(mub[s, slot], x_tile(s, b * bt + u))
            return jnp.exp2(a * (temp_ref[t] * (2.0 * LOG2E)) + twice(bcol[s, slot]) - tot_buf[idx, b, u:u + 1, :])

        acc_block(s, b, resp_of)

    def acc_result():
        cnt = jnp.sum(n_acc[...], axis=1, keepdims=True)
        mean = s_acc[...] / (cnt + EPS_COUNT)
        logw = jnp.log((cnt + PRIOR_ALPHA) / (total_pts + total_comp * PRIOR_ALPHA))
        return mean, logw

    def half(ref, k):
        return ref.at[pl.ds(2 * k, 2)]

    def pre(idx):
        return remote(half(l_buf.at[idx % 2], 1 - c), pre_buf.at[idx], pre_send.at[idx], pre_recv.at[idx], sib)

    def bcast(idx, k):
        q = lax.rem(chip + k, n_chips)
        return remote(bc_src.at[idx], bc_buf.at[idx, k - 1], bc_send.at[idx, k - 1], bc_recv.at[idx, k - 1],
                      {"comp": q // y_size, "row": (q % y_size) * CORES + c})

    def post(idx):
        return same(half(tot_buf.at[idx], c), post_send.at[idx], post_recv.at[idx], sib)

    def p2(idx):
        pre(idx).wait()
        bc_src[idx] = lse2_parts([l_buf[idx % 2, pl.ds(2 * c, 2)], pre_buf[idx]])
        for k in range(1, n_chips):
            bcast(idx, k).start()

    def p3(idx):
        for k in range(1, n_chips):
            bcast(idx, k).wait()
        tot_buf[idx, pl.ds(2 * c, 2)] = lse2_parts([bc_src[idx]] + [bc_buf[idx, k] for k in range(n_chips - 1)])
        post(idx).start()

    def zl(s, k):
        return remote(zl_src.at[s], zl_buf.at[s, k - 1], zl_send.at[s, k - 1], zl_recv.at[s, k - 1],
                      {"comp": lax.rem(z + k, comp_size)})

    def ag(s, k):
        return same(tot_buf.at[s, r], ag_send.at[s, k], ag_recv.at[s, k], (sib, yn, yd)[k])

    def orig_fit(s, _):
        def orig_slot(q, _):
            off = pl.multiple_of(q * n_own, n_own)
            set_params(s, q, mu_all[s, pl.ds(off, n_own), :], row_to_col(lp_ref[pl.ds(s, 1), pl.ds(off, n_own)]), 0)
            for u in range(bt):
                _, _, l = e_tile(s, q, 0, r * bt + u)
                lq_buf[q, u:u + 1, :] = l
            return 0

        lax.fori_loop(0, row_size, orig_slot, 0)
        zl_src[s] = lse2_parts([lq_buf[q] for q in range(row_size)])
        for k in range(1, comp_size):
            zl(s, k).start()
        relay(s)
        return 0

    lax.fori_loop(0, 2, orig_fit, 0)

    def comb(s, _):
        relays(2 + (comb_end - 2) // 2 * s, 2 + (comb_end - 2) // 2 * (s + 1))
        for k in range(1, comp_size):
            zl(s, k).wait()
        tot_buf[s, r] = lse2_parts([zl_src[s]] + [zl_buf[s, k] for k in range(comp_size - 1)])
        for k in range(3):
            ag(s, k).start()
        return 0

    lax.fori_loop(0, 2, comb, 0)

    ones = jnp.ones((8, half_dim), jnp.bfloat16)

    def sq_norms(s, _):
        for u in range(bt):
            x = x_tile(s, r * bt + u).astype(jnp.float32)
            sq = x * x
            hi = sq.astype(jnp.bfloat16)
            lo = (sq - hi.astype(jnp.float32)).astype(jnp.bfloat16)
            sq_buf[s, u:u + 1, :] = (dot_t(ones, hi) + dot_t(ones, lo))[0:1]
        return 0

    lax.fori_loop(0, 2, sq_norms, 0)

    def nth_block(k):
        yy = y + (k // 2) * (1 - 2 * y)
        cc = c + (k % 2) * (1 - 2 * c)
        return yy * CORES + cc

    first_end = ND + LAG
    hooks = total_pts // (TP * EU)

    def sweep0(s, _):
        begin = comb_end + s * (first_end + hooks - comb_end)
        relays(begin, begin + 1)
        for k in range(3):
            ag(s, k).wait()
        own_out(s).wait()
        acc_zero()

        def body(k, _):
            @pl.when(k == 2)
            def _():
                relays(begin + 1, first_end + s * (n_steps - first_end))

                def sib_waits(j, _):
                    sy_fwd(j).wait()

                    @pl.when(j % ND < NR)
                    def _():
                        sz_fwd(j).wait()

                    return 0

                lax.fori_loop(s * ND, (s + 1) * ND, sib_waits, 0)

            mr_block(s, r, 0, nth_block(k))
            return 0

        lax.fori_loop(0, row_size, body, 0)
        mean, logw = acc_result()
        set_params(s, r, mean, logw, 1)

        @pl.when(s == 1)
        def _():
            p2(2)

        def hook(i):
            @pl.when(s == 0)
            def _():
                relays(first_end + i, first_end + i + 1)

        e_step(s, 1, hook)
        pre(2 + s).start()

        @pl.when(s == 1)
        def _():
            p2(3)

        return 0

    lax.fori_loop(0, 2, sweep0, 0)

    def mx(s):
        return same(mub.at[s, r], mx_send.at[s], mx_recv.at[s], yn)

    def br(s):
        return same(brow.at[s, r], br_send.at[s], br_recv.at[s], yn)

    def fin(slot, s, k):
        return same(mu_fin.at[slot, s], fin_send.at[s, k], fin_recv.at[s, k], sib)

    def lpf(slot, k):
        return same(lp_fin.at[slot], lpf_send.at[k], lpf_recv.at[k], sib)

    def out(q, s):
        return pltpu.make_async_copy(
            mu_fin.at[q, s], mu_out.at[s, pl.ds(q * n_own, n_own), :], out_sem.at[q, s])

    def sweep(i, _):
        t, s = i // 2, i % 2
        last = t == sweeps - 1
        p3(i)
        post(i).wait()
        m_step(s, t)
        mean, logw = acc_result()

        @pl.when(t < sweeps - 1)
        def _():
            col = set_params(s, r, mean, logw, t + 1)

            @pl.when(t == sweeps - 2)
            def _():
                brow[s, r] = col_to_row(col)

            @pl.when(s == 1)
            def _():
                p2(i + 1)

                @pl.when(t == sweeps - 2)
                def _():
                    mx(0).start()
                    br(0).start()

            e_step(s, t + 1)
            pre(i + 2).start()

            @pl.when(s == 1)
            def _():
                p2(i + 2)

                @pl.when(t == sweeps - 2)
                def _():
                    mx(1).start()
                    br(1).start()

        @pl.when(last)
        def _():
            mu_fin[r, s] = mean
            lp_fin[r, pl.ds(s, 1), :] = col_to_row(logw)
            fin(r, s, 0).start()
            out(r, s).start()
            mx(s).wait()
            br(s).wait()
            bcol[s, ry] = jnp.broadcast_to(row_to_col(brow[s, ry]), (n_own, 128))
            acc_zero()

            def body(b, _):
                mr_block(s, ry, t, b)
                return 0

            lax.fori_loop(0, row_size, body, 0)
            mean2, logw2 = acc_result()
            mu_fin[ry, s] = mean2
            lp_fin[ry, pl.ds(s, 1), :] = col_to_row(logw2)
            fin(ry, s, 1).start()
            out(ry, s).start()

        return 0

    lax.fori_loop(2, 2 * sweeps, sweep, 0)
    lpf(r, 0).start()
    lpf(ry, 1).start()

    t = sweeps - 1
    for s in range(2):
        for j in range(bt):
            lse_out[s:s + 1, j * TP:(j + 1) * TP] = (
                tot_buf[2 * t + s, r, j:j + 1, :] * LN2 - temp_ref[t] * sq_buf[s, j:j + 1, :])

    yds = (1 - y) * CORES + (1 - c)
    for k, slot in ((0, rs), (1, yds)):
        for s in range(2):
            fin((r, ry)[k], s, k).wait()
            out(slot, s).start()
    lpf(r, 0).wait()
    lpf(ry, 1).wait()
    for q in range(row_size):
        lp_out[:, q * n_own:(q + 1) * n_own] = lp_fin[q]
    for q in range(row_size):
        for s in range(2):
            out(q, s).wait()


def solution(mesh):
    comp_size = mesh.shape["comp"]
    row_size = mesh.shape["row"]

    def local_fit(x_local, mu_init, logpi_init, inv_temp):
        block, dim = x_local.shape
        half_dim = dim // 2
        n_local = mu_init.shape[1]
        n_own = n_local // row_size
        total_pts = block * row_size
        tiles = total_pts // TP
        sweeps = inv_temp.shape[0]
        n_chips = comp_size * row_size // CORES
        ni = 2 * sweeps
        bt = block // TP
        f32, bf16 = jnp.float32, jnp.bfloat16
        dma = pltpu.SemaphoreType.DMA
        vm = pltpu.VMEM
        scratch = [
            vm((2, total_pts, half_dim), bf16),
            vm((2, n_local, half_dim), f32),
            vm((2, row_size, n_own, half_dim), bf16),
            vm((2, row_size, n_own, 128), f32),
            vm((2, row_size, 1, n_own), f32),
            vm((2, tiles, n_own, TP), f32),
            vm((2, row_size, bt, TP), f32),
            vm((2, row_size, bt, TP), f32),
            vm((row_size, bt, TP), f32),
            vm((n_own, half_dim), f32),
            vm((n_own, 128), f32),
            vm((row_size, 2, n_own, half_dim), f32),
            vm((row_size, 2, n_own), f32),
            vm((2, bt, TP), f32),
            vm((2, bt, TP), f32),
            vm((2, comp_size - 1, bt, TP), f32),
            vm((ni, 2, bt, TP), f32),
            vm((ni, 2, bt, TP), f32),
            vm((ni, n_chips - 1, 2, bt, TP), f32),
            vm((ni, row_size, bt, TP), f32),
            dma((4,)),
            dma((2 * ND,)), dma((2 * ND,)), dma((2 * ND,)), dma((2 * ND,)),
            dma((2 * ND,)), dma((2 * ND,)), dma((2 * ND,)), dma((2 * ND,)),
            dma((2,)), dma((2,)),
            dma((2, comp_size - 1)), dma((2, comp_size - 1)), dma((2, 3)), dma((2, 3)),
            dma((ni,)), dma((ni,)), dma((ni, n_chips - 1)), dma((ni, n_chips - 1)), dma((ni,)), dma((ni,)),
            dma((2,)), dma((2,)), dma((2,)), dma((2,)),
            dma((2, 2)), dma((2, 2)), dma((2,)), dma((2,)), dma((row_size, 2)),
        ]
        return pl.pallas_call(
            functools.partial(em_kernel, comp_size, row_size, sweeps),
            out_shape=(
                jax.ShapeDtypeStruct((2, n_local, half_dim), f32),
                jax.ShapeDtypeStruct((2, n_local), f32),
                jax.ShapeDtypeStruct((2, block), f32),
            ),
            in_specs=[
                pl.BlockSpec(memory_space=pltpu.SMEM),
                pl.BlockSpec(memory_space=pltpu.VMEM),
                pl.BlockSpec(memory_space=pl.ANY),
                pl.BlockSpec(memory_space=pl.ANY),
            ],
            out_specs=(
                pl.BlockSpec(memory_space=pl.ANY),
                pl.BlockSpec(memory_space=pltpu.VMEM),
                pl.BlockSpec(memory_space=pltpu.VMEM),
            ),
            scratch_shapes=scratch,
            compiler_params=pltpu.CompilerParams(
                collective_id=0, has_side_effects=True, vmem_limit_bytes=56 * 1024 * 1024),
        )(inv_temp, logpi_init, x_local, mu_init)

    return jax.shard_map(
        local_fit,
        mesh=mesh,
        in_specs=(P(("grp", "row"), None), P(None, ("grp", "comp"), None), P(None, ("grp", "comp")), P()),
        out_specs=(P(None, ("grp", "comp"), None), P(None, ("grp", "comp")), P(None, ("grp", "row"))),
        check_vma=False,
    )
```

```python
import functools

import jax
import jax.numpy as jnp
from jax import lax
from jax.experimental import pallas as pl
from jax.experimental.pallas import tpu as pltpu
from jax.sharding import PartitionSpec as P

EPS_COUNT = 1e-6
PRIOR_ALPHA = 1e-3
LOG2E = 1.4426950408889634
LN2 = 0.6931471805599453
MESH = pl.DeviceIdType.MESH

CORES = 2
TP = 256
NCK = 16
ND = 8
NR = NCK - ND
LAG = 4


def lse2_parts(parts):
    top = functools.reduce(jnp.maximum, parts)
    total = functools.reduce(jnp.add, [jnp.exp2(p - top) for p in parts])
    return top + jnp.log(total) * LOG2E


def dot_t(a, b):
    return lax.dot_general(a, b, (((1,), (1,)), ((), ())), preferred_element_type=jnp.float32)


def eye_mask(n):
    return lax.broadcasted_iota(jnp.int32, (n, n), 0) == lax.broadcasted_iota(jnp.int32, (n, n), 1)


def col_to_row(col):
    return jnp.sum(jnp.where(eye_mask(col.shape[0]), col, 0.0), axis=0, keepdims=True)


def row_to_col(row):
    return jnp.sum(jnp.where(eye_mask(row.shape[1]), row, 0.0), axis=1, keepdims=True)


def twice(b):
    return jnp.concatenate([b, b], axis=1)


def em_kernel(
    comp_size, row_size, sweeps,
    temp_ref, lp_ref, x_hbm, mu_hbm,
    mu_out, lp_out, lse_out,
    xg, mu_all, mub, bcol, brow, e_buf, m_buf, l_buf, lq_buf, s_acc, n_acc, mu_fin, lp_fin, sq_buf,
    zl_src, zl_buf, pre_buf, bc_src, bc_buf, tot_buf,
    load_sem, near_sem, far_sem, y_send, y_recv, z_send, z_recv, sy_send, sy_recv, sz_send, sz_recv, own_send, own_recv,
    zl_send, zl_recv, ag_send, ag_recv,
    pre_send, pre_recv, bc_send, bc_recv, post_send, post_recv,
    mx_send, mx_recv, br_send, br_recv, fin_send, fin_recv, lpf_send, lpf_recv, out_sem,
):
    z = lax.axis_index("comp")
    r = lax.axis_index("row")
    y, c = r // CORES, r % CORES
    n_chips = comp_size * row_size // CORES
    y_size = row_size // CORES
    chip = z * y_size + y
    block = x_hbm.shape[0]
    half_dim = x_hbm.shape[1] // 2
    total_pts = block * row_size
    n_own = mub.shape[2]
    total_comp = mu_hbm.shape[1] * comp_size
    bt = block // TP
    ch = block // NCK
    rs = y * CORES + (1 - c)
    ry = (1 - y) * CORES + c
    sib = {"row": rs}
    yn = {"row": ry}
    yd = {"row": (1 - y) * CORES + (1 - c)}
    zn = {"comp": z + 1 - 2 * (z % 2)}
    hz = z % 2

    def remote(src, dst, send, recv, dev):
        return pltpu.make_async_remote_copy(
            src_ref=src, dst_ref=dst, send_sem=send, recv_sem=recv, device_id=dev, device_id_type=MESH)

    def same(v, send, recv, dev):
        return remote(v, v, send, recv, dev)

    x_loads = [pltpu.make_async_copy(
        x_hbm.at[:, pl.ds(s * half_dim, half_dim)], xg.at[s, pl.ds(r * block, block), :], load_sem.at[s])
        for s in range(2)]
    mu_loads = [pltpu.make_async_copy(mu_hbm.at[s], mu_all.at[s], load_sem.at[2 + s]) for s in range(2)]
    for cp in x_loads + mu_loads:
        cp.start()

    n_z = (z > 0).astype(jnp.int32) + (z < comp_size - 1).astype(jnp.int32)

    def signal_z(sem):
        @pl.when(z > 0)
        def _():
            pl.semaphore_signal(sem, inc=1, device_id={"comp": z - 1}, device_id_type=MESH)

        @pl.when(z < comp_size - 1)
        def _():
            pl.semaphore_signal(sem, inc=1, device_id={"comp": z + 1}, device_id_type=MESH)

    def signal_near(sem):
        for dev in (sib, yn):
            pl.semaphore_signal(sem, inc=1, device_id=dev, device_id_type=MESH)
        signal_z(sem)

    barrier = pltpu.get_barrier_semaphore()
    signal_near(barrier)
    pl.semaphore_wait(barrier, 2 + n_z)
    signal_near(near_sem)

    def xrows(s, blk, cid):
        return xg.at[s, pl.ds(pl.multiple_of(blk * block + cid * ch, ch), ch), :]

    def cid_y(k):
        return k + hz * (NCK - 1 - 2 * k)

    def cid_z(k):
        return k + (1 - hz) * (NCK - 1 - 2 * k)

    def y_out(j):
        return same(xrows(j // ND, r, cid_y(j % ND)), y_send.at[j], y_recv.at[j], yn)

    def z_fwd(j):
        return same(xrows(j // ND, ry, cid_y(j % ND)), z_send.at[j], z_recv.at[j], zn)

    def sy_fwd(j):
        return same(xrows(j // ND, ry, cid_y(j % ND)), sy_send.at[j], sy_recv.at[j], sib)

    def sz_fwd(j):
        return same(xrows(j // ND, ry, cid_z(j % ND)), sz_send.at[j], sz_recv.at[j], sib)

    def own_out(s):
        return same(xg.at[s, pl.ds(r * block, block), :], own_send.at[s], own_recv.at[s], sib)

    n_steps = 2 * ND + LAG
    comb_end = 8
    first_end = ND + LAG

    def relay(j):
        @pl.when(j < 2 * ND)
        def _():
            y_out(j).wait()

            @pl.when(j % ND < NR)
            def _():
                z_fwd(j).start()

            sy_fwd(j).start()

        jz = j - LAG

        @pl.when(jnp.logical_and(jz >= 0, (jz + ND) % ND < NR))
        def _():
            z_fwd(jz).wait()
            sz_fwd(jz).start()

    def relays(a, b):
        def body(j, _):
            relay(j)
            return 0

        lax.fori_loop(a, b, body, 0)

    x_loads[0].wait()
    for j in range(ND):
        y_out(j).start()
    own_out(0).start()
    x_loads[1].wait()
    own_out(1).start()
    for cp in mu_loads:
        cp.wait()

    def set_params(s, slot, mean, logw, t):
        mub[s, slot] = mean.astype(jnp.bfloat16)
        mu_sq = jnp.sum(mean * mean, axis=1, keepdims=True)
        col = (logw - temp_ref[t] * mu_sq) * LOG2E
        bcol[s, slot] = jnp.broadcast_to(col, (n_own, 128))
        return col

    def x_tile(s, tile):
        return xg[s, pl.ds(pl.multiple_of(tile * TP, TP), TP), :]

    def e_tile(s, slot, t, tile):
        a = dot_t(mub[s, slot], x_tile(s, tile))
        l2 = a * (temp_ref[t] * (2.0 * LOG2E)) + twice(bcol[s, slot])
        m = jnp.max(l2, axis=0, keepdims=True)
        e = jnp.exp2(l2 - m)
        return e, m, m + jnp.log(jnp.sum(e, axis=0, keepdims=True)) * LOG2E

    def sib_half_first(i):
        return 2 * ((1 - c) + (i // 2) * (2 * c - 1)) + i % 2

    def own_half_first(i):
        return 2 * (c + (i // 2) * (1 - 2 * c)) + i % 2

    def e_step(s, t, idx, hook=None):
        def body(i, _):
            b = sib_half_first(i)
            for u in range(bt):
                e, m, l = e_tile(s, r, t, b * bt + u)
                e_buf[s, b * bt + u] = e
                m_buf[s, b, u:u + 1, :] = m
                l_buf[s, b, u:u + 1, :] = l

            @pl.when(i == 1)
            def _():
                pre(idx).start()

            if hook is not None:
                hook(i)
            return 0

        lax.fori_loop(0, row_size, body, 0)
        p2(idx)

    def acc_zero():
        s_acc[...] = jnp.zeros_like(s_acc)
        n_acc[...] = jnp.zeros_like(n_acc)

    def acc_block(s, b, resp_of):
        dots, ns = [], []
        for u in range(bt):
            resp = resp_of(u)
            ns.append(resp[:, :128] + resp[:, 128:])
            dots.append(jnp.dot(resp.astype(jnp.bfloat16), x_tile(s, b * bt + u), preferred_element_type=jnp.float32))
        s_acc[...] += functools.reduce(jnp.add, dots)
        n_acc[...] += functools.reduce(jnp.add, ns)

    def m_step(s, t):
        idx = 2 * t + s
        acc_zero()

        def body(i, _):
            @pl.when(i == 2)
            def _():
                post(idx).wait()

            b = own_half_first(i)

            def resp_of(u):
                f = jnp.exp2(m_buf[s, b, u:u + 1, :] - tot_buf[idx, b, u:u + 1, :])
                return e_buf[s, b * bt + u] * f

            acc_block(s, b, resp_of)
            return 0

        lax.fori_loop(0, row_size, body, 0)

    def mr_block(s, slot, t, b):
        idx = 2 * t + s

        def resp_of(u):
            a = dot_t(mub[s, slot], x_tile(s, b * bt + u))
            return jnp.exp2(a * (temp_ref[t] * (2.0 * LOG2E)) + twice(bcol[s, slot]) - tot_buf[idx, b, u:u + 1, :])

        acc_block(s, b, resp_of)

    def acc_result():
        cnt = jnp.sum(n_acc[...], axis=1, keepdims=True)
        mean = s_acc[...] / (cnt + EPS_COUNT)
        logw = jnp.log((cnt + PRIOR_ALPHA) / (total_pts + total_comp * PRIOR_ALPHA))
        return mean, logw

    def half(ref, k):
        return ref.at[pl.ds(2 * k, 2)]

    def pre(idx):
        return remote(half(l_buf.at[idx % 2], 1 - c), pre_buf.at[idx], pre_send.at[idx], pre_recv.at[idx], sib)

    def bcast(idx, k):
        q = lax.rem(chip + k, n_chips)
        return remote(bc_src.at[idx], bc_buf.at[idx, k - 1], bc_send.at[idx, k - 1], bc_recv.at[idx, k - 1],
                      {"comp": q // y_size, "row": (q % y_size) * CORES + c})

    def post(idx):
        return same(half(tot_buf.at[idx], c), post_send.at[idx], post_recv.at[idx], sib)

    def p2(idx):
        pre(idx).wait()
        bc_src[idx] = lse2_parts([l_buf[idx % 2, pl.ds(2 * c, 2)], pre_buf[idx]])
        for k in range(1, n_chips):
            bcast(idx, k).start()

    def p3(idx):
        for k in range(1, n_chips):
            bcast(idx, k).wait()
        tot_buf[idx, pl.ds(2 * c, 2)] = lse2_parts([bc_src[idx]] + [bc_buf[idx, k] for k in range(n_chips - 1)])
        post(idx).start()

    def zl(s, k):
        return remote(zl_src.at[s], zl_buf.at[s, k - 1], zl_send.at[s, k - 1], zl_recv.at[s, k - 1],
                      {"comp": lax.rem(z + k, comp_size)})

    def ag(s, k):
        return same(tot_buf.at[s, r], ag_send.at[s, k], ag_recv.at[s, k], (sib, yn, yd)[k])

    def orig_fit(s, _):
        def orig_slot(q, _):
            off = pl.multiple_of(q * n_own, n_own)
            set_params(s, q, mu_all[s, pl.ds(off, n_own), :], row_to_col(lp_ref[pl.ds(s, 1), pl.ds(off, n_own)]), 0)
            for u in range(bt):
                _, _, l = e_tile(s, q, 0, r * bt + u)
                lq_buf[q, u:u + 1, :] = l

            @pl.when(jnp.logical_and(s == 0, q == 1))
            def _():
                pl.semaphore_wait(near_sem, 2 + n_z)
                signal_z(far_sem)

            return 0

        lax.fori_loop(0, row_size, orig_slot, 0)
        zl_src[s] = lse2_parts([lq_buf[q] for q in range(row_size)])

        @pl.when(s == 0)
        def _():
            pl.semaphore_wait(far_sem, n_z)

        for k in range(1, comp_size):
            zl(s, k).start()
        relay(s)
        return 0

    lax.fori_loop(0, 2, orig_fit, 0)

    def comb(s, _):
        relays(2 + (comb_end - 2) // 2 * s, 2 + (comb_end - 2) // 2 * (s + 1))
        for k in range(1, comp_size):
            zl(s, k).wait()
        tot_buf[s, r] = lse2_parts([zl_src[s]] + [zl_buf[s, k] for k in range(comp_size - 1)])
        for k in range(3):
            ag(s, k).start()

        @pl.when(s == 0)
        def _():
            def send(j, _):
                y_out(j).start()
                return 0

            lax.fori_loop(ND, 2 * ND, send, 0)

        return 0

    lax.fori_loop(0, 2, comb, 0)

    def nth_block(k):
        yy = y + (k // 2) * (1 - 2 * y)
        cc = c + (k % 2) * (1 - 2 * c)
        return yy * CORES + cc

    def sweep0(s, _):
        @pl.when(s == 0)
        def _():
            relays(comb_end, first_end)

        for k in range(3):
            ag(s, k).wait()
        own_out(s).wait()
        acc_zero()

        def sib_waits(j, _):
            sy_fwd(j).wait()

            @pl.when(j % ND < NR)
            def _():
                sz_fwd(j).wait()

            return 0

        @pl.when(s == 0)
        def _():
            lax.fori_loop(0, ND, sib_waits, 0)

        def body(k, _):
            @pl.when(jnp.logical_and(s == 1, k == 2))
            def _():
                relays(first_end + 6, n_steps)
                lax.fori_loop(ND, 2 * ND, sib_waits, 0)

            mr_block(s, r, 0, nth_block(k))

            @pl.when(s == 0)
            def _():
                relay(first_end + k)

            return 0

        lax.fori_loop(0, row_size, body, 0)
        mean, logw = acc_result()
        set_params(s, r, mean, logw, 1)

        def hook(i):
            @pl.when(jnp.logical_and(s == 0, i < 2))
            def _():
                relay(first_end + 4 + i)

        e_step(s, 1, 2 + s, hook)
        return 0

    lax.fori_loop(0, 2, sweep0, 0)

    ones = jnp.ones((8, half_dim), jnp.bfloat16)

    def sq_norms(s, _):
        for u in range(bt):
            x = x_tile(s, r * bt + u).astype(jnp.float32)
            sq = x * x
            hi = sq.astype(jnp.bfloat16)
            lo = (sq - hi.astype(jnp.float32)).astype(jnp.bfloat16)
            sq_buf[s, u:u + 1, :] = (dot_t(ones, hi) + dot_t(ones, lo))[0:1]
        return 0

    lax.fori_loop(0, 2, sq_norms, 0)

    def mx(s):
        return same(mub.at[s, r], mx_send.at[s], mx_recv.at[s], yn)

    def br(s):
        return same(brow.at[s, r], br_send.at[s], br_recv.at[s], yn)

    def fin(slot, s, k):
        return same(mu_fin.at[slot, s], fin_send.at[s, k], fin_recv.at[s, k], sib)

    def lpf(slot, k):
        return same(lp_fin.at[slot], lpf_send.at[k], lpf_recv.at[k], sib)

    def out(q, s):
        return pltpu.make_async_copy(
            mu_fin.at[q, s], mu_out.at[s, pl.ds(q * n_own, n_own), :], out_sem.at[q, s])

    def sweep(i, _):
        t, s = i // 2, i % 2
        last = t == sweeps - 1
        p3(i)
        m_step(s, t)
        mean, logw = acc_result()

        @pl.when(t < sweeps - 1)
        def _():
            col = set_params(s, r, mean, logw, t + 1)

            @pl.when(t == sweeps - 2)
            def _():
                brow[s, r] = col_to_row(col)

            e_step(s, t + 1, i + 2)

            @pl.when(t == sweeps - 2)
            def _():
                mx(s).start()
                br(s).start()

        @pl.when(last)
        def _():
            mu_fin[r, s] = mean
            lp_fin[r, pl.ds(s, 1), :] = col_to_row(logw)
            fin(r, s, 0).start()
            out(r, s).start()
            mx(s).wait()
            br(s).wait()
            bcol[s, ry] = jnp.broadcast_to(row_to_col(brow[s, ry]), (n_own, 128))
            acc_zero()

            def body(b, _):
                mr_block(s, ry, t, b)
                return 0

            lax.fori_loop(0, row_size, body, 0)
            mean2, logw2 = acc_result()
            mu_fin[ry, s] = mean2
            lp_fin[ry, pl.ds(s, 1), :] = col_to_row(logw2)
            fin(ry, s, 1).start()
            out(ry, s).start()

        return 0

    lax.fori_loop(2, 2 * sweeps, sweep, 0)
    lpf(r, 0).start()
    lpf(ry, 1).start()

    t = sweeps - 1
    for s in range(2):
        for j in range(bt):
            lse_out[s:s + 1, j * TP:(j + 1) * TP] = (
                tot_buf[2 * t + s, r, j:j + 1, :] * LN2 - temp_ref[t] * sq_buf[s, j:j + 1, :])

    yds = (1 - y) * CORES + (1 - c)
    for k, slot in ((0, rs), (1, yds)):
        for s in range(2):
            fin((r, ry)[k], s, k).wait()
            out(slot, s).start()
    lpf(r, 0).wait()
    lpf(ry, 1).wait()
    for q in range(row_size):
        lp_out[:, q * n_own:(q + 1) * n_own] = lp_fin[q]
    for q in range(row_size):
        for s in range(2):
            out(q, s).wait()


def solution(mesh):
    comp_size = mesh.shape["comp"]
    row_size = mesh.shape["row"]

    def local_fit(x_local, mu_init, logpi_init, inv_temp):
        block, dim = x_local.shape
        half_dim = dim // 2
        n_local = mu_init.shape[1]
        n_own = n_local // row_size
        total_pts = block * row_size
        tiles = total_pts // TP
        sweeps = inv_temp.shape[0]
        n_chips = comp_size * row_size // CORES
        ni = 2 * sweeps
        bt = block // TP
        f32, bf16 = jnp.float32, jnp.bfloat16
        dma = pltpu.SemaphoreType.DMA
        vm = pltpu.VMEM
        scratch = [
            vm((2, total_pts, half_dim), bf16),
            vm((2, n_local, half_dim), f32),
            vm((2, row_size, n_own, half_dim), bf16),
            vm((2, row_size, n_own, 128), f32),
            vm((2, row_size, 1, n_own), f32),
            vm((2, tiles, n_own, TP), f32),
            vm((2, row_size, bt, TP), f32),
            vm((2, row_size, bt, TP), f32),
            vm((row_size, bt, TP), f32),
            vm((n_own, half_dim), f32),
            vm((n_own, 128), f32),
            vm((row_size, 2, n_own, half_dim), f32),
            vm((row_size, 2, n_own), f32),
            vm((2, bt, TP), f32),
            vm((2, bt, TP), f32),
            vm((2, comp_size - 1, bt, TP), f32),
            vm((ni, 2, bt, TP), f32),
            vm((ni, 2, bt, TP), f32),
            vm((ni, n_chips - 1, 2, bt, TP), f32),
            vm((ni, row_size, bt, TP), f32),
            dma((4,)), pltpu.SemaphoreType.REGULAR, pltpu.SemaphoreType.REGULAR,
            dma((2 * ND,)), dma((2 * ND,)), dma((2 * ND,)), dma((2 * ND,)),
            dma((2 * ND,)), dma((2 * ND,)), dma((2 * ND,)), dma((2 * ND,)),
            dma((2,)), dma((2,)),
            dma((2, comp_size - 1)), dma((2, comp_size - 1)), dma((2, 3)), dma((2, 3)),
            dma((ni,)), dma((ni,)), dma((ni, n_chips - 1)), dma((ni, n_chips - 1)), dma((ni,)), dma((ni,)),
            dma((2,)), dma((2,)), dma((2,)), dma((2,)),
            dma((2, 2)), dma((2, 2)), dma((2,)), dma((2,)), dma((row_size, 2)),
        ]
        return pl.pallas_call(
            functools.partial(em_kernel, comp_size, row_size, sweeps),
            out_shape=(
                jax.ShapeDtypeStruct((2, n_local, half_dim), f32),
                jax.ShapeDtypeStruct((2, n_local), f32),
                jax.ShapeDtypeStruct((2, block), f32),
            ),
            in_specs=[
                pl.BlockSpec(memory_space=pltpu.SMEM),
                pl.BlockSpec(memory_space=pltpu.VMEM),
                pl.BlockSpec(memory_space=pl.ANY),
                pl.BlockSpec(memory_space=pl.ANY),
            ],
            out_specs=(
                pl.BlockSpec(memory_space=pl.ANY),
                pl.BlockSpec(memory_space=pltpu.VMEM),
                pl.BlockSpec(memory_space=pltpu.VMEM),
            ),
            scratch_shapes=scratch,
            compiler_params=pltpu.CompilerParams(
                collective_id=0, has_side_effects=True, vmem_limit_bytes=56 * 1024 * 1024),
        )(inv_temp, logpi_init, x_local, mu_init)

    return jax.shard_map(
        local_fit,
        mesh=mesh,
        in_specs=(P(("grp", "row"), None), P(None, ("grp", "comp"), None), P(None, ("grp", "comp")), P()),
        out_specs=(P(None, ("grp", "comp"), None), P(None, ("grp", "comp")), P(None, ("grp", "row"))),
        check_vma=False,
    )
```

```python
import functools

import jax
import jax.numpy as jnp
from jax import lax
from jax.experimental import pallas as pl
from jax.experimental.pallas import tpu as pltpu
from jax.sharding import PartitionSpec as P

EPS_COUNT = 1e-6
PRIOR_ALPHA = 1e-3
LOG2E = 1.4426950408889634
LN2 = 0.6931471805599453
MESH = pl.DeviceIdType.MESH

CORES = 2
TP = 256
NCK = 16
ND = 8
NR = NCK - ND
LAG = 4


def lse2_parts(parts):
    top = functools.reduce(jnp.maximum, parts)
    total = functools.reduce(jnp.add, [jnp.exp2(p - top) for p in parts])
    return top + jnp.log(total) * LOG2E


def dot_t(a, b):
    return lax.dot_general(a, b, (((1,), (1,)), ((), ())), preferred_element_type=jnp.float32)


def eye_mask(n):
    return lax.broadcasted_iota(jnp.int32, (n, n), 0) == lax.broadcasted_iota(jnp.int32, (n, n), 1)


def col_to_row(col):
    return jnp.sum(jnp.where(eye_mask(col.shape[0]), col, 0.0), axis=0, keepdims=True)


def row_to_col(row):
    return jnp.sum(jnp.where(eye_mask(row.shape[1]), row, 0.0), axis=1, keepdims=True)


def twice(b):
    return jnp.concatenate([b, b], axis=1)


def em_kernel(
    comp_size, row_size, sweeps,
    temp_ref, lp_ref, x_hbm, mu_hbm,
    mu_out, lp_out, lse_out,
    xg, mu_all, mub, bcol, brow, e_buf, m_buf, l_buf, lq_buf, s_acc, n_acc, lp_fin, sq_buf,
    zl_src, zl_buf, pre_buf, bc_src, bc_buf, tot_buf,
    load_sem, near_sem, far_sem, y_send, y_recv, z_send, z_recv, sy_send, sy_recv, sz_send, sz_recv, own_send, own_recv,
    zl_send, zl_recv, ag_send, ag_recv,
    pre_send, pre_recv, bc_send, bc_recv, post_send, post_recv,
    mx_send, mx_recv, br_send, br_recv, fin_send, fin_recv, lpf_send, lpf_recv,
):
    z = lax.axis_index("comp")
    r = lax.axis_index("row")
    y, c = r // CORES, r % CORES
    n_chips = comp_size * row_size // CORES
    y_size = row_size // CORES
    chip = z * y_size + y
    block = x_hbm.shape[0]
    half_dim = x_hbm.shape[1] // 2
    total_pts = block * row_size
    n_own = mub.shape[2]
    total_comp = mu_hbm.shape[1] * comp_size
    bt = block // TP
    ch = block // NCK
    rs = y * CORES + (1 - c)
    ry = (1 - y) * CORES + c
    sib = {"row": rs}
    yn = {"row": ry}
    yd = {"row": (1 - y) * CORES + (1 - c)}
    zn = {"comp": z + 1 - 2 * (z % 2)}
    hz = z % 2

    def remote(src, dst, send, recv, dev):
        return pltpu.make_async_remote_copy(
            src_ref=src, dst_ref=dst, send_sem=send, recv_sem=recv, device_id=dev, device_id_type=MESH)

    def same(v, send, recv, dev):
        return remote(v, v, send, recv, dev)

    x_loads = [pltpu.make_async_copy(
        x_hbm.at[:, pl.ds(s * half_dim, half_dim)], xg.at[s, pl.ds(r * block, block), :], load_sem.at[s])
        for s in range(2)]
    mu_loads = [pltpu.make_async_copy(mu_hbm.at[s], mu_all.at[s], load_sem.at[2 + s]) for s in range(2)]
    for cp in x_loads + mu_loads:
        cp.start()

    n_z = (z > 0).astype(jnp.int32) + (z < comp_size - 1).astype(jnp.int32)

    def signal_z(sem):
        @pl.when(z > 0)
        def _():
            pl.semaphore_signal(sem, inc=1, device_id={"comp": z - 1}, device_id_type=MESH)

        @pl.when(z < comp_size - 1)
        def _():
            pl.semaphore_signal(sem, inc=1, device_id={"comp": z + 1}, device_id_type=MESH)

    def signal_near(sem):
        for dev in (sib, yn):
            pl.semaphore_signal(sem, inc=1, device_id=dev, device_id_type=MESH)
        signal_z(sem)

    barrier = pltpu.get_barrier_semaphore()
    signal_near(barrier)
    pl.semaphore_wait(barrier, 2 + n_z)
    signal_near(near_sem)

    def xrows(s, blk, cid):
        return xg.at[s, pl.ds(pl.multiple_of(blk * block + cid * ch, ch), ch), :]

    def cid_y(k):
        return k + hz * (NCK - 1 - 2 * k)

    def cid_z(k):
        return k + (1 - hz) * (NCK - 1 - 2 * k)

    def y_out(j):
        return same(xrows(j // ND, r, cid_y(j % ND)), y_send.at[j], y_recv.at[j], yn)

    def z_fwd(j):
        return same(xrows(j // ND, ry, cid_y(j % ND)), z_send.at[j], z_recv.at[j], zn)

    def sy_fwd(j):
        return same(xrows(j // ND, ry, cid_y(j % ND)), sy_send.at[j], sy_recv.at[j], sib)

    def sz_fwd(j):
        return same(xrows(j // ND, ry, cid_z(j % ND)), sz_send.at[j], sz_recv.at[j], sib)

    def own_out(s):
        return same(xg.at[s, pl.ds(r * block, block), :], own_send.at[s], own_recv.at[s], sib)

    n_steps = 2 * ND + LAG
    comb_end = 10
    first_end = ND + LAG

    def relay(j):
        @pl.when(j < 2 * ND)
        def _():
            y_out(j).wait()

            @pl.when(j % ND < NR)
            def _():
                z_fwd(j).start()

            sy_fwd(j).start()

        jz = j - LAG

        @pl.when(jnp.logical_and(jz >= 0, (jz + ND) % ND < NR))
        def _():
            z_fwd(jz).wait()
            sz_fwd(jz).start()

    def relays(a, b):
        def body(j, _):
            relay(j)
            return 0

        lax.fori_loop(a, b, body, 0)

    x_loads[0].wait()
    for j in range(ND):
        y_out(j).start()
    own_out(0).start()
    x_loads[1].wait()
    own_out(1).start()
    for cp in mu_loads:
        cp.wait()

    def set_params(s, slot, mean, logw, t):
        mub[s, slot] = mean.astype(jnp.bfloat16)
        mu_sq = jnp.sum(mean * mean, axis=1, keepdims=True)
        col = (logw - temp_ref[t] * mu_sq) * LOG2E
        bcol[s, slot] = jnp.broadcast_to(col, (n_own, 128))
        return col

    def x_tile(s, tile):
        return xg[s, pl.ds(pl.multiple_of(tile * TP, TP), TP), :]

    def e_tile(s, slot, t, tile):
        a = dot_t(mub[s, slot], x_tile(s, tile))
        l2 = a * (temp_ref[t] * (2.0 * LOG2E)) + twice(bcol[s, slot])
        m = jnp.max(l2, axis=0, keepdims=True)
        e = jnp.exp2(l2 - m)
        return e, m, m + jnp.log(jnp.sum(e, axis=0, keepdims=True)) * LOG2E

    def tiles_of(half_id):
        return [(2 * half_id + k // bt, k % bt) for k in range(2 * bt)]

    def e_step(s, t, idx, hook=None):
        def body(i, _):
            h = (1 - c) + i * (2 * c - 1)
            for b, u in tiles_of(h):
                e, m, l = e_tile(s, r, t, b * bt + u)
                e_buf[s, b * bt + u] = e
                m_buf[s, b, u:u + 1, :] = m
                l_buf[s, b, u:u + 1, :] = l

            @pl.when(i == 0)
            def _():
                pre(idx).start()

            if hook is not None:
                hook(i)
            return 0

        lax.fori_loop(0, 2, body, 0)
        p2(idx)

    def acc_zero():
        s_acc[...] = jnp.zeros_like(s_acc)
        n_acc[...] = jnp.zeros_like(n_acc)

    def acc_tiles(s, tiles, resp_of):
        dots, ns = [], []
        for b, u in tiles:
            resp = resp_of(b, u)
            ns.append(resp[:, :128] + resp[:, 128:])
            dots.append(jnp.dot(resp.astype(jnp.bfloat16), x_tile(s, b * bt + u), preferred_element_type=jnp.float32))
        s_acc[...] += functools.reduce(jnp.add, dots)
        n_acc[...] += functools.reduce(jnp.add, ns)

    def m_step(s, t):
        idx = 2 * t + s
        acc_zero()

        def body(i, _):
            @pl.when(i == 1)
            def _():
                post(idx).wait()

            def resp_of(b, u):
                f = jnp.exp2(m_buf[s, b, u:u + 1, :] - tot_buf[idx, b, u:u + 1, :])
                return e_buf[s, b * bt + u] * f

            acc_tiles(s, tiles_of(c + i * (1 - 2 * c)), resp_of)
            return 0

        lax.fori_loop(0, 2, body, 0)

    def mr_half(s, slot, t, half_id):
        idx = 2 * t + s

        def resp_of(b, u):
            a = dot_t(mub[s, slot], x_tile(s, b * bt + u))
            return jnp.exp2(a * (temp_ref[t] * (2.0 * LOG2E)) + twice(bcol[s, slot]) - tot_buf[idx, b, u:u + 1, :])

        acc_tiles(s, tiles_of(half_id), resp_of)

    def acc_result():
        cnt = jnp.sum(n_acc[...], axis=1, keepdims=True)
        mean = s_acc[...] / (cnt + EPS_COUNT)
        logw = jnp.log((cnt + PRIOR_ALPHA) / (total_pts + total_comp * PRIOR_ALPHA))
        return mean, logw

    def half(ref, k):
        return ref.at[pl.ds(2 * k, 2)]

    def pre(idx):
        return remote(half(l_buf.at[idx % 2], 1 - c), pre_buf.at[idx], pre_send.at[idx], pre_recv.at[idx], sib)

    def bcast(idx, k):
        q = lax.rem(chip + k, n_chips)
        return remote(bc_src.at[idx], bc_buf.at[idx, k - 1], bc_send.at[idx, k - 1], bc_recv.at[idx, k - 1],
                      {"comp": q // y_size, "row": (q % y_size) * CORES + c})

    def post(idx):
        return same(half(tot_buf.at[idx], c), post_send.at[idx], post_recv.at[idx], sib)

    def p2(idx):
        pre(idx).wait()
        bc_src[idx] = lse2_parts([l_buf[idx % 2, pl.ds(2 * c, 2)], pre_buf[idx]])
        for k in range(1, n_chips):
            bcast(idx, k).start()

    def p3(idx):
        for k in range(1, n_chips):
            bcast(idx, k).wait()
        tot_buf[idx, pl.ds(2 * c, 2)] = lse2_parts([bc_src[idx]] + [bc_buf[idx, k] for k in range(n_chips - 1)])
        post(idx).start()

    def zl(s, k):
        return remote(zl_src.at[s], zl_buf.at[s, k - 1], zl_send.at[s, k - 1], zl_recv.at[s, k - 1],
                      {"comp": lax.rem(z + k, comp_size)})

    def ag(s, k):
        return same(tot_buf.at[s, r], ag_send.at[s, k], ag_recv.at[s, k], (sib, yn, yd)[k])

    def orig_fit(s, _):
        def orig_slots(p, _):
            for k in range(2):
                q = 2 * p + k
                off = pl.multiple_of(q * n_own, n_own)
                set_params(s, q, mu_all[s, pl.ds(off, n_own), :], row_to_col(lp_ref[pl.ds(s, 1), pl.ds(off, n_own)]), 0)
                for u in range(bt):
                    _, _, l = e_tile(s, q, 0, r * bt + u)
                    lq_buf[q, u:u + 1, :] = l

            @pl.when(jnp.logical_and(s == 0, p == 0))
            def _():
                pl.semaphore_wait(near_sem, 2 + n_z)
                signal_z(far_sem)

            @pl.when(s == 1)
            def _():
                relays(2 * p, 2 * p + 2)

            return 0

        lax.fori_loop(0, row_size // 2, orig_slots, 0)
        zl_src[s] = lse2_parts([lq_buf[q] for q in range(row_size)])

        @pl.when(s == 0)
        def _():
            pl.semaphore_wait(far_sem, n_z)

        for k in range(1, comp_size):
            zl(s, k).start()
        return 0

    lax.fori_loop(0, 2, orig_fit, 0)

    def y_sends(a, b):
        def send(j, _):
            y_out(j).start()
            return 0

        lax.fori_loop(a, b, send, 0)

    early = ND + 3
    y_sends(ND, early)

    def comb(s, _):
        relays(4 + 3 * s, 7 + 3 * s)
        for k in range(1, comp_size):
            zl(s, k).wait()
        tot_buf[s, r] = lse2_parts([zl_src[s]] + [zl_buf[s, k] for k in range(comp_size - 1)])
        for k in range(3):
            ag(s, k).start()

        @pl.when(s == 0)
        def _():
            y_sends(early, 2 * ND)

        return 0

    lax.fori_loop(0, 2, comb, 0)

    def sweep0(s, _):
        @pl.when(s == 0)
        def _():
            relays(comb_end, first_end)

        for k in range(3):
            ag(s, k).wait()
        own_out(s).wait()
        acc_zero()

        def sib_waits(j, _):
            sy_fwd(j).wait()

            @pl.when(j % ND < NR)
            def _():
                sz_fwd(j).wait()

            return 0

        @pl.when(s == 0)
        def _():
            lax.fori_loop(0, ND, sib_waits, 0)

        def body(k, _):
            @pl.when(jnp.logical_and(s == 1, k == 1))
            def _():
                relays(first_end + 6, n_steps)
                lax.fori_loop(ND, 2 * ND, sib_waits, 0)

            mr_half(s, r, 0, y + k * (1 - 2 * y))

            @pl.when(s == 0)
            def _():
                relays(first_end + 2 * k, first_end + 2 * k + 2)

            return 0

        lax.fori_loop(0, 2, body, 0)
        mean, logw = acc_result()
        set_params(s, r, mean, logw, 1)

        def hook(i):
            @pl.when(jnp.logical_and(s == 0, i == 0))
            def _():
                relays(first_end + 4, first_end + 6)

        e_step(s, 1, 2 + s, hook)
        return 0

    lax.fori_loop(0, 2, sweep0, 0)

    ones = jnp.ones((8, half_dim), jnp.bfloat16)

    def sq_norms(s, _):
        for u in range(bt):
            x = x_tile(s, r * bt + u).astype(jnp.float32)
            sq = x * x
            hi = sq.astype(jnp.bfloat16)
            lo = (sq - hi.astype(jnp.float32)).astype(jnp.bfloat16)
            sq_buf[s, u:u + 1, :] = (dot_t(ones, hi) + dot_t(ones, lo))[0:1]
        return 0

    lax.fori_loop(0, 2, sq_norms, 0)

    def mx(s):
        return same(mub.at[s, r], mx_send.at[s], mx_recv.at[s], yn)

    def br(s):
        return same(brow.at[s, r], br_send.at[s], br_recv.at[s], yn)

    def mean_rows(slot, s):
        return mu_out.at[s, pl.ds(pl.multiple_of(slot * n_own, n_own), n_own), :]

    def fin(slot, s, k):
        return same(mean_rows(slot, s), fin_send.at[s, k], fin_recv.at[s, k], sib)

    def lpf(slot, k):
        return same(lp_fin.at[slot], lpf_send.at[k], lpf_recv.at[k], sib)

    def sweep(i, _):
        t, s = i // 2, i % 2
        last = t == sweeps - 1
        p3(i)
        m_step(s, t)
        mean, logw = acc_result()

        @pl.when(t < sweeps - 1)
        def _():
            col = set_params(s, r, mean, logw, t + 1)

            @pl.when(t == sweeps - 2)
            def _():
                brow[s, r] = col_to_row(col)

            e_step(s, t + 1, i + 2)

            @pl.when(t == sweeps - 2)
            def _():
                mx(s).start()
                br(s).start()

        @pl.when(last)
        def _():
            mean_rows(r, s)[...] = mean
            lp_fin[r, pl.ds(s, 1), :] = col_to_row(logw)
            fin(r, s, 0).start()
            mx(s).wait()
            br(s).wait()
            bcol[s, ry] = jnp.broadcast_to(row_to_col(brow[s, ry]), (n_own, 128))
            acc_zero()

            def body(h, _):
                mr_half(s, ry, t, h)
                return 0

            lax.fori_loop(0, 2, body, 0)
            mean2, logw2 = acc_result()
            mean_rows(ry, s)[...] = mean2
            lp_fin[ry, pl.ds(s, 1), :] = col_to_row(logw2)
            fin(ry, s, 1).start()

        return 0

    lax.fori_loop(2, 2 * sweeps, sweep, 0)
    lpf(r, 0).start()
    lpf(ry, 1).start()

    t = sweeps - 1
    for s in range(2):
        for j in range(bt):
            lse_out[s:s + 1, j * TP:(j + 1) * TP] = (
                tot_buf[2 * t + s, r, j:j + 1, :] * LN2 - temp_ref[t] * sq_buf[s, j:j + 1, :])

    for k in range(2):
        for s in range(2):
            fin((r, ry)[k], s, k).wait()
    lpf(r, 0).wait()
    lpf(ry, 1).wait()
    for q in range(row_size):
        lp_out[:, q * n_own:(q + 1) * n_own] = lp_fin[q]


def solution(mesh):
    comp_size = mesh.shape["comp"]
    row_size = mesh.shape["row"]

    def local_fit(x_local, mu_init, logpi_init, inv_temp):
        block, dim = x_local.shape
        half_dim = dim // 2
        n_local = mu_init.shape[1]
        n_own = n_local // row_size
        total_pts = block * row_size
        tiles = total_pts // TP
        sweeps = inv_temp.shape[0]
        n_chips = comp_size * row_size // CORES
        ni = 2 * sweeps
        bt = block // TP
        f32, bf16 = jnp.float32, jnp.bfloat16
        dma = pltpu.SemaphoreType.DMA
        vm = pltpu.VMEM
        scratch = [
            vm((2, total_pts, half_dim), bf16),
            vm((2, n_local, half_dim), f32),
            vm((2, row_size, n_own, half_dim), bf16),
            vm((2, row_size, n_own, 128), f32),
            vm((2, row_size, 1, n_own), f32),
            vm((2, tiles, n_own, TP), f32),
            vm((2, row_size, bt, TP), f32),
            vm((2, row_size, bt, TP), f32),
            vm((row_size, bt, TP), f32),
            vm((n_own, half_dim), f32),
            vm((n_own, 128), f32),
            vm((row_size, 2, n_own), f32),
            vm((2, bt, TP), f32),
            vm((2, bt, TP), f32),
            vm((2, comp_size - 1, bt, TP), f32),
            vm((ni, 2, bt, TP), f32),
            vm((ni, 2, bt, TP), f32),
            vm((ni, n_chips - 1, 2, bt, TP), f32),
            vm((ni, row_size, bt, TP), f32),
            dma((4,)), pltpu.SemaphoreType.REGULAR, pltpu.SemaphoreType.REGULAR,
            dma((2 * ND,)), dma((2 * ND,)), dma((2 * ND,)), dma((2 * ND,)),
            dma((2 * ND,)), dma((2 * ND,)), dma((2 * ND,)), dma((2 * ND,)),
            dma((2,)), dma((2,)),
            dma((2, comp_size - 1)), dma((2, comp_size - 1)), dma((2, 3)), dma((2, 3)),
            dma((ni,)), dma((ni,)), dma((ni, n_chips - 1)), dma((ni, n_chips - 1)), dma((ni,)), dma((ni,)),
            dma((2,)), dma((2,)), dma((2,)), dma((2,)),
            dma((2, 2)), dma((2, 2)), dma((2,)), dma((2,)),
        ]
        return pl.pallas_call(
            functools.partial(em_kernel, comp_size, row_size, sweeps),
            out_shape=(vm((2, n_local, half_dim), f32), vm((2, n_local), f32), vm((2, block), f32)),
            in_specs=[
                pl.BlockSpec(memory_space=pltpu.SMEM),
                pl.BlockSpec(memory_space=pltpu.VMEM),
                pl.BlockSpec(memory_space=pl.ANY),
                pl.BlockSpec(memory_space=pl.ANY),
            ],
            out_specs=(pl.BlockSpec(memory_space=pltpu.VMEM),) * 3,
            scratch_shapes=scratch,
            compiler_params=pltpu.CompilerParams(
                collective_id=0, has_side_effects=True, vmem_limit_bytes=56 * 1024 * 1024),
        )(inv_temp, logpi_init, x_local, mu_init)

    return jax.shard_map(
        local_fit,
        mesh=mesh,
        in_specs=(P(("grp", "row"), None), P(None, ("grp", "comp"), None), P(None, ("grp", "comp")), P()),
        out_specs=(P(None, ("grp", "comp"), None), P(None, ("grp", "comp")), P(None, ("grp", "row"))),
        check_vma=False,
    )
```

```python
import functools

import jax
import jax.numpy as jnp
from jax import lax
from jax.experimental import pallas as pl
from jax.experimental.pallas import tpu as pltpu
from jax.sharding import PartitionSpec as P

EPS_COUNT = 1e-6
PRIOR_ALPHA = 1e-3
LOG2E = 1.4426950408889634
LN2 = 0.6931471805599453
MESH = pl.DeviceIdType.MESH

CORES = 2
TP = 256
NCK = 16
ND = 8


def lse2_parts(parts):
    top = functools.reduce(jnp.maximum, parts)
    total = functools.reduce(jnp.add, [jnp.exp2(p - top) for p in parts])
    return top + jnp.log(total) * LOG2E


def dot_t(a, b):
    return lax.dot_general(a, b, (((1,), (1,)), ((), ())), preferred_element_type=jnp.float32)


def eye_mask(n):
    return lax.broadcasted_iota(jnp.int32, (n, n), 0) == lax.broadcasted_iota(jnp.int32, (n, n), 1)


def col_to_row(col):
    return jnp.sum(jnp.where(eye_mask(col.shape[0]), col, 0.0), axis=0, keepdims=True)


def row_to_col(row):
    return jnp.sum(jnp.where(eye_mask(row.shape[1]), row, 0.0), axis=1, keepdims=True)


def twice(b):
    return jnp.concatenate([b, b], axis=1)


def write_kernel(a, b, c, a_out, b_out, c_out, sems):
    copies = [pltpu.make_async_copy(v, o, sems.at[k]) for k, (v, o) in enumerate(((a, a_out), (b, b_out), (c, c_out)))]
    for cp in copies:
        cp.start()
    for cp in copies:
        cp.wait()


def em_kernel(
    comp_size, row_size, sweeps,
    temp_ref, lp_ref, x_hbm, mu_hbm,
    mu_out, lp_out, lse_out,
    xg, mu_all, mub, bcol, brow, e_buf, m_buf, l_buf, lq_buf, s_acc, n_acc, lp_fin, sq_buf,
    zl_src, zl_buf, pre_buf, bc_src, bc_buf, tot_buf,
    load_sem, near_sem, far_sem, y_send, y_recv, z_send, z_recv, sy_send, sy_recv, sz_send, sz_recv, own_send, own_recv,
    zl_send, zl_recv, ag_send, ag_recv,
    pre_send, pre_recv, bc_send, bc_recv, post_send, post_recv,
    mx_send, mx_recv, br_send, br_recv, fin_send, fin_recv, lpf_send, lpf_recv,
):
    z = lax.axis_index("comp")
    r = lax.axis_index("row")
    y, c = r // CORES, r % CORES
    n_chips = comp_size * row_size // CORES
    y_size = row_size // CORES
    chip = z * y_size + y
    block = x_hbm.shape[0]
    half_dim = x_hbm.shape[1] // 2
    total_pts = block * row_size
    n_own = mub.shape[2]
    total_comp = mu_hbm.shape[1] * comp_size
    bt = block // TP
    ch = block // NCK
    rs = y * CORES + (1 - c)
    ry = (1 - y) * CORES + c
    sib = {"row": rs}
    yn = {"row": ry}
    yd = {"row": (1 - y) * CORES + (1 - c)}
    zn = {"comp": z + 1 - 2 * (z % 2)}
    hz = z % 2

    def remote(src, dst, send, recv, dev):
        return pltpu.make_async_remote_copy(
            src_ref=src, dst_ref=dst, send_sem=send, recv_sem=recv, device_id=dev, device_id_type=MESH)

    def same(v, send, recv, dev):
        return remote(v, v, send, recv, dev)

    x_loads = [pltpu.make_async_copy(
        x_hbm.at[:, pl.ds(s * half_dim, half_dim)], xg.at[s, pl.ds(r * block, block), :], load_sem.at[s])
        for s in range(2)]
    mu_loads = [pltpu.make_async_copy(mu_hbm.at[s], mu_all.at[s], load_sem.at[2 + s]) for s in range(2)]
    for cp in x_loads + mu_loads:
        cp.start()

    n_z = (z > 0).astype(jnp.int32) + (z < comp_size - 1).astype(jnp.int32)

    def signal_z(sem):
        @pl.when(z > 0)
        def _():
            pl.semaphore_signal(sem, inc=1, device_id={"comp": z - 1}, device_id_type=MESH)

        @pl.when(z < comp_size - 1)
        def _():
            pl.semaphore_signal(sem, inc=1, device_id={"comp": z + 1}, device_id_type=MESH)

    def signal_near(sem):
        for dev in (sib, yn):
            pl.semaphore_signal(sem, inc=1, device_id=dev, device_id_type=MESH)
        signal_z(sem)

    barrier = pltpu.get_barrier_semaphore()
    signal_near(barrier)
    pl.semaphore_wait(barrier, 2 + n_z)
    signal_near(near_sem)

    def xrows(s, blk, cid):
        return xg.at[s, pl.ds(pl.multiple_of(blk * block + cid * ch, ch), ch), :]

    def cid_y(k):
        return k + hz * (NCK - 1 - 2 * k)

    def cid_z(k):
        return k + (1 - hz) * (NCK - 1 - 2 * k)

    def y_out(j):
        return same(xrows(j // ND, r, cid_y(j % ND)), y_send.at[j // ND], y_recv.at[j], yn)

    def z_fwd(j):
        return same(xrows(j // ND, ry, cid_y(j % ND)), z_send.at[j // ND], z_recv.at[j], zn)

    def sy_fwd(j):
        return same(xrows(j // ND, ry, cid_y(j % ND)), sy_send.at[j // ND], sy_recv.at[j // ND], sib)

    def sz_fwd(j):
        return same(xrows(j // ND, ry, cid_z(j % ND)), sz_send.at[j // ND], sz_recv.at[j // ND], sib)

    def own_out(s):
        return same(xg.at[s, pl.ds(r * block, block), :], own_send.at[s], own_recv.at[s], sib)

    def y_steps(a, b):
        def body(j, _):
            y_out(j).wait_recv()
            z_fwd(j).start()
            sy_fwd(j).start()
            return 0

        lax.fori_loop(a, b, body, 0)

    def z_steps(a, b):
        def body(j, _):
            z_fwd(j).wait_recv()
            sz_fwd(j).start()
            return 0

        lax.fori_loop(a, b, body, 0)

    def half_rows(s):
        return xg.at[s, pl.ds(0, ND * ch), :]

    def sib_waits(s):
        same(half_rows(s), sy_send.at[s], sy_recv.at[s], sib).wait_recv()
        same(half_rows(s), sz_send.at[s], sz_recv.at[s], sib).wait_recv()

    def gather_sends_wait(s):
        for send, recv, dev in ((y_send, own_recv, yn), (z_send, own_recv, zn), (sy_send, own_recv, sib),
                                (sz_send, own_recv, sib)):
            same(half_rows(s), send.at[s], recv.at[s], dev).wait_send()

    x_loads[0].wait()
    for j in range(ND):
        y_out(j).start()
    own_out(0).start()
    x_loads[1].wait()
    own_out(1).start()
    for cp in mu_loads:
        cp.wait()

    def set_params(s, slot, mean, logw, t):
        mub[s, slot] = mean.astype(jnp.bfloat16)
        mu_sq = jnp.sum(mean * mean, axis=1, keepdims=True)
        col = (logw - temp_ref[t] * mu_sq) * LOG2E
        bcol[s, slot] = jnp.broadcast_to(col, (n_own, 128))
        return col

    def x_tile(s, tile):
        return xg[s, pl.ds(pl.multiple_of(tile * TP, TP), TP), :]

    def e_tile(s, slot, t, tile):
        a = dot_t(mub[s, slot], x_tile(s, tile))
        l2 = a * (temp_ref[t] * (2.0 * LOG2E)) + twice(bcol[s, slot])
        m = jnp.max(l2, axis=0, keepdims=True)
        e = jnp.exp2(l2 - m)
        return e, m, m + jnp.log(jnp.sum(e, axis=0, keepdims=True)) * LOG2E

    def tiles_of(half_id):
        return [(2 * half_id + k // bt, k % bt) for k in range(2 * bt)]

    def e_step(s, t, idx, hook=None):
        def body(i, _):
            h = (1 - c) + i * (2 * c - 1)
            for b, u in tiles_of(h):
                e, m, l = e_tile(s, r, t, b * bt + u)
                e_buf[s, b * bt + u] = e
                m_buf[s, b, u:u + 1, :] = m
                l_buf[s, b, u:u + 1, :] = l

            @pl.when(i == 0)
            def _():
                pre(idx).start()

            if hook is not None:
                hook(i)
            return 0

        lax.fori_loop(0, 2, body, 0)
        p2(idx)

    def acc_zero():
        s_acc[...] = jnp.zeros_like(s_acc)
        n_acc[...] = jnp.zeros_like(n_acc)

    def acc_tiles(s, tiles, resp_of):
        dots, ns = [], []
        for b, u in tiles:
            resp = resp_of(b, u)
            ns.append(resp[:, :128] + resp[:, 128:])
            dots.append(jnp.dot(resp.astype(jnp.bfloat16), x_tile(s, b * bt + u), preferred_element_type=jnp.float32))
        s_acc[...] += functools.reduce(jnp.add, dots)
        n_acc[...] += functools.reduce(jnp.add, ns)

    def m_step(s, t):
        idx = 2 * t + s
        acc_zero()

        def body(i, _):
            @pl.when(i == 1)
            def _():
                post(idx).wait()

            def resp_of(b, u):
                f = jnp.exp2(m_buf[s, b, u:u + 1, :] - tot_buf[idx, b, u:u + 1, :])
                return e_buf[s, b * bt + u] * f

            acc_tiles(s, tiles_of(c + i * (1 - 2 * c)), resp_of)
            return 0

        lax.fori_loop(0, 2, body, 0)

    def mr_half(s, slot, t, half_id):
        idx = 2 * t + s

        def resp_of(b, u):
            a = dot_t(mub[s, slot], x_tile(s, b * bt + u))
            return jnp.exp2(a * (temp_ref[t] * (2.0 * LOG2E)) + twice(bcol[s, slot]) - tot_buf[idx, b, u:u + 1, :])

        acc_tiles(s, tiles_of(half_id), resp_of)

    def acc_result():
        cnt = jnp.sum(n_acc[...], axis=1, keepdims=True)
        mean = s_acc[...] / (cnt + EPS_COUNT)
        logw = jnp.log((cnt + PRIOR_ALPHA) / (total_pts + total_comp * PRIOR_ALPHA))
        return mean, logw

    def half(ref, k):
        return ref.at[pl.ds(2 * k, 2)]

    def pre(idx):
        return remote(half(l_buf.at[idx % 2], 1 - c), pre_buf.at[idx], pre_send.at[idx - 2], pre_recv.at[idx - 2], sib)

    def bcast(idx, k):
        q = lax.rem(chip + k, n_chips)
        return remote(bc_src.at[idx], bc_buf.at[idx, k - 1], bc_send.at[idx - 2], bc_recv.at[idx - 2],
                      {"comp": q // y_size, "row": (q % y_size) * CORES + c})

    def post(idx):
        return same(half(tot_buf.at[idx], c), post_send.at[idx - 2], post_recv.at[idx - 2], sib)

    def p2(idx):
        pre(idx).wait()
        bc_src[idx] = lse2_parts([l_buf[idx % 2, pl.ds(2 * c, 2)], pre_buf[idx]])
        for k in range(1, n_chips):
            bcast(idx, k).start()

    def p3(idx):
        same(bc_buf.at[idx], bc_send.at[idx - 2], bc_recv.at[idx - 2], sib).wait()
        tot_buf[idx, pl.ds(2 * c, 2)] = lse2_parts([bc_src[idx]] + [bc_buf[idx, k] for k in range(n_chips - 1)])
        post(idx).start()

    def zl(s, k):
        return remote(zl_src.at[s], zl_buf.at[s, k - 1], zl_send.at[s], zl_recv.at[s],
                      {"comp": lax.rem(z + k, comp_size)})

    def ag(s, k):
        return same(tot_buf.at[s, r], ag_send.at[s], ag_recv.at[s], (sib, yn, yd)[k])

    def orig_fit(s, _):
        def orig_slots(p, _):
            for k in range(2):
                q = 2 * p + k
                off = pl.multiple_of(q * n_own, n_own)
                set_params(s, q, mu_all[s, pl.ds(off, n_own), :], row_to_col(lp_ref[pl.ds(s, 1), pl.ds(off, n_own)]), 0)
                for u in range(bt):
                    _, _, l = e_tile(s, q, 0, r * bt + u)
                    lq_buf[q, u:u + 1, :] = l

            @pl.when(jnp.logical_and(s == 0, p == 0))
            def _():
                pl.semaphore_wait(near_sem, 2 + n_z)
                signal_z(far_sem)

            @pl.when(s == 1)
            def _():
                y_steps(1 + 2 * p, 3 + 2 * p)

            return 0

        lax.fori_loop(0, row_size // 2, orig_slots, 0)
        zl_src[s] = lse2_parts([lq_buf[q] for q in range(row_size)])

        @pl.when(s == 0)
        def _():
            pl.semaphore_wait(far_sem, n_z)

        for k in range(1, comp_size):
            zl(s, k).start()

        @pl.when(s == 0)
        def _():
            y_steps(0, 1)

        return 0

    lax.fori_loop(0, 2, orig_fit, 0)

    def y_sends(a, b):
        def send(j, _):
            y_out(j).start()
            return 0

        lax.fori_loop(a, b, send, 0)

    def comb(s):
        same(zl_buf.at[s], zl_send.at[s], zl_recv.at[s], sib).wait()
        tot_buf[s, r] = lse2_parts([zl_src[s]] + [zl_buf[s, k] for k in range(comp_size - 1)])
        for k in range(3):
            ag(s, k).start()

    early = ND + 5
    y_sends(ND, early)
    y_steps(5, 6)
    comb(0)
    y_sends(early, 2 * ND)
    y_steps(6, 8)
    z_steps(0, 4)
    y_steps(8, 9)
    z_steps(4, 6)
    y_steps(9, 10)
    comb(1)
    z_steps(6, 8)
    y_steps(10, 12)

    def sweep0(s, _):
        same(tot_buf.at[s, pl.ds(0, 3)], ag_send.at[s], ag_recv.at[s], sib).wait()
        own_out(s).wait()
        acc_zero()

        @pl.when(s == 0)
        def _():
            sib_waits(0)

        def body(k, _):
            @pl.when(jnp.logical_and(s == 1, k == 1))
            def _():
                z_steps(14, 16)
                sib_waits(1)

            mr_half(s, r, 0, y + k * (1 - 2 * y))

            @pl.when(s == 0)
            def _():
                y_steps(12 + 2 * k, 14 + k)
                z_steps(8 + k, 9 + 2 * k)

            return 0

        lax.fori_loop(0, 2, body, 0)
        mean, logw = acc_result()
        set_params(s, r, mean, logw, 1)

        def hook(i):
            @pl.when(jnp.logical_and(s == 0, i == 0))
            def _():
                y_steps(15, 16)
                z_steps(11, 13)

        e_step(s, 1, 2 + s, hook)

        @pl.when(s == 0)
        def _():
            z_steps(13, 14)

        return 0

    lax.fori_loop(0, 2, sweep0, 0)

    def mx(s):
        return same(mub.at[s, r], mx_send.at[s], mx_recv.at[s], yn)

    def br(s):
        return same(brow.at[s, r], br_send.at[s], br_recv.at[s], yn)

    def mean_rows(slot, s):
        return mu_out.at[s, pl.ds(pl.multiple_of(slot * n_own, n_own), n_own), :]

    def fin(slot, s, k):
        return same(mean_rows(slot, s), fin_send.at[s, k], fin_recv.at[s, k], sib)

    def lpf(slot, k):
        return same(lp_fin.at[slot], lpf_send.at[k], lpf_recv.at[k], sib)

    def sweep(i, _):
        t, s = i // 2, i % 2
        last = t == sweeps - 1
        p3(i)
        m_step(s, t)
        mean, logw = acc_result()

        @pl.when(t < sweeps - 1)
        def _():
            col = set_params(s, r, mean, logw, t + 1)

            @pl.when(t == sweeps - 2)
            def _():
                brow[s, r] = col_to_row(col)

            e_step(s, t + 1, i + 2)

            @pl.when(t == sweeps - 2)
            def _():
                mx(s).start()
                br(s).start()

        @pl.when(last)
        def _():
            mean_rows(r, s)[...] = mean
            lp_fin[r, pl.ds(s, 1), :] = col_to_row(logw)
            fin(r, s, 0).start()
            mx(s).wait()
            br(s).wait()
            bcol[s, ry] = jnp.broadcast_to(row_to_col(brow[s, ry]), (n_own, 128))
            acc_zero()

            def body(h, _):
                mr_half(s, ry, t, h)
                return 0

            lax.fori_loop(0, 2, body, 0)
            mean2, logw2 = acc_result()
            mean_rows(ry, s)[...] = mean2
            lp_fin[ry, pl.ds(s, 1), :] = col_to_row(logw2)
            fin(ry, s, 1).start()

        return 0

    lax.fori_loop(2, 2 * sweeps, sweep, 0)
    lpf(r, 0).start()
    lpf(ry, 1).start()

    ones = jnp.ones((8, half_dim), jnp.bfloat16)

    def sq_norms(s, _):
        for u in range(bt):
            x = x_tile(s, r * bt + u).astype(jnp.float32)
            sq = x * x
            hi = sq.astype(jnp.bfloat16)
            lo = (sq - hi.astype(jnp.float32)).astype(jnp.bfloat16)
            sq_buf[s, u:u + 1, :] = (dot_t(ones, hi) + dot_t(ones, lo))[0:1]
        return 0

    lax.fori_loop(0, 2, sq_norms, 0)

    for s in range(2):
        gather_sends_wait(s)

    t = sweeps - 1
    for s in range(2):
        for j in range(bt):
            lse_out[s:s + 1, j * TP:(j + 1) * TP] = (
                tot_buf[2 * t + s, r, j:j + 1, :] * LN2 - temp_ref[t] * sq_buf[s, j:j + 1, :])

    for k in range(2):
        for s in range(2):
            fin((r, ry)[k], s, k).wait()
    lpf(r, 0).wait()
    lpf(ry, 1).wait()
    for q in range(row_size):
        lp_out[:, q * n_own:(q + 1) * n_own] = lp_fin[q]


def solution(mesh):
    comp_size = mesh.shape["comp"]
    row_size = mesh.shape["row"]

    def local_fit(x_local, mu_init, logpi_init, inv_temp):
        block, dim = x_local.shape
        half_dim = dim // 2
        n_local = mu_init.shape[1]
        n_own = n_local // row_size
        total_pts = block * row_size
        tiles = total_pts // TP
        sweeps = inv_temp.shape[0]
        n_chips = comp_size * row_size // CORES
        ni = 2 * sweeps
        bt = block // TP
        f32, bf16 = jnp.float32, jnp.bfloat16
        dma = pltpu.SemaphoreType.DMA
        vm = pltpu.VMEM
        scratch = [
            vm((2, total_pts, half_dim), bf16),
            vm((2, n_local, half_dim), f32),
            vm((2, row_size, n_own, half_dim), bf16),
            vm((2, row_size, n_own, 128), f32),
            vm((2, row_size, 1, n_own), f32),
            vm((2, tiles, n_own, TP), f32),
            vm((2, row_size, bt, TP), f32),
            vm((2, row_size, bt, TP), f32),
            vm((row_size, bt, TP), f32),
            vm((n_own, half_dim), f32),
            vm((n_own, 128), f32),
            vm((row_size, 2, n_own), f32),
            vm((2, bt, TP), f32),
            vm((2, bt, TP), f32),
            vm((2, comp_size - 1, bt, TP), f32),
            vm((ni, 2, bt, TP), f32),
            vm((ni, 2, bt, TP), f32),
            vm((ni, n_chips - 1, 2, bt, TP), f32),
            vm((ni, row_size, bt, TP), f32),
            dma((4,)), pltpu.SemaphoreType.REGULAR, pltpu.SemaphoreType.REGULAR,
            dma((2,)), dma((2 * ND,)), dma((2,)), dma((2 * ND,)), dma((2,)), dma((2,)), dma((2,)), dma((2,)),
            dma((2,)), dma((2,)), dma((2,)), dma((2,)), dma((2,)), dma((2,)),
            dma((ni - 2,)), dma((ni - 2,)), dma((ni - 2,)), dma((ni - 2,)), dma((ni - 2,)), dma((ni - 2,)),
            dma((2,)), dma((2,)), dma((2,)), dma((2,)),
            dma((2, 2)), dma((2, 2)), dma((2,)), dma((2,)),
        ]
        outs = pl.pallas_call(
            functools.partial(em_kernel, comp_size, row_size, sweeps),
            out_shape=(vm((2, n_local, half_dim), f32), vm((2, n_local), f32), vm((2, block), f32)),
            in_specs=[
                pl.BlockSpec(memory_space=pltpu.SMEM),
                pl.BlockSpec(memory_space=pltpu.VMEM),
                pl.BlockSpec(memory_space=pl.ANY),
                pl.BlockSpec(memory_space=pl.ANY),
            ],
            out_specs=(pl.BlockSpec(memory_space=pltpu.VMEM),) * 3,
            scratch_shapes=scratch,
            compiler_params=pltpu.CompilerParams(
                collective_id=0, has_side_effects=True, vmem_limit_bytes=56 * 1024 * 1024),
        )(inv_temp, logpi_init, x_local, mu_init)
        return pl.pallas_call(
            write_kernel,
            out_shape=tuple(jax.ShapeDtypeStruct(o.shape, o.dtype) for o in outs),
            in_specs=[pl.BlockSpec(memory_space=pltpu.VMEM)] * 3,
            out_specs=(pl.BlockSpec(memory_space=pl.ANY),) * 3,
            scratch_shapes=[dma((3,))],
        )(*[pltpu.with_memory_space_constraint(o, pltpu.VMEM) for o in outs])

    return jax.shard_map(
        local_fit,
        mesh=mesh,
        in_specs=(P(("grp", "row"), None), P(None, ("grp", "comp"), None), P(None, ("grp", "comp")), P()),
        out_specs=(P(None, ("grp", "comp"), None), P(None, ("grp", "comp")), P(None, ("grp", "row"))),
        check_vma=False,
    )
```

```python
import functools

import jax
import jax.numpy as jnp
from jax import lax
from jax.experimental import pallas as pl
from jax.experimental.pallas import tpu as pltpu
from jax.sharding import PartitionSpec as P

EPS_COUNT = 1e-6
PRIOR_ALPHA = 1e-3
LOG2E = 1.4426950408889634
LN2 = 0.6931471805599453
MESH = pl.DeviceIdType.MESH

CORES = 2
TP = 256
NCK = 16
ND = 8


def lse2_parts(parts):
    top = functools.reduce(jnp.maximum, parts)
    total = functools.reduce(jnp.add, [jnp.exp2(p - top) for p in parts])
    return top + jnp.log(total) * LOG2E


def dot_t(a, b):
    return lax.dot_general(a, b, (((1,), (1,)), ((), ())), preferred_element_type=jnp.float32)


def eye_mask(n):
    return lax.broadcasted_iota(jnp.int32, (n, n), 0) == lax.broadcasted_iota(jnp.int32, (n, n), 1)


def col_to_row(col):
    return jnp.sum(jnp.where(eye_mask(col.shape[0]), col, 0.0), axis=0, keepdims=True)


def row_to_col(row):
    return jnp.sum(jnp.where(eye_mask(row.shape[1]), row, 0.0), axis=1, keepdims=True)


def twice(b):
    return jnp.concatenate([b, b], axis=1)


def write_kernel(a, b, c, a_out, b_out, c_out, sems):
    copies = [pltpu.make_async_copy(v, o, sems.at[k]) for k, (v, o) in enumerate(((a, a_out), (b, b_out), (c, c_out)))]
    for cp in copies:
        cp.start()
    for cp in copies:
        cp.wait()


def em_kernel(
    comp_size, row_size, sweeps,
    temp_ref, lp_ref, x_hbm, mu_hbm,
    mu_out, lp_out, lse_out,
    xg, mu_all, mub, bcol, brow, e_buf, m_buf, l_buf, lq_buf, s_acc, n_acc, lp_fin, sq_buf,
    zl_src, zl_buf, pre_buf, bc_src, bc_buf, tot_buf,
    load_sem, near_sem, far_sem, y_send, y_recv, z_send, z_recv, sy_send, sy_recv, sz_send, sz_recv, own_send, own_recv,
    zl_send, zl_recv, ag_send, ag_recv,
    pre_send, pre_recv, bc_send, bc_recv, post_send, post_recv,
    mx_send, mx_recv, br_send, br_recv, fin_send, fin_recv, lpf_send, lpf_recv,
):
    z = lax.axis_index("comp")
    r = lax.axis_index("row")
    y, c = r // CORES, r % CORES
    n_chips = comp_size * row_size // CORES
    y_size = row_size // CORES
    chip = z * y_size + y
    block = x_hbm.shape[0]
    half_dim = x_hbm.shape[1] // 2
    total_pts = block * row_size
    n_own = mub.shape[2]
    total_comp = mu_hbm.shape[1] * comp_size
    bt = block // TP
    ch = block // NCK
    rs = y * CORES + (1 - c)
    ry = (1 - y) * CORES + c
    sib = {"row": rs}
    yn = {"row": ry}
    yd = {"row": (1 - y) * CORES + (1 - c)}
    zn = {"comp": z + 1 - 2 * (z % 2)}
    hz = z % 2

    def remote(src, dst, send, recv, dev):
        return pltpu.make_async_remote_copy(
            src_ref=src, dst_ref=dst, send_sem=send, recv_sem=recv, device_id=dev, device_id_type=MESH)

    def same(v, send, recv, dev):
        return remote(v, v, send, recv, dev)

    x_loads = [pltpu.make_async_copy(
        x_hbm.at[:, pl.ds(s * half_dim, half_dim)], xg.at[s, pl.ds(r * block, block), :], load_sem.at[s])
        for s in range(2)]
    mu_loads = [pltpu.make_async_copy(mu_hbm.at[s], mu_all.at[s], load_sem.at[2 + s]) for s in range(2)]
    for cp in x_loads:
        cp.start()

    n_z = (z > 0).astype(jnp.int32) + (z < comp_size - 1).astype(jnp.int32)

    def signal_z(sem):
        @pl.when(z > 0)
        def _():
            pl.semaphore_signal(sem, inc=1, device_id={"comp": z - 1}, device_id_type=MESH)

        @pl.when(z < comp_size - 1)
        def _():
            pl.semaphore_signal(sem, inc=1, device_id={"comp": z + 1}, device_id_type=MESH)

    def signal_near(sem):
        for dev in (sib, yn):
            pl.semaphore_signal(sem, inc=1, device_id=dev, device_id_type=MESH)
        signal_z(sem)

    barrier = pltpu.get_barrier_semaphore()
    signal_near(barrier)
    pl.semaphore_wait(barrier, 2 + n_z)
    signal_near(near_sem)
    for cp in mu_loads:
        cp.start()

    def xrows(s, blk, cid):
        return xg.at[s, pl.ds(pl.multiple_of(blk * block + cid * ch, ch), ch), :]

    def cid_y(k):
        return k + hz * (NCK - 1 - 2 * k)

    def cid_z(k):
        return k + (1 - hz) * (NCK - 1 - 2 * k)

    def y_out(j):
        return same(xrows(j // ND, r, cid_y(j % ND)), y_send.at[j // ND], y_recv.at[j], yn)

    def z_fwd(j):
        return same(xrows(j // ND, ry, cid_y(j % ND)), z_send.at[j // ND], z_recv.at[j], zn)

    def sy_fwd(j):
        return same(xrows(j // ND, ry, cid_y(j % ND)), sy_send.at[j // ND], sy_recv.at[j // ND], sib)

    def sz_fwd(j):
        return same(xrows(j // ND, ry, cid_z(j % ND)), sz_send.at[j // ND], sz_recv.at[j // ND], sib)

    def own_out(s):
        return same(xg.at[s, pl.ds(r * block, block), :], own_send.at[s], own_recv.at[s], sib)

    def y_steps(a, b):
        def body(j, _):
            y_out(j).wait_recv()
            z_fwd(j).start()
            sy_fwd(j).start()
            return 0

        lax.fori_loop(a, b, body, 0)

    def z_steps(a, b):
        def body(j, _):
            z_fwd(j).wait_recv()
            sz_fwd(j).start()
            return 0

        lax.fori_loop(a, b, body, 0)

    def half_rows(s):
        return xg.at[s, pl.ds(0, ND * ch), :]

    def sib_waits(s):
        same(half_rows(s), sy_send.at[s], sy_recv.at[s], sib).wait_recv()
        same(half_rows(s), sz_send.at[s], sz_recv.at[s], sib).wait_recv()

    def gather_sends_wait(s):
        for send, recv, dev in ((y_send, own_recv, yn), (z_send, own_recv, zn), (sy_send, own_recv, sib),
                                (sz_send, own_recv, sib)):
            same(half_rows(s), send.at[s], recv.at[s], dev).wait_send()

    x_loads[0].wait()
    for j in range(ND):
        y_out(j).start()
    own_out(0).start()
    x_loads[1].wait()
    own_out(1).start()
    for cp in mu_loads:
        cp.wait()

    def set_params(s, slot, mean, logw, t):
        mub[s, slot] = mean.astype(jnp.bfloat16)
        mu_sq = jnp.sum(mean * mean, axis=1, keepdims=True)
        col = (logw - temp_ref[t] * mu_sq) * LOG2E
        bcol[s, slot] = jnp.broadcast_to(col, (n_own, 128))
        return col

    def x_tile(s, tile):
        return xg[s, pl.ds(pl.multiple_of(tile * TP, TP), TP), :]

    def e_tile(s, slot, t, tile):
        a = dot_t(mub[s, slot], x_tile(s, tile))
        l2 = a * (temp_ref[t] * (2.0 * LOG2E)) + twice(bcol[s, slot])
        m = jnp.max(l2, axis=0, keepdims=True)
        e = jnp.exp2(l2 - m)
        return e, m, m + jnp.log(jnp.sum(e, axis=0, keepdims=True)) * LOG2E

    def tiles_of(half_id):
        return [(2 * half_id + k // bt, k % bt) for k in range(2 * bt)]

    def e_step(s, t, idx, hook=None):
        def body(i, _):
            h = (1 - c) + i * (2 * c - 1)
            for b, u in tiles_of(h):
                e, m, l = e_tile(s, r, t, b * bt + u)
                e_buf[s, b * bt + u] = e
                m_buf[s, b, u:u + 1, :] = m
                l_buf[s, b, u:u + 1, :] = l

            @pl.when(i == 0)
            def _():
                pre(idx).start()

            if hook is not None:
                hook(i)
            return 0

        lax.fori_loop(0, 2, body, 0)
        p2(idx)

    def acc_zero():
        s_acc[...] = jnp.zeros_like(s_acc)
        n_acc[...] = jnp.zeros_like(n_acc)

    def acc_tiles(s, tiles, resp_of):
        dots, ns = [], []
        for b, u in tiles:
            resp = resp_of(b, u)
            ns.append(resp[:, :128] + resp[:, 128:])
            dots.append(jnp.dot(resp.astype(jnp.bfloat16), x_tile(s, b * bt + u), preferred_element_type=jnp.float32))
        s_acc[...] += functools.reduce(jnp.add, dots)
        n_acc[...] += functools.reduce(jnp.add, ns)

    def m_step(s, t):
        idx = 2 * t + s
        acc_zero()

        def body(i, _):
            @pl.when(i == 1)
            def _():
                post(idx).wait()

            def resp_of(b, u):
                f = jnp.exp2(m_buf[s, b, u:u + 1, :] - tot_buf[idx, b, u:u + 1, :])
                return e_buf[s, b * bt + u] * f

            acc_tiles(s, tiles_of(c + i * (1 - 2 * c)), resp_of)
            return 0

        lax.fori_loop(0, 2, body, 0)

    def mr_half(s, slot, t, half_id):
        idx = 2 * t + s

        def resp_of(b, u):
            a = dot_t(mub[s, slot], x_tile(s, b * bt + u))
            return jnp.exp2(a * (temp_ref[t] * (2.0 * LOG2E)) + twice(bcol[s, slot]) - tot_buf[idx, b, u:u + 1, :])

        acc_tiles(s, tiles_of(half_id), resp_of)

    def mr_all(s, slot, t):
        for h in range(2):
            mr_half(s, slot, t, h)

    def acc_result():
        cnt = jnp.sum(n_acc[...], axis=1, keepdims=True)
        mean = s_acc[...] / (cnt + EPS_COUNT)
        logw = jnp.log((cnt + PRIOR_ALPHA) / (total_pts + total_comp * PRIOR_ALPHA))
        return mean, logw

    def half(ref, k):
        return ref.at[pl.ds(2 * k, 2)]

    def pre(idx):
        return remote(half(l_buf.at[idx % 2], 1 - c), pre_buf.at[idx], pre_send.at[idx - 2], pre_recv.at[idx - 2], sib)

    def bcast(idx, k):
        q = lax.rem(chip + k, n_chips)
        return remote(bc_src.at[idx], bc_buf.at[idx, k - 1], bc_send.at[idx - 2], bc_recv.at[idx - 2],
                      {"comp": q // y_size, "row": (q % y_size) * CORES + c})

    def post(idx):
        return same(half(tot_buf.at[idx], c), post_send.at[idx - 2], post_recv.at[idx - 2], sib)

    def p2(idx):
        pre(idx).wait()
        bc_src[idx] = lse2_parts([l_buf[idx % 2, pl.ds(2 * c, 2)], pre_buf[idx]])
        for k in range(1, n_chips):
            bcast(idx, k).start()

    def p3(idx):
        same(bc_buf.at[idx], bc_send.at[idx - 2], bc_recv.at[idx - 2], sib).wait()
        tot_buf[idx, pl.ds(2 * c, 2)] = lse2_parts([bc_src[idx]] + [bc_buf[idx, k] for k in range(n_chips - 1)])
        post(idx).start()

    def zl(s, k):
        return remote(zl_src.at[s], zl_buf.at[s, k - 1], zl_send.at[s], zl_recv.at[s],
                      {"comp": lax.rem(z + k, comp_size)})

    def ag(s, k):
        return same(tot_buf.at[s, r], ag_send.at[s], ag_recv.at[s], (sib, yn, yd)[k])

    def orig_fit(s, _):
        def orig_slots(p, _):
            for k in range(2):
                q = 2 * p + k
                off = pl.multiple_of(q * n_own, n_own)
                set_params(s, q, mu_all[s, pl.ds(off, n_own), :], row_to_col(lp_ref[pl.ds(s, 1), pl.ds(off, n_own)]), 0)
                for u in range(bt):
                    _, _, l = e_tile(s, q, 0, r * bt + u)
                    lq_buf[q, u:u + 1, :] = l

            @pl.when(jnp.logical_and(s == 0, p == 0))
            def _():
                pl.semaphore_wait(near_sem, 2 + n_z)
                signal_z(far_sem)

            @pl.when(s == 1)
            def _():
                y_steps(1 + 2 * p, 3 + 2 * p)

            return 0

        lax.fori_loop(0, row_size // 2, orig_slots, 0)
        zl_src[s] = lse2_parts([lq_buf[q] for q in range(row_size)])

        @pl.when(s == 0)
        def _():
            pl.semaphore_wait(far_sem, n_z)

        for k in range(1, comp_size):
            zl(s, k).start()

        @pl.when(s == 0)
        def _():
            y_steps(0, 1)

        return 0

    lax.fori_loop(0, 2, orig_fit, 0)

    def y_sends(a, b):
        def send(j, _):
            y_out(j).start()
            return 0

        lax.fori_loop(a, b, send, 0)

    def comb(s):
        same(zl_buf.at[s], zl_send.at[s], zl_recv.at[s], sib).wait()
        tot_buf[s, r] = lse2_parts([zl_src[s]] + [zl_buf[s, k] for k in range(comp_size - 1)])
        for k in range(3):
            ag(s, k).start()

    early = ND + 3
    y_sends(ND, early)
    y_steps(5, 6)
    comb(0)
    y_sends(early, 2 * ND)
    y_steps(6, 8)
    z_steps(0, 4)
    y_steps(8, 9)
    z_steps(4, 6)
    y_steps(9, 10)
    comb(1)
    z_steps(6, 8)
    y_steps(10, 12)

    ones = jnp.ones((8, half_dim), jnp.bfloat16)

    def sq_norms(s, _):
        for u in range(bt):
            x = x_tile(s, r * bt + u).astype(jnp.float32)
            sq = x * x
            hi = sq.astype(jnp.bfloat16)
            lo = (sq - hi.astype(jnp.float32)).astype(jnp.bfloat16)
            sq_buf[s, u:u + 1, :] = (dot_t(ones, hi) + dot_t(ones, lo))[0:1]
        return 0

    def sweep0(s, _):
        same(tot_buf.at[s, pl.ds(0, 3)], ag_send.at[s], ag_recv.at[s], sib).wait()
        own_out(s).wait()
        acc_zero()

        @pl.when(s == 0)
        def _():
            sib_waits(0)
            y_steps(12, 14)

        def body(k, _):
            @pl.when(jnp.logical_and(s == 1, k == 1))
            def _():
                z_steps(15, 16)
                lax.fori_loop(0, 2, sq_norms, 0)
                sib_waits(1)

            mr_half(s, r, 0, y + k * (1 - 2 * y))

            @pl.when(s == 0)
            def _():
                y_steps(14 + k, 15 + k)
                z_steps(8 + 2 * k, 10 + k)

            return 0

        lax.fori_loop(0, 2, body, 0)
        mean, logw = acc_result()
        set_params(s, r, mean, logw, 1)

        def hook(i):
            @pl.when(jnp.logical_and(s == 0, i == 0))
            def _():
                z_steps(11, 13)

        e_step(s, 1, 2 + s, hook)

        @pl.when(s == 0)
        def _():
            z_steps(13, 15)

        return 0

    lax.fori_loop(0, 2, sweep0, 0)

    def mx(s):
        return same(mub.at[s, r], mx_send.at[s], mx_recv.at[s], yn)

    def br(s):
        return same(brow.at[s, r], br_send.at[s], br_recv.at[s], yn)

    def mean_rows(slot, s):
        return mu_out.at[s, pl.ds(pl.multiple_of(slot * n_own, n_own), n_own), :]

    def fin(slot, s, k):
        return same(mean_rows(slot, s), fin_send.at[s, k], fin_recv.at[s, k], sib)

    def lpf(slot, k):
        return same(lp_fin.at[slot], lpf_send.at[k], lpf_recv.at[k], sib)

    def sweep(i, _):
        t, s = i // 2, i % 2
        last = t == sweeps - 1
        p3(i)
        m_step(s, t)
        mean, logw = acc_result()

        @pl.when(t < sweeps - 1)
        def _():
            col = set_params(s, r, mean, logw, t + 1)

            @pl.when(t == sweeps - 2)
            def _():
                brow[s, r] = col_to_row(col)

            e_step(s, t + 1, i + 2)

            @pl.when(t == sweeps - 2)
            def _():
                mx(s).start()
                br(s).start()

        @pl.when(last)
        def _():
            mean_rows(r, s)[...] = mean
            lp_fin[r, pl.ds(s, 1), :] = col_to_row(logw)
            fin(r, s, 0).start()
            mx(s).wait()
            br(s).wait()
            bcol[s, ry] = jnp.broadcast_to(row_to_col(brow[s, ry]), (n_own, 128))
            acc_zero()

            mr_all(s, ry, t)
            mean2, logw2 = acc_result()
            mean_rows(ry, s)[...] = mean2
            lp_fin[ry, pl.ds(s, 1), :] = col_to_row(logw2)
            fin(ry, s, 1).start()

        return 0

    lax.fori_loop(2, 2 * sweeps, sweep, 0)
    lpf(r, 0).start()
    lpf(ry, 1).start()

    for s in range(2):
        gather_sends_wait(s)

    t = sweeps - 1
    for s in range(2):
        for j in range(bt):
            lse_out[s:s + 1, j * TP:(j + 1) * TP] = (
                tot_buf[2 * t + s, r, j:j + 1, :] * LN2 - temp_ref[t] * sq_buf[s, j:j + 1, :])

    for k in range(2):
        for s in range(2):
            fin((r, ry)[k], s, k).wait()
    lpf(r, 0).wait()
    lpf(ry, 1).wait()
    for q in range(row_size):
        lp_out[:, q * n_own:(q + 1) * n_own] = lp_fin[q]


def solution(mesh):
    comp_size = mesh.shape["comp"]
    row_size = mesh.shape["row"]

    def local_fit(x_local, mu_init, logpi_init, inv_temp):
        block, dim = x_local.shape
        half_dim = dim // 2
        n_local = mu_init.shape[1]
        n_own = n_local // row_size
        total_pts = block * row_size
        tiles = total_pts // TP
        sweeps = inv_temp.shape[0]
        n_chips = comp_size * row_size // CORES
        ni = 2 * sweeps
        bt = block // TP
        f32, bf16 = jnp.float32, jnp.bfloat16
        dma = pltpu.SemaphoreType.DMA
        vm = pltpu.VMEM
        scratch = [
            vm((2, total_pts, half_dim), bf16),
            vm((2, n_local, half_dim), f32),
            vm((2, row_size, n_own, half_dim), bf16),
            vm((2, row_size, n_own, 128), f32),
            vm((2, row_size, 1, n_own), f32),
            vm((2, tiles, n_own, TP), f32),
            vm((2, row_size, bt, TP), f32),
            vm((2, row_size, bt, TP), f32),
            vm((row_size, bt, TP), f32),
            vm((n_own, half_dim), f32),
            vm((n_own, 128), f32),
            vm((row_size, 2, n_own), f32),
            vm((2, bt, TP), f32),
            vm((2, bt, TP), f32),
            vm((2, comp_size - 1, bt, TP), f32),
            vm((ni, 2, bt, TP), f32),
            vm((ni, 2, bt, TP), f32),
            vm((ni, n_chips - 1, 2, bt, TP), f32),
            vm((ni, row_size, bt, TP), f32),
            dma((4,)), pltpu.SemaphoreType.REGULAR, pltpu.SemaphoreType.REGULAR,
            dma((2,)), dma((2 * ND,)), dma((2,)), dma((2 * ND,)), dma((2,)), dma((2,)), dma((2,)), dma((2,)),
            dma((2,)), dma((2,)), dma((2,)), dma((2,)), dma((2,)), dma((2,)),
            dma((ni - 2,)), dma((ni - 2,)), dma((ni - 2,)), dma((ni - 2,)), dma((ni - 2,)), dma((ni - 2,)),
            dma((2,)), dma((2,)), dma((2,)), dma((2,)),
            dma((2, 2)), dma((2, 2)), dma((2,)), dma((2,)),
        ]
        outs = pl.pallas_call(
            functools.partial(em_kernel, comp_size, row_size, sweeps),
            out_shape=(vm((2, n_local, half_dim), f32), vm((2, n_local), f32), vm((2, block), f32)),
            in_specs=[
                pl.BlockSpec(memory_space=pltpu.SMEM),
                pl.BlockSpec(memory_space=pltpu.VMEM),
                pl.BlockSpec(memory_space=pl.ANY),
                pl.BlockSpec(memory_space=pl.ANY),
            ],
            out_specs=(pl.BlockSpec(memory_space=pltpu.VMEM),) * 3,
            scratch_shapes=scratch,
            compiler_params=pltpu.CompilerParams(
                collective_id=0, has_side_effects=True, vmem_limit_bytes=56 * 1024 * 1024),
        )(inv_temp, logpi_init, x_local, mu_init)
        return pl.pallas_call(
            write_kernel,
            out_shape=tuple(jax.ShapeDtypeStruct(o.shape, o.dtype) for o in outs),
            in_specs=[pl.BlockSpec(memory_space=pltpu.VMEM)] * 3,
            out_specs=(pl.BlockSpec(memory_space=pl.ANY),) * 3,
            scratch_shapes=[dma((3,))],
        )(*[pltpu.with_memory_space_constraint(o, pltpu.VMEM) for o in outs])

    return jax.shard_map(
        local_fit,
        mesh=mesh,
        in_specs=(P(("grp", "row"), None), P(None, ("grp", "comp"), None), P(None, ("grp", "comp")), P()),
        out_specs=(P(None, ("grp", "comp"), None), P(None, ("grp", "comp")), P(None, ("grp", "row"))),
        check_vma=False,
    )
```

```python
import functools

import jax
import jax.numpy as jnp
from jax import lax
from jax.experimental import pallas as pl
from jax.experimental.pallas import tpu as pltpu
from jax.sharding import PartitionSpec as P

EPS_COUNT = 1e-6
PRIOR_ALPHA = 1e-3
LOG2E = 1.4426950408889634
LN2 = 0.6931471805599453
MESH = pl.DeviceIdType.MESH

CORES = 2
TP = 256
NCK = 16
ND = 8


def lse2_parts(parts):
    top = functools.reduce(jnp.maximum, parts)
    total = functools.reduce(jnp.add, [jnp.exp2(p - top) for p in parts])
    return top + jnp.log(total) * LOG2E


def dot_t(a, b):
    return lax.dot_general(a, b, (((1,), (1,)), ((), ())), preferred_element_type=jnp.float32)


def eye_mask(n):
    return lax.broadcasted_iota(jnp.int32, (n, n), 0) == lax.broadcasted_iota(jnp.int32, (n, n), 1)


def col_to_row(col):
    return jnp.sum(jnp.where(eye_mask(col.shape[0]), col, 0.0), axis=0, keepdims=True)


def row_to_col(row):
    return jnp.sum(jnp.where(eye_mask(row.shape[1]), row, 0.0), axis=1, keepdims=True)


def twice(b):
    return jnp.concatenate([b, b], axis=1)


def write_kernel(a, b, c, a_out, b_out, c_out, sems):
    copies = [pltpu.make_async_copy(v, o, sems.at[k]) for k, (v, o) in enumerate(((a, a_out), (b, b_out), (c, c_out)))]
    for cp in copies:
        cp.start()
    for cp in copies:
        cp.wait()


def em_kernel(
    comp_size, row_size, sweeps,
    temp_hbm, lp_hbm, x_hbm, mu_hbm,
    mu_out, lp_out, lse_out,
    temp_ref, lp_ref, xg, mu_all, mub, bcol, brow, e_buf, m_buf, l_buf, lq_buf, s_acc, n_acc, lp_fin, sq_buf,
    zl_src, zl_buf, pre_buf, bc_src, bc_buf, tot_buf,
    load_sem, near_sem, far_sem, g_send, y_recv, z_recv, sy_recv, sz_recv, own_recv,
    zl_send, zl_recv, ag_send, ag_recv,
    pre_send, pre_recv, bc_send, bc_recv, post_send, post_recv,
    mx_send, mx_recv, br_send, br_recv, fin_send, fin_recv, lpf_send, lpf_recv,
):
    z = lax.axis_index("comp")
    r = lax.axis_index("row")
    y, c = r // CORES, r % CORES
    n_chips = comp_size * row_size // CORES
    y_size = row_size // CORES
    chip = z * y_size + y
    block = x_hbm.shape[0]
    half_dim = x_hbm.shape[1] // 2
    total_pts = block * row_size
    n_own = mub.shape[2]
    total_comp = mu_hbm.shape[1] * comp_size
    bt = block // TP
    ch = block // NCK
    rs = y * CORES + (1 - c)
    ry = (1 - y) * CORES + c
    sib = {"row": rs}
    yn = {"row": ry}
    yd = {"row": (1 - y) * CORES + (1 - c)}
    zn = {"comp": z + 1 - 2 * (z % 2)}
    hz = z % 2

    def remote(src, dst, send, recv, dev):
        return pltpu.make_async_remote_copy(
            src_ref=src, dst_ref=dst, send_sem=send, recv_sem=recv, device_id=dev, device_id_type=MESH)

    def same(v, send, recv, dev):
        return remote(v, v, send, recv, dev)

    x_loads = [pltpu.make_async_copy(
        x_hbm.at[:, pl.ds(s * half_dim, half_dim)], xg.at[s, pl.ds(r * block, block), :], load_sem.at[s])
        for s in range(2)]
    mu_loads = [pltpu.make_async_copy(mu_hbm.at[s], mu_all.at[s], load_sem.at[2 + s]) for s in range(2)]
    small_loads = [pltpu.make_async_copy(temp_hbm, temp_ref, load_sem.at[4]),
                   pltpu.make_async_copy(lp_hbm, lp_ref, load_sem.at[5])]
    for cp in x_loads + small_loads:
        cp.start()

    n_z = (z > 0).astype(jnp.int32) + (z < comp_size - 1).astype(jnp.int32)

    def signal_z(sem):
        @pl.when(z > 0)
        def _():
            pl.semaphore_signal(sem, inc=1, device_id={"comp": z - 1}, device_id_type=MESH)

        @pl.when(z < comp_size - 1)
        def _():
            pl.semaphore_signal(sem, inc=1, device_id={"comp": z + 1}, device_id_type=MESH)

    def signal_near(sem):
        for dev in (sib, yn):
            pl.semaphore_signal(sem, inc=1, device_id=dev, device_id_type=MESH)
        signal_z(sem)

    barrier = pltpu.get_barrier_semaphore()
    signal_near(barrier)
    pl.semaphore_wait(barrier, 2 + n_z)
    signal_near(near_sem)
    for cp in mu_loads:
        cp.start()

    def xrows(s, blk, cid):
        return xg.at[s, pl.ds(pl.multiple_of(blk * block + cid * ch, ch), ch), :]

    def cid_y(k):
        return k + hz * (NCK - 1 - 2 * k)

    def cid_z(k):
        return k + (1 - hz) * (NCK - 1 - 2 * k)

    def y_out(j):
        return same(xrows(j // ND, r, cid_y(j % ND)), g_send.at[0], y_recv.at[j], yn)

    def z_fwd(j):
        return same(xrows(j // ND, ry, cid_y(j % ND)), g_send.at[0], z_recv.at[j], zn)

    def sy_fwd(j):
        return same(xrows(j // ND, ry, cid_y(j % ND)), g_send.at[0], sy_recv.at[j // ND], sib)

    def sz_fwd(j):
        return same(xrows(j // ND, ry, cid_z(j % ND)), g_send.at[0], sz_recv.at[j // ND], sib)

    def own_out(s):
        return same(xg.at[s, pl.ds(r * block, block), :], g_send.at[0], own_recv.at[s], sib)

    def y_steps(a, b):
        def body(j, _):
            y_out(j).wait_recv()
            z_fwd(j).start()
            sy_fwd(j).start()
            return 0

        lax.fori_loop(a, b, body, 0)

    def z_steps(a, b):
        def body(j, _):
            z_fwd(j).wait_recv()
            sz_fwd(j).start()
            return 0

        lax.fori_loop(a, b, body, 0)

    def half_rows(s):
        return xg.at[s, pl.ds(0, ND * ch), :]

    def sib_waits(s):
        same(half_rows(s), g_send.at[0], sy_recv.at[s], sib).wait_recv()
        same(half_rows(s), g_send.at[0], sz_recv.at[s], sib).wait_recv()

    def gather_sends_wait(s):
        for _ in range(4):
            same(half_rows(s), g_send.at[0], sy_recv.at[s], sib).wait_send()
        own_out(s).wait_send()

    x_loads[0].wait()
    for j in range(ND):
        y_out(j).start()
    own_out(0).start()
    x_loads[1].wait()
    own_out(1).start()
    for cp in mu_loads + small_loads:
        cp.wait()

    def set_params(s, slot, mean, logw, t):
        mub[s, slot] = mean.astype(jnp.bfloat16)
        mu_sq = jnp.sum(mean * mean, axis=1, keepdims=True)
        col = (logw - temp_ref[t] * mu_sq) * LOG2E
        bcol[s, slot] = jnp.broadcast_to(col, (n_own, 128))
        return col

    def x_tile(s, tile):
        return xg[s, pl.ds(pl.multiple_of(tile * TP, TP), TP), :]

    def e_tile(s, slot, t, tile):
        a = dot_t(mub[s, slot], x_tile(s, tile))
        l2 = a * (temp_ref[t] * (2.0 * LOG2E)) + twice(bcol[s, slot])
        m = jnp.max(l2, axis=0, keepdims=True)
        e = jnp.exp2(l2 - m)
        return e, m, m + jnp.log(jnp.sum(e, axis=0, keepdims=True)) * LOG2E

    def tiles_of(half_id):
        return [(2 * half_id + k // bt, k % bt) for k in range(2 * bt)]

    def e_step(s, t, idx, hook=None):
        def body(i, _):
            h = (1 - c) + i * (2 * c - 1)
            for b, u in tiles_of(h):
                e, m, l = e_tile(s, r, t, b * bt + u)
                e_buf[s, b * bt + u] = e
                m_buf[s, b, u:u + 1, :] = m
                l_buf[s, b, u:u + 1, :] = l

            @pl.when(i == 0)
            def _():
                pre(idx).start()

            if hook is not None:
                hook(i)
            return 0

        lax.fori_loop(0, 2, body, 0)
        p2(idx)

    def acc_zero():
        s_acc[...] = jnp.zeros_like(s_acc)
        n_acc[...] = jnp.zeros_like(n_acc)

    def acc_tiles(s, tiles, resp_of):
        dots, ns = [], []
        for b, u in tiles:
            resp = resp_of(b, u)
            ns.append(resp[:, :128] + resp[:, 128:])
            dots.append(jnp.dot(resp.astype(jnp.bfloat16), x_tile(s, b * bt + u), preferred_element_type=jnp.float32))
        s_acc[...] += functools.reduce(jnp.add, dots)
        n_acc[...] += functools.reduce(jnp.add, ns)

    def m_step(s, t):
        idx = 2 * t + s
        acc_zero()

        def body(i, _):
            @pl.when(i == 1)
            def _():
                post(idx).wait()

            def resp_of(b, u):
                f = jnp.exp2(m_buf[s, b, u:u + 1, :] - tot_buf[idx, b, u:u + 1, :])
                return e_buf[s, b * bt + u] * f

            acc_tiles(s, tiles_of(c + i * (1 - 2 * c)), resp_of)
            return 0

        lax.fori_loop(0, 2, body, 0)

    def mr_half(s, slot, t, half_id):
        idx = 2 * t + s

        def resp_of(b, u):
            a = dot_t(mub[s, slot], x_tile(s, b * bt + u))
            return jnp.exp2(a * (temp_ref[t] * (2.0 * LOG2E)) + twice(bcol[s, slot]) - tot_buf[idx, b, u:u + 1, :])

        acc_tiles(s, tiles_of(half_id), resp_of)

    def mr_all(s, slot, t):
        for h in range(2):
            mr_half(s, slot, t, h)

    def acc_result():
        cnt = jnp.sum(n_acc[...], axis=1, keepdims=True)
        mean = s_acc[...] * (1.0 / (cnt + EPS_COUNT))
        logw = jnp.log((cnt + PRIOR_ALPHA) / (total_pts + total_comp * PRIOR_ALPHA))
        return mean, logw

    def half(ref, k):
        return ref.at[pl.ds(2 * k, 2)]

    def pre(idx):
        return remote(half(l_buf.at[idx % 2], 1 - c), pre_buf.at[idx], pre_send.at[idx - 2], pre_recv.at[idx - 2], sib)

    def bcast(idx, j):
        k = jnp.where(z < comp_size // 2, n_chips - j, j)
        q = lax.rem(chip + k, n_chips)
        return remote(bc_src.at[idx], bc_buf.at[idx, k - 1], bc_send.at[idx - 2], bc_recv.at[idx - 2],
                      {"comp": q // y_size, "row": (q % y_size) * CORES + c})

    def post(idx):
        return same(half(tot_buf.at[idx], c), post_send.at[idx - 2], post_recv.at[idx - 2], sib)

    def p2(idx):
        pre(idx).wait()
        bc_src[idx] = lse2_parts([l_buf[idx % 2, pl.ds(2 * c, 2)], pre_buf[idx]])
        for k in range(1, n_chips):
            bcast(idx, k).start()

    def p3(idx):
        same(bc_buf.at[idx], bc_send.at[idx - 2], bc_recv.at[idx - 2], sib).wait()
        tot_buf[idx, pl.ds(2 * c, 2)] = lse2_parts([bc_src[idx]] + [bc_buf[idx, k] for k in range(n_chips - 1)])
        post(idx).start()

    def zl(s, k):
        return remote(zl_src.at[s], zl_buf.at[s, k - 1], zl_send.at[s], zl_recv.at[s],
                      {"comp": lax.rem(z + k, comp_size)})

    def ag(s, k):
        return same(tot_buf.at[s, r], ag_send.at[s], ag_recv.at[s], (sib, yn, yd)[k])

    def orig_fit(s, _):
        def orig_slots(p, _):
            for k in range(2):
                q = 2 * p + k
                off = pl.multiple_of(q * n_own, n_own)
                set_params(s, q, mu_all[s, pl.ds(off, n_own), :], row_to_col(lp_ref[pl.ds(s, 1), pl.ds(off, n_own)]), 0)
                for u in range(bt):
                    _, _, l = e_tile(s, q, 0, r * bt + u)
                    lq_buf[q, u:u + 1, :] = l

            @pl.when(jnp.logical_and(s == 0, p == 0))
            def _():
                pl.semaphore_wait(near_sem, 2 + n_z)
                signal_z(far_sem)

            @pl.when(s == 1)
            def _():
                y_steps(1 + 2 * p, 3 + 2 * p)

            return 0

        lax.fori_loop(0, row_size // 2, orig_slots, 0)
        zl_src[s] = lse2_parts([lq_buf[q] for q in range(row_size)])

        @pl.when(s == 0)
        def _():
            pl.semaphore_wait(far_sem, n_z)

        for k in range(1, comp_size):
            zl(s, k).start()

        @pl.when(s == 0)
        def _():
            y_steps(0, 1)

        return 0

    lax.fori_loop(0, 2, orig_fit, 0)

    def y_sends(a, b):
        def send(j, _):
            y_out(j).start()
            return 0

        lax.fori_loop(a, b, send, 0)

    def comb(s):
        same(zl_buf.at[s], zl_send.at[s], zl_recv.at[s], sib).wait()
        tot_buf[s, r] = lse2_parts([zl_src[s]] + [zl_buf[s, k] for k in range(comp_size - 1)])
        for k in range(3):
            ag(s, k).start()

    early = ND + 3
    y_sends(ND, early)
    y_steps(5, 6)
    comb(0)
    y_sends(early, 2 * ND)
    y_steps(6, 8)
    z_steps(0, 4)
    y_steps(8, 9)
    z_steps(4, 6)
    y_steps(9, 10)
    comb(1)
    z_steps(6, 8)
    y_steps(10, 12)

    ones = jnp.ones((8, half_dim), jnp.bfloat16)

    def sq_norms(s, _):
        for u in range(bt):
            x = x_tile(s, r * bt + u).astype(jnp.float32)
            sq = x * x
            hi = sq.astype(jnp.bfloat16)
            lo = (sq - hi.astype(jnp.float32)).astype(jnp.bfloat16)
            sq_buf[s, u:u + 1, :] = (dot_t(ones, hi) + dot_t(ones, lo))[0:1]
        return 0

    def sweep0(s, _):
        same(tot_buf.at[s, pl.ds(0, 3)], ag_send.at[s], ag_recv.at[s], sib).wait()
        own_out(s).wait_recv()
        acc_zero()

        @pl.when(s == 0)
        def _():
            sib_waits(0)
            y_steps(12, 15)

        def body(k, _):
            @pl.when(jnp.logical_and(s == 1, k == 1))
            def _():
                lax.fori_loop(0, 2, sq_norms, 0)
                sib_waits(1)

            mr_half(s, r, 0, y + k * (1 - 2 * y))

            @pl.when(s == 0)
            def _():
                y_steps(15, 16 - k)
                z_steps(8 + 3 * k, 11 + 2 * k)

            return 0

        lax.fori_loop(0, 2, body, 0)
        mean, logw = acc_result()
        set_params(s, r, mean, logw, 1)

        def hook(i):
            @pl.when(jnp.logical_and(s == 0, i == 0))
            def _():
                z_steps(13, 15)

        e_step(s, 1, 2 + s, hook)

        @pl.when(s == 0)
        def _():
            z_steps(15, 16)

        return 0

    lax.fori_loop(0, 2, sweep0, 0)

    def mx(s):
        return same(mub.at[s, r], mx_send.at[s], mx_recv.at[s], yn)

    def br(s):
        return same(brow.at[s, r], br_send.at[s], br_recv.at[s], yn)

    def mean_rows(slot, s):
        return mu_out.at[s, pl.ds(pl.multiple_of(slot * n_own, n_own), n_own), :]

    def fin(slot, s, k):
        return same(mean_rows(slot, s), fin_send.at[s, k], fin_recv.at[s, k], sib)

    def lpf(slot, k):
        return same(lp_fin.at[slot], lpf_send.at[k], lpf_recv.at[k], sib)

    def sweep(i, _):
        t, s = i // 2, i % 2
        last = t == sweeps - 1
        p3(i)
        m_step(s, t)
        mean, logw = acc_result()

        @pl.when(t < sweeps - 1)
        def _():
            col = set_params(s, r, mean, logw, t + 1)

            @pl.when(t == sweeps - 2)
            def _():
                brow[s, r] = col_to_row(col)

            e_step(s, t + 1, i + 2)

            @pl.when(t == sweeps - 2)
            def _():
                mx(s).start()
                br(s).start()

        @pl.when(last)
        def _():
            mean_rows(r, s)[...] = mean
            lp_fin[r, pl.ds(s, 1), :] = col_to_row(logw)
            fin(r, s, 0).start()
            mx(s).wait()
            br(s).wait()
            bcol[s, ry] = jnp.broadcast_to(row_to_col(brow[s, ry]), (n_own, 128))
            acc_zero()

            mr_all(s, ry, t)
            mean2, logw2 = acc_result()
            mean_rows(ry, s)[...] = mean2
            lp_fin[ry, pl.ds(s, 1), :] = col_to_row(logw2)
            fin(ry, s, 1).start()

        return 0

    lax.fori_loop(2, 2 * sweeps, sweep, 0)
    lpf(r, 0).start()
    lpf(ry, 1).start()

    for s in range(2):
        gather_sends_wait(s)

    t = sweeps - 1
    for s in range(2):
        for j in range(bt):
            lse_out[s:s + 1, j * TP:(j + 1) * TP] = (
                tot_buf[2 * t + s, r, j:j + 1, :] * LN2 - temp_ref[t] * sq_buf[s, j:j + 1, :])

    for k in range(2):
        for s in range(2):
            fin((r, ry)[k], s, k).wait()
    lpf(r, 0).wait()
    lpf(ry, 1).wait()
    for q in range(row_size):
        lp_out[:, q * n_own:(q + 1) * n_own] = lp_fin[q]


def solution(mesh):
    comp_size = mesh.shape["comp"]
    row_size = mesh.shape["row"]

    def local_fit(x_local, mu_init, logpi_init, inv_temp):
        block, dim = x_local.shape
        half_dim = dim // 2
        n_local = mu_init.shape[1]
        n_own = n_local // row_size
        total_pts = block * row_size
        tiles = total_pts // TP
        sweeps = inv_temp.shape[0]
        n_chips = comp_size * row_size // CORES
        ni = 2 * sweeps
        bt = block // TP
        f32, bf16 = jnp.float32, jnp.bfloat16
        dma = pltpu.SemaphoreType.DMA
        vm = pltpu.VMEM
        scratch = [
            pltpu.SMEM((sweeps,), f32), vm((2, n_local), f32),
            vm((2, total_pts, half_dim), bf16),
            vm((2, n_local, half_dim), f32),
            vm((2, row_size, n_own, half_dim), bf16),
            vm((2, row_size, n_own, 128), f32),
            vm((2, row_size, 1, n_own), f32),
            vm((2, tiles, n_own, TP), f32),
            vm((2, row_size, bt, TP), f32),
            vm((2, row_size, bt, TP), f32),
            vm((row_size, bt, TP), f32),
            vm((n_own, half_dim), f32),
            vm((n_own, 128), f32),
            vm((row_size, 2, n_own), f32),
            vm((2, bt, TP), f32),
            vm((2, bt, TP), f32),
            vm((2, comp_size - 1, bt, TP), f32),
            vm((ni, 2, bt, TP), f32),
            vm((ni, 2, bt, TP), f32),
            vm((ni, n_chips - 1, 2, bt, TP), f32),
            vm((ni, row_size, bt, TP), f32),
            dma((6,)), pltpu.SemaphoreType.REGULAR, pltpu.SemaphoreType.REGULAR,
            dma((1,)), dma((2 * ND,)), dma((2 * ND,)), dma((2,)), dma((2,)), dma((2,)),
            dma((2,)), dma((2,)), dma((2,)), dma((2,)),
            dma((ni - 2,)), dma((ni - 2,)), dma((ni - 2,)), dma((ni - 2,)), dma((ni - 2,)), dma((ni - 2,)),
            dma((2,)), dma((2,)), dma((2,)), dma((2,)),
            dma((2, 2)), dma((2, 2)), dma((2,)), dma((2,)),
        ]
        outs = pl.pallas_call(
            functools.partial(em_kernel, comp_size, row_size, sweeps),
            out_shape=(vm((2, n_local, half_dim), f32), vm((2, n_local), f32), vm((2, block), f32)),
            in_specs=[
                pl.BlockSpec(memory_space=pl.ANY),
            ] * 4,
            out_specs=(pl.BlockSpec(memory_space=pltpu.VMEM),) * 3,
            scratch_shapes=scratch,
            compiler_params=pltpu.CompilerParams(
                collective_id=0, has_side_effects=True, vmem_limit_bytes=56 * 1024 * 1024),
        )(inv_temp, logpi_init, x_local, mu_init)
        return pl.pallas_call(
            write_kernel,
            out_shape=tuple(jax.ShapeDtypeStruct(o.shape, o.dtype) for o in outs),
            in_specs=[pl.BlockSpec(memory_space=pltpu.VMEM)] * 3,
            out_specs=(pl.BlockSpec(memory_space=pl.ANY),) * 3,
            scratch_shapes=[dma((3,))],
        )(*[pltpu.with_memory_space_constraint(o, pltpu.VMEM) for o in outs])

    return jax.shard_map(
        local_fit,
        mesh=mesh,
        in_specs=(P(("grp", "row"), None), P(None, ("grp", "comp"), None), P(None, ("grp", "comp")), P()),
        out_specs=(P(None, ("grp", "comp"), None), P(None, ("grp", "comp")), P(None, ("grp", "row"))),
        check_vma=False,
    )
```

```python
import functools

import jax
import jax.numpy as jnp
from jax import lax
from jax.experimental import pallas as pl
from jax.experimental.pallas import tpu as pltpu
from jax.sharding import PartitionSpec as P

EPS_COUNT = 1e-6
PRIOR_ALPHA = 1e-3
LOG2E = 1.4426950408889634
LN2 = 0.6931471805599453
MESH = pl.DeviceIdType.MESH

CORES = 2
TP = 256
NCK = 16
ND = 8


def lse2_parts(parts):
    top = functools.reduce(jnp.maximum, parts)
    total = functools.reduce(jnp.add, [jnp.exp2(p - top) for p in parts])
    return top + jnp.log(total) * LOG2E


def dot_t(a, b):
    return lax.dot_general(a, b, (((1,), (1,)), ((), ())), preferred_element_type=jnp.float32)


def eye_mask(n):
    return lax.broadcasted_iota(jnp.int32, (n, n), 0) == lax.broadcasted_iota(jnp.int32, (n, n), 1)


def col_to_row(col):
    return jnp.sum(jnp.where(eye_mask(col.shape[0]), col, 0.0), axis=0, keepdims=True)


def row_to_col(row):
    return jnp.sum(jnp.where(eye_mask(row.shape[1]), row, 0.0), axis=1, keepdims=True)


def twice(b):
    return jnp.concatenate([b, b], axis=1)


def write_kernel(a, b, c, a_out, b_out, c_out, sems):
    copies = [pltpu.make_async_copy(v, o, sems.at[k]) for k, (v, o) in enumerate(((a, a_out), (b, b_out), (c, c_out)))]
    for cp in copies:
        cp.start()
    for cp in copies:
        cp.wait()


def em_kernel(
    comp_size, row_size, sweeps,
    temp_hbm, lp_hbm, x_hbm, mu_hbm,
    mu_out, lp_out, lse_out,
    temp_ref, lp_ref, xg, mu_all, mub, bcol, brow, e_buf, m_buf, l_buf, lq_buf, s_acc, n_acc, lp_fin, sq_buf,
    zl_src, zl_buf, pre_buf, bc_src, bc_buf, tot_buf,
    load_sem, near_sem, far_sem, g_send, y_recv, z_recv, sy_recv, sz_recv, own_recv,
    zl_send, zl_recv, ag_send, ag_recv,
    pre_send, pre_recv, bc_send, bc_recv, post_send, post_recv,
    mx_send, mx_recv, br_send, br_recv, fin_send, fin_recv, lpf_send, lpf_recv,
):
    z = lax.axis_index("comp")
    r = lax.axis_index("row")
    y, c = r // CORES, r % CORES
    n_chips = comp_size * row_size // CORES
    y_size = row_size // CORES
    chip = z * y_size + y
    block = x_hbm.shape[0]
    half_dim = x_hbm.shape[1] // 2
    total_pts = block * row_size
    n_own = mub.shape[2]
    total_comp = mu_hbm.shape[1] * comp_size
    bt = block // TP
    ch = block // NCK
    rs = y * CORES + (1 - c)
    ry = (1 - y) * CORES + c
    sib = {"row": rs}
    yn = {"row": ry}
    yd = {"row": (1 - y) * CORES + (1 - c)}
    zn = {"comp": z + 1 - 2 * (z % 2)}
    hz = z % 2

    def remote(src, dst, send, recv, dev):
        return pltpu.make_async_remote_copy(
            src_ref=src, dst_ref=dst, send_sem=send, recv_sem=recv, device_id=dev, device_id_type=MESH)

    def same(v, send, recv, dev):
        return remote(v, v, send, recv, dev)

    x_loads = [pltpu.make_async_copy(
        x_hbm.at[:, pl.ds(s * half_dim, half_dim)], xg.at[s, pl.ds(r * block, block), :], load_sem.at[s])
        for s in range(2)]
    mu_loads = [pltpu.make_async_copy(mu_hbm.at[s], mu_all.at[s], load_sem.at[2 + s]) for s in range(2)]
    small_loads = [pltpu.make_async_copy(temp_hbm, temp_ref, load_sem.at[4]),
                   pltpu.make_async_copy(lp_hbm, lp_ref, load_sem.at[5])]
    for cp in x_loads + small_loads:
        cp.start()

    n_z = (z > 0).astype(jnp.int32) + (z < comp_size - 1).astype(jnp.int32)

    def signal_z(sem):
        @pl.when(z > 0)
        def _():
            pl.semaphore_signal(sem, inc=1, device_id={"comp": z - 1}, device_id_type=MESH)

        @pl.when(z < comp_size - 1)
        def _():
            pl.semaphore_signal(sem, inc=1, device_id={"comp": z + 1}, device_id_type=MESH)

    def signal_near(sem):
        for dev in (sib, yn):
            pl.semaphore_signal(sem, inc=1, device_id=dev, device_id_type=MESH)
        signal_z(sem)

    barrier = pltpu.get_barrier_semaphore()
    signal_near(barrier)
    pl.semaphore_wait(barrier, 2 + n_z)
    signal_near(near_sem)
    for cp in mu_loads:
        cp.start()

    def xrows(s, blk, cid):
        return xg.at[s, pl.ds(pl.multiple_of(blk * block + cid * ch, ch), ch), :]

    def cid_y(k):
        return k + hz * (NCK - 1 - 2 * k)

    def cid_z(k):
        return k + (1 - hz) * (NCK - 1 - 2 * k)

    def y_out(j):
        return same(xrows(j // ND, r, cid_y(j % ND)), g_send.at[0], y_recv.at[j], yn)

    def z_fwd(j):
        return same(xrows(j // ND, ry, cid_y(j % ND)), g_send.at[0], z_recv.at[j], zn)

    def sy_fwd(j):
        return same(xrows(j // ND, ry, cid_y(j % ND)), g_send.at[0], sy_recv.at[j // ND], sib)

    def sz_fwd(j):
        return same(xrows(j // ND, ry, cid_z(j % ND)), g_send.at[0], sz_recv.at[j // ND], sib)

    def own_out(s):
        return same(xg.at[s, pl.ds(r * block, block), :], g_send.at[0], own_recv.at[s], sib)

    def y_steps(a, b):
        def body(j, _):
            y_out(j).wait_recv()
            z_fwd(j).start()
            sy_fwd(j).start()
            return 0

        lax.fori_loop(a, b, body, 0)

    def z_steps(a, b):
        def body(j, _):
            z_fwd(j).wait_recv()
            sz_fwd(j).start()
            return 0

        lax.fori_loop(a, b, body, 0)

    def half_rows(s):
        return xg.at[s, pl.ds(0, ND * ch), :]

    def sib_waits(s):
        same(half_rows(s), g_send.at[0], sy_recv.at[s], sib).wait_recv()
        same(half_rows(s), g_send.at[0], sz_recv.at[s], sib).wait_recv()

    def gather_sends_wait(s):
        for _ in range(4):
            same(half_rows(s), g_send.at[0], sy_recv.at[s], sib).wait_send()
        own_out(s).wait_send()

    x_loads[0].wait()
    for j in range(ND):
        y_out(j).start()
    own_out(0).start()
    x_loads[1].wait()
    own_out(1).start()
    for cp in mu_loads + small_loads:
        cp.wait()

    def set_params(s, slot, mean, logw, t):
        mub[s, slot] = mean.astype(jnp.bfloat16)
        mu_sq = jnp.sum(mean * mean, axis=1, keepdims=True)
        col = (logw - temp_ref[t] * mu_sq) * LOG2E
        bcol[s, slot] = jnp.broadcast_to(col, (n_own, 128))
        return col

    def x_tile(s, tile):
        return xg[s, pl.ds(pl.multiple_of(tile * TP, TP), TP), :]

    def e_tile(s, slot, t, tile):
        a = dot_t(mub[s, slot], x_tile(s, tile))
        l2 = a * (temp_ref[t] * (2.0 * LOG2E)) + twice(bcol[s, slot])
        m = jnp.max(l2, axis=0, keepdims=True)
        e = jnp.exp2(l2 - m)
        return e, m, m + jnp.log(jnp.sum(e, axis=0, keepdims=True)) * LOG2E

    def tiles_of(half_id):
        return [(2 * half_id + k // bt, k % bt) for k in range(2 * bt)]

    def e_step(s, t, idx, hook=None):
        def body(i, _):
            h = (1 - c) + i * (2 * c - 1)
            for b, u in tiles_of(h):
                e, m, l = e_tile(s, r, t, b * bt + u)
                e_buf[s, b * bt + u] = e
                m_buf[s, b, u:u + 1, :] = m
                l_buf[s, b, u:u + 1, :] = l

            @pl.when(i == 0)
            def _():
                pre(idx).start()

            if hook is not None:
                hook(i)
            return 0

        lax.fori_loop(0, 2, body, 0)
        p2(idx)

    def acc_zero():
        s_acc[...] = jnp.zeros_like(s_acc)
        n_acc[...] = jnp.zeros_like(n_acc)

    def acc_tiles(s, tiles, resp_of):
        dots, ns = [], []
        for b, u in tiles:
            resp = resp_of(b, u)
            ns.append(resp[:, :128] + resp[:, 128:])
            dots.append(jnp.dot(resp.astype(jnp.bfloat16), x_tile(s, b * bt + u), preferred_element_type=jnp.float32))
        s_acc[...] += functools.reduce(jnp.add, dots)
        n_acc[...] += functools.reduce(jnp.add, ns)

    def m_step(s, t):
        idx = 2 * t + s
        acc_zero()

        def body(i, _):
            @pl.when(i == 1)
            def _():
                post(idx).wait()

            def resp_of(b, u):
                f = jnp.exp2(m_buf[s, b, u:u + 1, :] - tot_buf[idx, b, u:u + 1, :])
                return e_buf[s, b * bt + u] * f

            acc_tiles(s, tiles_of(c + i * (1 - 2 * c)), resp_of)
            return 0

        lax.fori_loop(0, 2, body, 0)

    def mr_half(s, slot, t, half_id):
        idx = 2 * t + s

        def resp_of(b, u):
            a = dot_t(mub[s, slot], x_tile(s, b * bt + u))
            return jnp.exp2(a * (temp_ref[t] * (2.0 * LOG2E)) + twice(bcol[s, slot]) - tot_buf[idx, b, u:u + 1, :])

        acc_tiles(s, tiles_of(half_id), resp_of)

    def mr_all(s, slot, t):
        for h in range(2):
            mr_half(s, slot, t, h)

    def acc_result():
        cnt = jnp.sum(n_acc[...], axis=1, keepdims=True)
        mean = s_acc[...] * (1.0 / (cnt + EPS_COUNT))
        logw = jnp.log((cnt + PRIOR_ALPHA) / (total_pts + total_comp * PRIOR_ALPHA))
        return mean, logw

    def half(ref, k):
        return ref.at[pl.ds(2 * k, 2)]

    def pre(idx):
        return remote(half(l_buf.at[idx % 2], 1 - c), pre_buf.at[idx], pre_send.at[idx - 2], pre_recv.at[idx - 2], sib)

    def bcast(idx, j):
        k = jnp.where(z < comp_size // 2, n_chips - j, j)
        q = lax.rem(chip + k, n_chips)
        return remote(bc_src.at[idx], bc_buf.at[idx, k - 1], bc_send.at[idx - 2], bc_recv.at[idx - 2],
                      {"comp": q // y_size, "row": (q % y_size) * CORES + c})

    def post(idx):
        return same(half(tot_buf.at[idx], c), post_send.at[idx - 2], post_recv.at[idx - 2], sib)

    def p2(idx):
        pre(idx).wait()
        bc_src[idx] = lse2_parts([l_buf[idx % 2, pl.ds(2 * c, 2)], pre_buf[idx]])
        for k in range(1, n_chips):
            bcast(idx, k).start()

    def p3(idx):
        same(bc_buf.at[idx], bc_send.at[idx - 2], bc_recv.at[idx - 2], sib).wait()
        tot_buf[idx, pl.ds(2 * c, 2)] = lse2_parts([bc_src[idx]] + [bc_buf[idx, k] for k in range(n_chips - 1)])
        post(idx).start()

    def zl(s, k):
        return remote(zl_src.at[s], zl_buf.at[s, k - 1], zl_send.at[s], zl_recv.at[s],
                      {"comp": lax.rem(z + k, comp_size)})

    def ag(s, k):
        return same(tot_buf.at[s, r], ag_send.at[s], ag_recv.at[s], (sib, yn, yd)[k])

    def orig_fit(s, _):
        def orig_slots(p, _):
            for k in range(2):
                q = 2 * p + k
                off = pl.multiple_of(q * n_own, n_own)
                set_params(s, q, mu_all[s, pl.ds(off, n_own), :], row_to_col(lp_ref[pl.ds(s, 1), pl.ds(off, n_own)]), 0)
                for u in range(bt):
                    _, _, l = e_tile(s, q, 0, r * bt + u)
                    lq_buf[q, u:u + 1, :] = l

            @pl.when(jnp.logical_and(s == 0, p == 0))
            def _():
                pl.semaphore_wait(near_sem, 2 + n_z)
                signal_z(far_sem)

            @pl.when(s == 1)
            def _():
                y_steps(1 + 2 * p, 3 + 2 * p)

            return 0

        lax.fori_loop(0, row_size // 2, orig_slots, 0)
        zl_src[s] = lse2_parts([lq_buf[q] for q in range(row_size)])

        @pl.when(s == 0)
        def _():
            pl.semaphore_wait(far_sem, n_z)

        for k in range(1, comp_size):
            zl(s, k).start()

        @pl.when(s == 0)
        def _():
            y_steps(0, 1)

        return 0

    lax.fori_loop(0, 2, orig_fit, 0)

    def y_sends(a, b):
        def send(j, _):
            y_out(j).start()
            return 0

        lax.fori_loop(a, b, send, 0)

    def comb(s):
        same(zl_buf.at[s], zl_send.at[s], zl_recv.at[s], sib).wait()
        tot_buf[s, r] = lse2_parts([zl_src[s]] + [zl_buf[s, k] for k in range(comp_size - 1)])
        for k in range(3):
            ag(s, k).start()

    early = ND + 3
    y_sends(ND, early)
    y_steps(5, 6)
    comb(0)
    y_sends(early, 2 * ND)
    y_steps(6, 8)
    z_steps(0, 4)
    y_steps(8, 9)
    z_steps(4, 6)
    y_steps(9, 10)
    comb(1)
    z_steps(6, 8)
    y_steps(10, 12)

    def sweep0(s, _):
        same(tot_buf.at[s, pl.ds(0, 3)], ag_send.at[s], ag_recv.at[s], sib).wait()
        own_out(s).wait_recv()
        acc_zero()

        @pl.when(s == 0)
        def _():
            sib_waits(0)
            y_steps(12, 15)

        def body(k, _):
            @pl.when(jnp.logical_and(s == 1, k == 1))
            def _():
                z_steps(15, 16)
                sib_waits(1)

            mr_half(s, r, 0, y + k * (1 - 2 * y))

            @pl.when(s == 0)
            def _():
                y_steps(16 - k, 16)
                z_steps(8 + 3 * k, 11 + k)

            return 0

        lax.fori_loop(0, 2, body, 0)
        mean, logw = acc_result()
        set_params(s, r, mean, logw, 1)

        def hook(i):
            @pl.when(jnp.logical_and(s == 0, i == 0))
            def _():
                z_steps(12, 14)

        e_step(s, 1, 2 + s, hook)

        @pl.when(s == 0)
        def _():
            z_steps(14, 15)

        return 0

    lax.fori_loop(0, 2, sweep0, 0)

    def mx(s):
        return same(mub.at[s, r], mx_send.at[s], mx_recv.at[s], yn)

    def br(s):
        return same(brow.at[s, r], br_send.at[s], br_recv.at[s], yn)

    def mean_rows(slot, s):
        return mu_out.at[s, pl.ds(pl.multiple_of(slot * n_own, n_own), n_own), :]

    def fin(slot, s, k):
        return same(mean_rows(slot, s), fin_send.at[s, k], fin_recv.at[s, k], sib)

    def lpf(slot, k):
        return same(lp_fin.at[slot], lpf_send.at[k], lpf_recv.at[k], sib)

    def sweep(i, _):
        t, s = i // 2, i % 2
        last = t == sweeps - 1
        p3(i)
        m_step(s, t)
        mean, logw = acc_result()

        @pl.when(t < sweeps - 1)
        def _():
            col = set_params(s, r, mean, logw, t + 1)

            @pl.when(t == sweeps - 2)
            def _():
                brow[s, r] = col_to_row(col)

            e_step(s, t + 1, i + 2)

            @pl.when(t == sweeps - 2)
            def _():
                mx(s).start()
                br(s).start()

        @pl.when(last)
        def _():
            mean_rows(r, s)[...] = mean
            lp_fin[r, pl.ds(s, 1), :] = col_to_row(logw)
            fin(r, s, 0).start()
            mx(s).wait()
            br(s).wait()
            bcol[s, ry] = jnp.broadcast_to(row_to_col(brow[s, ry]), (n_own, 128))
            acc_zero()

            mr_all(s, ry, t)
            mean2, logw2 = acc_result()
            mean_rows(ry, s)[...] = mean2
            lp_fin[ry, pl.ds(s, 1), :] = col_to_row(logw2)
            fin(ry, s, 1).start()

        return 0

    lax.fori_loop(2, 2 * sweeps, sweep, 0)
    lpf(r, 0).start()
    lpf(ry, 1).start()

    ones = jnp.ones((8, half_dim), jnp.bfloat16)

    def sq_norms(s, _):
        for u in range(bt):
            x = x_tile(s, r * bt + u).astype(jnp.float32)
            sq = x * x
            hi = sq.astype(jnp.bfloat16)
            lo = (sq - hi.astype(jnp.float32)).astype(jnp.bfloat16)
            sq_buf[s, u:u + 1, :] = (dot_t(ones, hi) + dot_t(ones, lo))[0:1]
        return 0

    lax.fori_loop(0, 2, sq_norms, 0)
    for s in range(2):
        gather_sends_wait(s)

    t = sweeps - 1
    for s in range(2):
        for j in range(bt):
            lse_out[s:s + 1, j * TP:(j + 1) * TP] = (
                tot_buf[2 * t + s, r, j:j + 1, :] * LN2 - temp_ref[t] * sq_buf[s, j:j + 1, :])

    for k in range(2):
        for s in range(2):
            fin((r, ry)[k], s, k).wait()
    lpf(r, 0).wait()
    lpf(ry, 1).wait()
    for q in range(row_size):
        lp_out[:, q * n_own:(q + 1) * n_own] = lp_fin[q]


def solution(mesh):
    comp_size = mesh.shape["comp"]
    row_size = mesh.shape["row"]

    def local_fit(x_local, mu_init, logpi_init, inv_temp):
        block, dim = x_local.shape
        half_dim = dim // 2
        n_local = mu_init.shape[1]
        n_own = n_local // row_size
        total_pts = block * row_size
        tiles = total_pts // TP
        sweeps = inv_temp.shape[0]
        n_chips = comp_size * row_size // CORES
        ni = 2 * sweeps
        bt = block // TP
        f32, bf16 = jnp.float32, jnp.bfloat16
        dma = pltpu.SemaphoreType.DMA
        vm = pltpu.VMEM
        scratch = [
            pltpu.SMEM((sweeps,), f32), vm((2, n_local), f32),
            vm((2, total_pts, half_dim), bf16),
            vm((2, n_local, half_dim), f32),
            vm((2, row_size, n_own, half_dim), bf16),
            vm((2, row_size, n_own, 128), f32),
            vm((2, row_size, 1, n_own), f32),
            vm((2, tiles, n_own, TP), f32),
            vm((2, row_size, bt, TP), f32),
            vm((2, row_size, bt, TP), f32),
            vm((row_size, bt, TP), f32),
            vm((n_own, half_dim), f32),
            vm((n_own, 128), f32),
            vm((row_size, 2, n_own), f32),
            vm((2, bt, TP), f32),
            vm((2, bt, TP), f32),
            vm((2, comp_size - 1, bt, TP), f32),
            vm((ni, 2, bt, TP), f32),
            vm((ni, 2, bt, TP), f32),
            vm((ni, n_chips - 1, 2, bt, TP), f32),
            vm((ni, row_size, bt, TP), f32),
            dma((6,)), pltpu.SemaphoreType.REGULAR, pltpu.SemaphoreType.REGULAR,
            dma((1,)), dma((2 * ND,)), dma((2 * ND,)), dma((2,)), dma((2,)), dma((2,)),
            dma((2,)), dma((2,)), dma((2,)), dma((2,)),
            dma((ni - 2,)), dma((ni - 2,)), dma((ni - 2,)), dma((ni - 2,)), dma((ni - 2,)), dma((ni - 2,)),
            dma((2,)), dma((2,)), dma((2,)), dma((2,)),
            dma((2, 2)), dma((2, 2)), dma((2,)), dma((2,)),
        ]
        outs = pl.pallas_call(
            functools.partial(em_kernel, comp_size, row_size, sweeps),
            out_shape=(vm((2, n_local, half_dim), f32), vm((2, n_local), f32), vm((2, block), f32)),
            in_specs=[
                pl.BlockSpec(memory_space=pl.ANY),
            ] * 4,
            out_specs=(pl.BlockSpec(memory_space=pltpu.VMEM),) * 3,
            scratch_shapes=scratch,
            compiler_params=pltpu.CompilerParams(
                collective_id=0, has_side_effects=True, vmem_limit_bytes=56 * 1024 * 1024),
        )(inv_temp, logpi_init, x_local, mu_init)
        return pl.pallas_call(
            write_kernel,
            out_shape=tuple(jax.ShapeDtypeStruct(o.shape, o.dtype) for o in outs),
            in_specs=[pl.BlockSpec(memory_space=pltpu.VMEM)] * 3,
            out_specs=(pl.BlockSpec(memory_space=pl.ANY),) * 3,
            scratch_shapes=[dma((3,))],
        )(*[pltpu.with_memory_space_constraint(o, pltpu.VMEM) for o in outs])

    return jax.shard_map(
        local_fit,
        mesh=mesh,
        in_specs=(P(("grp", "row"), None), P(None, ("grp", "comp"), None), P(None, ("grp", "comp")), P()),
        out_specs=(P(None, ("grp", "comp"), None), P(None, ("grp", "comp")), P(None, ("grp", "row"))),
        check_vma=False,
    )
```

```python
import functools

import jax
import jax.numpy as jnp
from jax import lax
from jax.experimental import pallas as pl
from jax.experimental.pallas import tpu as pltpu
from jax.sharding import PartitionSpec as P

EPS_COUNT = 1e-6
PRIOR_ALPHA = 1e-3
LOG2E = 1.4426950408889634
LN2 = 0.6931471805599453
MESH = pl.DeviceIdType.MESH

CORES = 2
TP = 256
NCK = 16
ND = 8


def lse2_parts(parts):
    top = functools.reduce(jnp.maximum, parts)
    total = functools.reduce(jnp.add, [jnp.exp2(p - top) for p in parts])
    return top + jnp.log(total) * LOG2E


def dot_t(a, b):
    return lax.dot_general(a, b, (((1,), (1,)), ((), ())), preferred_element_type=jnp.float32)


def eye_mask(n):
    return lax.broadcasted_iota(jnp.int32, (n, n), 0) == lax.broadcasted_iota(jnp.int32, (n, n), 1)


def col_to_row(col):
    return jnp.sum(jnp.where(eye_mask(col.shape[0]), col, 0.0), axis=0, keepdims=True)


def row_to_col(row):
    return jnp.sum(jnp.where(eye_mask(row.shape[1]), row, 0.0), axis=1, keepdims=True)


def twice(b):
    return jnp.concatenate([b, b], axis=1)


def write_kernel(a, b, c, a_out, b_out, c_out, sems):
    copies = [pltpu.make_async_copy(v, o, sems.at[k]) for k, (v, o) in enumerate(((a, a_out), (b, b_out), (c, c_out)))]
    for cp in copies:
        cp.start()
    for cp in copies:
        cp.wait()


def em_kernel(
    comp_size, row_size, sweeps,
    temp_hbm, lp_hbm, x_hbm, mu_hbm,
    mu_out, lp_out, lse_out,
    temp_ref, lp_ref, xg, mu_all, mub, bcol, brow, e_buf, m_buf, l_buf, lq_buf, s_acc, n_acc, lp_fin, sq_buf,
    zl_src, zl_buf, pre_buf, bc_src, bc_buf, tot_buf,
    load_sem, near_sem, far_sem, g_send, y_recv, z_recv, sy_recv, sz_recv, own_recv,
    zl_send, zl_recv, ag_send, ag_recv,
    pre_send, pre_recv, bc_send, bc_recv, post_send, post_recv,
    mx_send, mx_recv, br_send, br_recv, fin_send, fin_recv, lpf_send, lpf_recv,
):
    z = lax.axis_index("comp")
    r = lax.axis_index("row")
    y, c = r // CORES, r % CORES
    n_chips = comp_size * row_size // CORES
    y_size = row_size // CORES
    chip = z * y_size + y
    block = x_hbm.shape[0]
    half_dim = x_hbm.shape[1] // 2
    total_pts = block * row_size
    n_own = mub.shape[2]
    total_comp = mu_hbm.shape[1] * comp_size
    bt = block // TP
    ch = block // NCK
    rs = y * CORES + (1 - c)
    ry = (1 - y) * CORES + c
    sib = {"row": rs}
    yn = {"row": ry}
    rx = (1 - y) * CORES + (1 - c)
    yd = {"row": rx}
    zx = {"comp": z + 1 - 2 * (z % 2), "row": rs}
    hz = z % 2

    def remote(src, dst, send, recv, dev):
        return pltpu.make_async_remote_copy(
            src_ref=src, dst_ref=dst, send_sem=send, recv_sem=recv, device_id=dev, device_id_type=MESH)

    def same(v, send, recv, dev):
        return remote(v, v, send, recv, dev)

    x_loads = [pltpu.make_async_copy(
        x_hbm.at[:, pl.ds(s * half_dim, half_dim)], xg.at[s, pl.ds(r * block, block), :], load_sem.at[s])
        for s in range(2)]
    mu_loads = [pltpu.make_async_copy(mu_hbm.at[s], mu_all.at[s], load_sem.at[2 + s]) for s in range(2)]
    small_loads = [pltpu.make_async_copy(temp_hbm, temp_ref, load_sem.at[4]),
                   pltpu.make_async_copy(lp_hbm, lp_ref, load_sem.at[5])]
    for cp in x_loads + small_loads:
        cp.start()

    n_z = (z > 0).astype(jnp.int32) + (z < comp_size - 1).astype(jnp.int32)

    def signal_z(sem):
        @pl.when(z > 0)
        def _():
            pl.semaphore_signal(sem, inc=1, device_id={"comp": z - 1}, device_id_type=MESH)

        @pl.when(z < comp_size - 1)
        def _():
            pl.semaphore_signal(sem, inc=1, device_id={"comp": z + 1}, device_id_type=MESH)

    def signal_near(sem):
        for dev in (sib, yn, yd):
            pl.semaphore_signal(sem, inc=1, device_id=dev, device_id_type=MESH)
        signal_z(sem)

    barrier = pltpu.get_barrier_semaphore()
    signal_near(barrier)
    pl.semaphore_wait(barrier, 3 + n_z)
    signal_near(near_sem)
    for cp in mu_loads:
        cp.start()

    def xrows(s, blk, cid):
        return xg.at[s, pl.ds(pl.multiple_of(blk * block + cid * ch, ch), ch), :]

    def cid_y(k):
        return k + hz * (NCK - 1 - 2 * k)

    def cid_z(k):
        return k + (1 - hz) * (NCK - 1 - 2 * k)

    def y_out(j):
        return same(xrows(j // ND, r, cid_y(j % ND)), g_send.at[0], y_recv.at[j], yd)

    def z_fwd(j):
        return same(xrows(j // ND, rx, cid_y(j % ND)), g_send.at[0], z_recv.at[j], zx)

    def sy_fwd(j):
        return same(xrows(j // ND, rx, cid_y(j % ND)), g_send.at[0], sy_recv.at[j // ND], sib)

    def sz_fwd(j):
        return same(xrows(j // ND, ry, cid_z(j % ND)), g_send.at[0], sz_recv.at[j // ND], sib)

    def own_out(s):
        return same(xg.at[s, pl.ds(r * block, block), :], g_send.at[0], own_recv.at[s], sib)

    def y_steps(a, b):
        def body(j, _):
            y_out(j).wait_recv()
            z_fwd(j).start()
            sy_fwd(j).start()
            return 0

        lax.fori_loop(a, b, body, 0)

    def z_steps(a, b):
        def body(j, _):
            z_fwd(j).wait_recv()
            sz_fwd(j).start()
            return 0

        lax.fori_loop(a, b, body, 0)

    def half_rows(s):
        return xg.at[s, pl.ds(0, ND * ch), :]

    def sib_waits(s):
        same(half_rows(s), g_send.at[0], sy_recv.at[s], sib).wait_recv()
        same(half_rows(s), g_send.at[0], sz_recv.at[s], sib).wait_recv()

    def gather_sends_wait(s):
        for _ in range(4):
            same(half_rows(s), g_send.at[0], sy_recv.at[s], sib).wait_send()
        own_out(s).wait_send()

    x_loads[0].wait()
    for j in range(ND):
        y_out(j).start()
    own_out(0).start()
    x_loads[1].wait()
    own_out(1).start()
    for cp in mu_loads + small_loads:
        cp.wait()

    def set_params(s, slot, mean, logw, t):
        mub[s, slot] = mean.astype(jnp.bfloat16)
        mu_sq = jnp.sum(mean * mean, axis=1, keepdims=True)
        col = (logw - temp_ref[t] * mu_sq) * LOG2E
        bcol[s, slot] = jnp.broadcast_to(col, (n_own, 128))
        return col

    def x_tile(s, tile):
        return xg[s, pl.ds(pl.multiple_of(tile * TP, TP), TP), :]

    def e_tile(s, slot, t, tile):
        a = dot_t(mub[s, slot], x_tile(s, tile))
        l2 = a * (temp_ref[t] * (2.0 * LOG2E)) + twice(bcol[s, slot])
        m = jnp.max(l2, axis=0, keepdims=True)
        e = jnp.exp2(l2 - m)
        return e, m, m + jnp.log(jnp.sum(e, axis=0, keepdims=True)) * LOG2E

    def tiles_of(half_id):
        return [(2 * half_id + k // bt, k % bt) for k in range(2 * bt)]

    def e_step(s, t, idx, hook=None):
        def body(i, _):
            h = (1 - c) + i * (2 * c - 1)
            for b, u in tiles_of(h):
                e, m, l = e_tile(s, r, t, b * bt + u)
                e_buf[s, b * bt + u] = e
                m_buf[s, b, u:u + 1, :] = m
                l_buf[s, b, u:u + 1, :] = l

            @pl.when(i == 0)
            def _():
                pre(idx).start()

            if hook is not None:
                hook(i)
            return 0

        lax.fori_loop(0, 2, body, 0)
        p2(idx)

    def acc_zero():
        s_acc[...] = jnp.zeros_like(s_acc)
        n_acc[...] = jnp.zeros_like(n_acc)

    def acc_tiles(s, tiles, resp_of):
        dots, ns = [], []
        for b, u in tiles:
            resp = resp_of(b, u)
            ns.append(resp[:, :128] + resp[:, 128:])
            dots.append(jnp.dot(resp.astype(jnp.bfloat16), x_tile(s, b * bt + u), preferred_element_type=jnp.float32))
        s_acc[...] += functools.reduce(jnp.add, dots)
        n_acc[...] += functools.reduce(jnp.add, ns)

    def m_step(s, t):
        idx = 2 * t + s
        acc_zero()

        def body(i, _):
            @pl.when(i == 1)
            def _():
                post(idx).wait()

            def resp_of(b, u):
                f = jnp.exp2(m_buf[s, b, u:u + 1, :] - tot_buf[idx, b, u:u + 1, :])
                return e_buf[s, b * bt + u] * f

            acc_tiles(s, tiles_of((1 - c) + i * (2 * c - 1)), resp_of)
            return 0

        lax.fori_loop(0, 2, body, 0)

    def mr_half(s, slot, t, half_id):
        idx = 2 * t + s

        def resp_of(b, u):
            a = dot_t(mub[s, slot], x_tile(s, b * bt + u))
            return jnp.exp2(a * (temp_ref[t] * (2.0 * LOG2E)) + twice(bcol[s, slot]) - tot_buf[idx, b, u:u + 1, :])

        acc_tiles(s, tiles_of(half_id), resp_of)

    def mr_all(s, slot, t):
        for h in range(2):
            mr_half(s, slot, t, h)

    def acc_result():
        cnt = jnp.sum(n_acc[...], axis=1, keepdims=True)
        mean = s_acc[...] * (1.0 / (cnt + EPS_COUNT))
        logw = jnp.log((cnt + PRIOR_ALPHA) / (total_pts + total_comp * PRIOR_ALPHA))
        return mean, logw

    def half(ref, k):
        return ref.at[pl.ds(2 * k, 2)]

    def pre(idx):
        return remote(half(l_buf.at[idx % 2], 1 - c), pre_buf.at[idx], pre_send.at[idx - 2], pre_recv.at[idx - 2], sib)

    def bcast(idx, j):
        k = lax.rem(jnp.where(z < comp_size // 2, n_chips - j, j), n_chips)
        q = lax.rem(chip + k, n_chips)
        return remote(bc_src.at[idx], bc_buf.at[idx, k], bc_send.at[idx - 2], bc_recv.at[idx - 2],
                      {"comp": q // y_size, "row": (q % y_size) * CORES + (1 - c)})

    def post(idx):
        return same(half(tot_buf.at[idx], 1 - c), post_send.at[idx - 2], post_recv.at[idx - 2], sib)

    def p2(idx):
        pre(idx).wait()
        bc_src[idx] = lse2_parts([l_buf[idx % 2, pl.ds(2 * c, 2)], pre_buf[idx]])
        for j in range(1, n_chips + 1):
            bcast(idx, j).start()

    def p3(idx):
        same(bc_buf.at[idx], bc_send.at[idx - 2], bc_recv.at[idx - 2], sib).wait()
        tot_buf[idx, pl.ds(2 * (1 - c), 2)] = lse2_parts([bc_buf[idx, k] for k in range(n_chips)])
        post(idx).start()

    def zl(s, k):
        return remote(zl_src.at[s], zl_buf.at[s, k - 1], zl_send.at[s], zl_recv.at[s],
                      {"comp": lax.rem(z + k, comp_size)})

    def ag(s, k):
        return same(tot_buf.at[s, r], ag_send.at[s], ag_recv.at[s], (sib, yn, yd)[k])

    def orig_fit(s, _):
        def orig_slots(p, _):
            for k in range(2):
                q = 2 * p + k
                off = pl.multiple_of(q * n_own, n_own)
                set_params(s, q, mu_all[s, pl.ds(off, n_own), :], row_to_col(lp_ref[pl.ds(s, 1), pl.ds(off, n_own)]), 0)
                for u in range(bt):
                    _, _, l = e_tile(s, q, 0, r * bt + u)
                    lq_buf[q, u:u + 1, :] = l

            @pl.when(jnp.logical_and(s == 0, p == 0))
            def _():
                pl.semaphore_wait(near_sem, 3 + n_z)
                signal_z(far_sem)

            @pl.when(s == 1)
            def _():
                y_steps(1 + 2 * p, 3 + 2 * p)

            return 0

        lax.fori_loop(0, row_size // 2, orig_slots, 0)
        zl_src[s] = lse2_parts([lq_buf[q] for q in range(row_size)])

        @pl.when(s == 0)
        def _():
            pl.semaphore_wait(far_sem, n_z)

        for k in range(1, comp_size):
            zl(s, k).start()

        @pl.when(s == 0)
        def _():
            y_steps(0, 1)

        return 0

    lax.fori_loop(0, 2, orig_fit, 0)

    def y_sends(a, b):
        def send(j, _):
            y_out(j).start()
            return 0

        lax.fori_loop(a, b, send, 0)

    def comb(s):
        same(zl_buf.at[s], zl_send.at[s], zl_recv.at[s], sib).wait()
        tot_buf[s, r] = lse2_parts([zl_src[s]] + [zl_buf[s, k] for k in range(comp_size - 1)])
        for k in range(3):
            ag(s, k).start()

    early = ND + 3
    y_sends(ND, early)
    y_steps(5, 6)
    comb(0)
    y_sends(early, 2 * ND)
    y_steps(6, 8)
    z_steps(0, 4)
    y_steps(8, 9)
    z_steps(4, 6)
    y_steps(9, 10)
    comb(1)
    z_steps(6, 8)
    y_steps(10, 12)

    def sweep0(s, _):
        same(tot_buf.at[s, pl.ds(0, 3)], ag_send.at[s], ag_recv.at[s], sib).wait()
        own_out(s).wait_recv()
        acc_zero()

        @pl.when(s == 0)
        def _():
            sib_waits(0)
            y_steps(12, 15)

        def body(k, _):
            @pl.when(jnp.logical_and(s == 1, k == 1))
            def _():
                z_steps(15, 16)
                sib_waits(1)

            mr_half(s, r, 0, y + k * (1 - 2 * y))

            @pl.when(s == 0)
            def _():
                y_steps(16 - k, 16)
                z_steps(8 + 3 * k, 11 + k)

            return 0

        lax.fori_loop(0, 2, body, 0)
        mean, logw = acc_result()
        set_params(s, r, mean, logw, 1)

        def hook(i):
            @pl.when(jnp.logical_and(s == 0, i == 0))
            def _():
                z_steps(12, 14)

        e_step(s, 1, 2 + s, hook)

        @pl.when(s == 0)
        def _():
            z_steps(14, 15)

        return 0

    lax.fori_loop(0, 2, sweep0, 0)

    def mx(s):
        return same(mub.at[s, r], mx_send.at[s], mx_recv.at[s], yn)

    def br(s):
        return same(brow.at[s, r], br_send.at[s], br_recv.at[s], yn)

    def mean_rows(slot, s):
        return mu_out.at[s, pl.ds(pl.multiple_of(slot * n_own, n_own), n_own), :]

    def fin(slot, s, k):
        return same(mean_rows(slot, s), fin_send.at[s, k], fin_recv.at[s, k], sib)

    def lpf(slot, k):
        return same(lp_fin.at[slot], lpf_send.at[k], lpf_recv.at[k], sib)

    def sweep(i, _):
        t, s = i // 2, i % 2
        last = t == sweeps - 1
        p3(i)
        m_step(s, t)
        mean, logw = acc_result()

        @pl.when(t < sweeps - 1)
        def _():
            col = set_params(s, r, mean, logw, t + 1)

            @pl.when(t == sweeps - 2)
            def _():
                brow[s, r] = col_to_row(col)

            e_step(s, t + 1, i + 2)

            @pl.when(t == sweeps - 2)
            def _():
                mx(s).start()
                br(s).start()

        @pl.when(last)
        def _():
            mean_rows(r, s)[...] = mean
            lp_fin[r, pl.ds(s, 1), :] = col_to_row(logw)
            fin(r, s, 0).start()
            mx(s).wait()
            br(s).wait()
            bcol[s, ry] = jnp.broadcast_to(row_to_col(brow[s, ry]), (n_own, 128))
            acc_zero()

            mr_all(s, ry, t)
            mean2, logw2 = acc_result()
            mean_rows(ry, s)[...] = mean2
            lp_fin[ry, pl.ds(s, 1), :] = col_to_row(logw2)
            fin(ry, s, 1).start()

        return 0

    lax.fori_loop(2, 2 * sweeps, sweep, 0)
    lpf(r, 0).start()
    lpf(ry, 1).start()

    ones = jnp.ones((8, half_dim), jnp.bfloat16)

    def sq_norms(s, _):
        for u in range(bt):
            x = x_tile(s, r * bt + u).astype(jnp.float32)
            sq = x * x
            hi = sq.astype(jnp.bfloat16)
            lo = (sq - hi.astype(jnp.float32)).astype(jnp.bfloat16)
            sq_buf[s, u:u + 1, :] = (dot_t(ones, hi) + dot_t(ones, lo))[0:1]
        return 0

    lax.fori_loop(0, 2, sq_norms, 0)
    for s in range(2):
        gather_sends_wait(s)

    t = sweeps - 1
    for s in range(2):
        for j in range(bt):
            lse_out[s:s + 1, j * TP:(j + 1) * TP] = (
                tot_buf[2 * t + s, r, j:j + 1, :] * LN2 - temp_ref[t] * sq_buf[s, j:j + 1, :])

    for k in range(2):
        for s in range(2):
            fin((r, ry)[k], s, k).wait()
    lpf(r, 0).wait()
    lpf(ry, 1).wait()
    for q in range(row_size):
        lp_out[:, q * n_own:(q + 1) * n_own] = lp_fin[q]


def solution(mesh):
    comp_size = mesh.shape["comp"]
    row_size = mesh.shape["row"]

    def local_fit(x_local, mu_init, logpi_init, inv_temp):
        block, dim = x_local.shape
        half_dim = dim // 2
        n_local = mu_init.shape[1]
        n_own = n_local // row_size
        total_pts = block * row_size
        tiles = total_pts // TP
        sweeps = inv_temp.shape[0]
        n_chips = comp_size * row_size // CORES
        ni = 2 * sweeps
        bt = block // TP
        f32, bf16 = jnp.float32, jnp.bfloat16
        dma = pltpu.SemaphoreType.DMA
        vm = pltpu.VMEM
        scratch = [
            pltpu.SMEM((sweeps,), f32), vm((2, n_local), f32),
            vm((2, total_pts, half_dim), bf16),
            vm((2, n_local, half_dim), f32),
            vm((2, row_size, n_own, half_dim), bf16),
            vm((2, row_size, n_own, 128), f32),
            vm((2, row_size, 1, n_own), f32),
            vm((2, tiles, n_own, TP), f32),
            vm((2, row_size, bt, TP), f32),
            vm((2, row_size, bt, TP), f32),
            vm((row_size, bt, TP), f32),
            vm((n_own, half_dim), f32),
            vm((n_own, 128), f32),
            vm((row_size, 2, n_own), f32),
            vm((2, bt, TP), f32),
            vm((2, bt, TP), f32),
            vm((2, comp_size - 1, bt, TP), f32),
            vm((ni, 2, bt, TP), f32),
            vm((ni, 2, bt, TP), f32),
            vm((ni, n_chips, 2, bt, TP), f32),
            vm((ni, row_size, bt, TP), f32),
            dma((6,)), pltpu.SemaphoreType.REGULAR, pltpu.SemaphoreType.REGULAR,
            dma((1,)), dma((2 * ND,)), dma((2 * ND,)), dma((2,)), dma((2,)), dma((2,)),
            dma((2,)), dma((2,)), dma((2,)), dma((2,)),
            dma((ni - 2,)), dma((ni - 2,)), dma((ni - 2,)), dma((ni - 2,)), dma((ni - 2,)), dma((ni - 2,)),
            dma((2,)), dma((2,)), dma((2,)), dma((2,)),
            dma((2, 2)), dma((2, 2)), dma((2,)), dma((2,)),
        ]
        outs = pl.pallas_call(
            functools.partial(em_kernel, comp_size, row_size, sweeps),
            out_shape=(vm((2, n_local, half_dim), f32), vm((2, n_local), f32), vm((2, block), f32)),
            in_specs=[
                pl.BlockSpec(memory_space=pl.ANY),
            ] * 4,
            out_specs=(pl.BlockSpec(memory_space=pltpu.VMEM),) * 3,
            scratch_shapes=scratch,
            compiler_params=pltpu.CompilerParams(
                collective_id=0, has_side_effects=True, vmem_limit_bytes=56 * 1024 * 1024),
        )(inv_temp, logpi_init, x_local, mu_init)
        return pl.pallas_call(
            write_kernel,
            out_shape=tuple(jax.ShapeDtypeStruct(o.shape, o.dtype) for o in outs),
            in_specs=[pl.BlockSpec(memory_space=pltpu.VMEM)] * 3,
            out_specs=(pl.BlockSpec(memory_space=pl.ANY),) * 3,
            scratch_shapes=[dma((3,))],
        )(*[pltpu.with_memory_space_constraint(o, pltpu.VMEM) for o in outs])

    return jax.shard_map(
        local_fit,
        mesh=mesh,
        in_specs=(P(("grp", "row"), None), P(None, ("grp", "comp"), None), P(None, ("grp", "comp")), P()),
        out_specs=(P(None, ("grp", "comp"), None), P(None, ("grp", "comp")), P(None, ("grp", "row"))),
        check_vma=False,
    )
```

```python
import functools

import jax
import jax.numpy as jnp
from jax import lax
from jax.experimental import pallas as pl
from jax.experimental.pallas import tpu as pltpu
from jax.sharding import PartitionSpec as P

EPS_COUNT = 1e-6
PRIOR_ALPHA = 1e-3
LOG2E = 1.4426950408889634
LN2 = 0.6931471805599453
MESH = pl.DeviceIdType.MESH

CORES = 2
TP = 256
NCK = 16
ND = 8


def lse2_parts(parts):
    top = functools.reduce(jnp.maximum, parts)
    total = functools.reduce(jnp.add, [jnp.exp2(p - top) for p in parts])
    return top + jnp.log(total) * LOG2E


def dot_t(a, b):
    return lax.dot_general(a, b, (((1,), (1,)), ((), ())), preferred_element_type=jnp.float32)


def eye_mask(n):
    return lax.broadcasted_iota(jnp.int32, (n, n), 0) == lax.broadcasted_iota(jnp.int32, (n, n), 1)


def col_to_row(col):
    return jnp.sum(jnp.where(eye_mask(col.shape[0]), col, 0.0), axis=0, keepdims=True)


def row_to_col(row):
    return jnp.sum(jnp.where(eye_mask(row.shape[1]), row, 0.0), axis=1, keepdims=True)


def twice(b):
    return jnp.concatenate([b, b], axis=1)


def write_kernel(a, b, c, a_out, b_out, c_out, sems):
    copies = [pltpu.make_async_copy(v, o, sems.at[k]) for k, (v, o) in enumerate(((a, a_out), (b, b_out), (c, c_out)))]
    for cp in copies:
        cp.start()
    for cp in copies:
        cp.wait()


def em_kernel(
    comp_size, row_size, sweeps,
    temp_hbm, lp_hbm, x_hbm, mu_hbm,
    mu_out, lp_out, lse_out,
    temp_ref, lp_ref, xg, mu_all, mub, bcol, brow, e_buf, m_buf, l_buf, lq_buf, s_acc, n_acc, lp_fin, sq_buf,
    zl_src, zl_buf, pre_buf, bc_src, bc_buf, tot_buf,
    load_sem, near_sem, far_sem, g_send, y_recv, z_recv, sy_recv, sz_recv, own_recv,
    zl_send, zl_recv, ag_send, ag_recv,
    pre_send, pre_recv, bc_send, bc_recv, post_send, post_recv,
    mx_send, mx_recv, br_send, br_recv, fin_send, fin_recv, lpf_send, lpf_recv,
):
    z = lax.axis_index("comp")
    r = lax.axis_index("row")
    y, c = r // CORES, r % CORES
    n_chips = comp_size * row_size // CORES
    y_size = row_size // CORES
    chip = z * y_size + y
    block = x_hbm.shape[0]
    half_dim = x_hbm.shape[1] // 2
    total_pts = block * row_size
    n_own = mub.shape[2]
    total_comp = mu_hbm.shape[1] * comp_size
    bt = block // TP
    ch = block // NCK
    rs = y * CORES + (1 - c)
    ry = (1 - y) * CORES + c
    sib = {"row": rs}
    yn = {"row": ry}
    rx = (1 - y) * CORES + (1 - c)
    yd = {"row": rx}
    zx = {"comp": z + 1 - 2 * (z % 2), "row": rs}
    hz = z % 2

    def remote(src, dst, send, recv, dev):
        return pltpu.make_async_remote_copy(
            src_ref=src, dst_ref=dst, send_sem=send, recv_sem=recv, device_id=dev, device_id_type=MESH)

    def same(v, send, recv, dev):
        return remote(v, v, send, recv, dev)

    x_loads = [pltpu.make_async_copy(
        x_hbm.at[:, pl.ds(s * half_dim, half_dim)], xg.at[s, pl.ds(r * block, block), :], load_sem.at[s])
        for s in range(2)]
    mu_loads = [pltpu.make_async_copy(mu_hbm.at[s], mu_all.at[s], load_sem.at[2 + s]) for s in range(2)]
    small_loads = [pltpu.make_async_copy(temp_hbm, temp_ref, load_sem.at[4]),
                   pltpu.make_async_copy(lp_hbm, lp_ref, load_sem.at[5])]
    for cp in x_loads + small_loads:
        cp.start()

    n_z = (z > 0).astype(jnp.int32) + (z < comp_size - 1).astype(jnp.int32)

    def signal_z(sem):
        @pl.when(z > 0)
        def _():
            pl.semaphore_signal(sem, inc=1, device_id={"comp": z - 1}, device_id_type=MESH)

        @pl.when(z < comp_size - 1)
        def _():
            pl.semaphore_signal(sem, inc=1, device_id={"comp": z + 1}, device_id_type=MESH)

    def signal_near(sem):
        for dev in (sib, yn, yd):
            pl.semaphore_signal(sem, inc=1, device_id=dev, device_id_type=MESH)
        signal_z(sem)

    barrier = pltpu.get_barrier_semaphore()
    signal_near(barrier)
    pl.semaphore_wait(barrier, 3 + n_z)
    signal_near(near_sem)
    for cp in mu_loads:
        cp.start()

    def xrows(s, blk, cid):
        return xg.at[s, pl.ds(pl.multiple_of(blk * block + cid * ch, ch), ch), :]

    def cid_y(k):
        return k + hz * (NCK - 1 - 2 * k)

    def cid_z(k):
        return k + (1 - hz) * (NCK - 1 - 2 * k)

    def y_out(j):
        return same(xrows(j // ND, r, cid_y(j % ND)), g_send.at[0], y_recv.at[j], yd)

    def z_fwd(j):
        return same(xrows(j // ND, rx, cid_y(j % ND)), g_send.at[0], z_recv.at[j], zx)

    def sy_fwd(j):
        return same(xrows(j // ND, rx, cid_y(j % ND)), g_send.at[0], sy_recv.at[j // ND], sib)

    def sz_fwd(j):
        return same(xrows(j // ND, ry, cid_z(j % ND)), g_send.at[0], sz_recv.at[j // ND], sib)

    def own_out(s):
        return same(xg.at[s, pl.ds(r * block, block), :], g_send.at[0], own_recv.at[s], sib)

    def y_steps(a, b):
        def body(j, _):
            y_out(j).wait_recv()
            z_fwd(j).start()
            sy_fwd(j).start()
            return 0

        lax.fori_loop(a, b, body, 0)

    def z_steps(a, b):
        def body(j, _):
            z_fwd(j).wait_recv()
            sz_fwd(j).start()
            return 0

        lax.fori_loop(a, b, body, 0)

    def half_rows(s):
        return xg.at[s, pl.ds(0, ND * ch), :]

    def sib_waits(s):
        same(half_rows(s), g_send.at[0], sy_recv.at[s], sib).wait_recv()
        same(half_rows(s), g_send.at[0], sz_recv.at[s], sib).wait_recv()

    def gather_sends_wait(s):
        for _ in range(4):
            same(half_rows(s), g_send.at[0], sy_recv.at[s], sib).wait_send()
        own_out(s).wait_send()

    x_loads[0].wait()
    for j in range(ND):
        y_out(j).start()
    own_out(0).start()
    x_loads[1].wait()
    own_out(1).start()
    for cp in mu_loads + small_loads:
        cp.wait()

    def set_params(s, slot, mean, logw, t):
        mub[s, slot] = mean.astype(jnp.bfloat16)
        mu_sq = jnp.sum(mean * mean, axis=1, keepdims=True)
        col = (logw - temp_ref[t] * mu_sq) * LOG2E
        bcol[s, slot] = jnp.broadcast_to(col, (n_own, 128))
        return col

    def x_tile(s, tile):
        return xg[s, pl.ds(pl.multiple_of(tile * TP, TP), TP), :]

    def e_tile(s, slot, t, tile):
        a = dot_t(mub[s, slot], x_tile(s, tile))
        l2 = a * (temp_ref[t] * (2.0 * LOG2E)) + twice(bcol[s, slot])
        m = jnp.max(l2, axis=0, keepdims=True)
        e = jnp.exp2(l2 - m)
        return e, m, m + jnp.log(jnp.sum(e, axis=0, keepdims=True)) * LOG2E

    def tiles_of(half_id):
        return [(2 * half_id + k // bt, k % bt) for k in range(2 * bt)]

    def e_step(s, t, idx, hook=None, early=None):
        def body(i, _):
            h = (1 - c) + i * (2 * c - 1)
            for b, u in tiles_of(h):
                e, m, l = e_tile(s, r, t, b * bt + u)
                e_buf[s, b * bt + u] = e
                m_buf[s, b, u:u + 1, :] = m
                l_buf[s, b, u:u + 1, :] = l

            @pl.when(i == 0)
            def _():
                pre(idx).start()

            if hook is not None:
                hook(i)
            return 0

        lax.fori_loop(0, 2, body, 0)
        if early is not None:
            early()
        p2(idx)

    def acc_zero():
        s_acc[...] = jnp.zeros_like(s_acc)
        n_acc[...] = jnp.zeros_like(n_acc)

    def acc_tiles(s, tiles, resp_of):
        dots, ns = [], []
        for b, u in tiles:
            resp = resp_of(b, u)
            ns.append(resp[:, :128] + resp[:, 128:])
            dots.append(jnp.dot(resp.astype(jnp.bfloat16), x_tile(s, b * bt + u), preferred_element_type=jnp.float32))
        s_acc[...] += functools.reduce(jnp.add, dots)
        n_acc[...] += functools.reduce(jnp.add, ns)

    def m_step(s, t):
        idx = 2 * t + s
        acc_zero()

        def body(i, _):
            @pl.when(i == 1)
            def _():
                post(idx).wait()

            def resp_of(b, u):
                f = jnp.exp2(m_buf[s, b, u:u + 1, :] - tot_buf[idx, b, u:u + 1, :])
                return e_buf[s, b * bt + u] * f

            acc_tiles(s, tiles_of((1 - c) + i * (2 * c - 1)), resp_of)
            return 0

        lax.fori_loop(0, 2, body, 0)

    def mr_half(s, slot, t, half_id):
        idx = 2 * t + s

        def resp_of(b, u):
            a = dot_t(mub[s, slot], x_tile(s, b * bt + u))
            return jnp.exp2(a * (temp_ref[t] * (2.0 * LOG2E)) + twice(bcol[s, slot]) - tot_buf[idx, b, u:u + 1, :])

        acc_tiles(s, tiles_of(half_id), resp_of)

    def mr_all(s, slot, t):
        for h in range(2):
            mr_half(s, slot, t, h)

    def acc_result():
        cnt = jnp.sum(n_acc[...], axis=1, keepdims=True)
        mean = s_acc[...] * (1.0 / (cnt + EPS_COUNT))
        logw = jnp.log((cnt + PRIOR_ALPHA) / (total_pts + total_comp * PRIOR_ALPHA))
        return mean, logw

    def half(ref, k):
        return ref.at[pl.ds(2 * k, 2)]

    def pre(idx):
        return remote(half(l_buf.at[idx % 2], 1 - c), pre_buf.at[idx], pre_send.at[idx - 2], pre_recv.at[idx - 2], sib)

    def bcast(idx, j):
        k = lax.rem(jnp.where(z < comp_size // 2, n_chips - j, j), n_chips)
        q = lax.rem(chip + k, n_chips)
        return remote(bc_src.at[idx], bc_buf.at[idx, k], bc_send.at[idx - 2], bc_recv.at[idx - 2],
                      {"comp": q // y_size, "row": (q % y_size) * CORES + (1 - c)})

    def post(idx):
        return same(half(tot_buf.at[idx], 1 - c), post_send.at[idx - 2], post_recv.at[idx - 2], sib)

    def p2(idx):
        pre(idx).wait()
        bc_src[idx] = lse2_parts([l_buf[idx % 2, pl.ds(2 * c, 2)], pre_buf[idx]])
        for j in range(1, n_chips + 1):
            bcast(idx, j).start()

    def p3(idx):
        same(bc_buf.at[idx], bc_send.at[idx - 2], bc_recv.at[idx - 2], sib).wait()
        tot_buf[idx, pl.ds(2 * (1 - c), 2)] = lse2_parts([bc_buf[idx, k] for k in range(n_chips)])
        post(idx).start()

    def zl(s, k):
        return remote(zl_src.at[s], zl_buf.at[s, k - 1], zl_send.at[s], zl_recv.at[s],
                      {"comp": lax.rem(z + k, comp_size)})

    def ag(s, k):
        return same(tot_buf.at[s, r], ag_send.at[s], ag_recv.at[s], (sib, yn, yd)[k])

    def orig_fit(s, _):
        def orig_slots(p, _):
            for k in range(2):
                q = 2 * p + k
                off = pl.multiple_of(q * n_own, n_own)
                set_params(s, q, mu_all[s, pl.ds(off, n_own), :], row_to_col(lp_ref[pl.ds(s, 1), pl.ds(off, n_own)]), 0)
                for u in range(bt):
                    _, _, l = e_tile(s, q, 0, r * bt + u)
                    lq_buf[q, u:u + 1, :] = l

            @pl.when(jnp.logical_and(s == 0, p == 0))
            def _():
                pl.semaphore_wait(near_sem, 3 + n_z)
                signal_z(far_sem)

            @pl.when(s == 1)
            def _():
                y_steps(1 + 2 * p, 3 + 2 * p)

            return 0

        lax.fori_loop(0, row_size // 2, orig_slots, 0)
        zl_src[s] = lse2_parts([lq_buf[q] for q in range(row_size)])

        @pl.when(s == 0)
        def _():
            pl.semaphore_wait(far_sem, n_z)

        for k in range(1, comp_size):
            zl(s, k).start()

        @pl.when(s == 0)
        def _():
            y_steps(0, 1)

        return 0

    lax.fori_loop(0, 2, orig_fit, 0)

    def y_sends(a, b):
        def send(j, _):
            y_out(j).start()
            return 0

        lax.fori_loop(a, b, send, 0)

    def comb(s):
        same(zl_buf.at[s], zl_send.at[s], zl_recv.at[s], sib).wait()
        tot_buf[s, r] = lse2_parts([zl_src[s]] + [zl_buf[s, k] for k in range(comp_size - 1)])
        for k in range(3):
            ag(s, k).start()

    early = ND + 3
    y_sends(ND, early)
    y_steps(5, 6)
    comb(0)
    y_sends(early, 2 * ND)
    y_steps(6, 8)
    z_steps(0, 4)
    y_steps(8, 9)
    z_steps(4, 6)
    y_steps(9, 10)
    comb(1)
    z_steps(6, 8)
    y_steps(10, 12)

    def sweep0(s, _):
        same(tot_buf.at[s, pl.ds(0, 3)], ag_send.at[s], ag_recv.at[s], sib).wait()
        own_out(s).wait_recv()
        acc_zero()

        def body(k, _):
            @pl.when(jnp.logical_and(s == 0, k == 1))
            def _():
                y_steps(12, 14)
                sib_waits(0)
                y_steps(14, 15)

            @pl.when(jnp.logical_and(s == 1, k == 1))
            def _():
                z_steps(15, 16)
                sib_waits(1)

            mr_half(s, r, 0, y + k * (1 - 2 * y))

            @pl.when(jnp.logical_and(s == 0, k == 1))
            def _():
                y_steps(15, 16)
                z_steps(8, 12)

            return 0

        lax.fori_loop(0, 2, body, 0)
        mean, logw = acc_result()
        set_params(s, r, mean, logw, 1)

        def hook(i):
            @pl.when(jnp.logical_and(s == 0, i == 0))
            def _():
                z_steps(12, 13)

        def first_p3():
            @pl.when(s == 1)
            def _():
                p3(2)

        e_step(s, 1, 2 + s, hook, first_p3)

        @pl.when(s == 0)
        def _():
            z_steps(13, 15)

        return 0

    lax.fori_loop(0, 2, sweep0, 0)

    def mx(s):
        return same(mub.at[s, r], mx_send.at[s], mx_recv.at[s], yn)

    def br(s):
        return same(brow.at[s, r], br_send.at[s], br_recv.at[s], yn)

    def mean_rows(slot, s):
        return mu_out.at[s, pl.ds(pl.multiple_of(slot * n_own, n_own), n_own), :]

    def fin(slot, s, k):
        return same(mean_rows(slot, s), fin_send.at[s, k], fin_recv.at[s, k], sib)

    def lpf(slot, k):
        return same(lp_fin.at[slot], lpf_send.at[k], lpf_recv.at[k], sib)

    def sweep(i, _):
        t, s = i // 2, i % 2
        last = t == sweeps - 1
        m_step(s, t)
        mean, logw = acc_result()

        @pl.when(t < sweeps - 1)
        def _():
            col = set_params(s, r, mean, logw, t + 1)

            @pl.when(t == sweeps - 2)
            def _():
                brow[s, r] = col_to_row(col)

            e_step(s, t + 1, i + 2, early=lambda: p3(i + 1))

            @pl.when(t == sweeps - 2)
            def _():
                mx(s).start()
                br(s).start()

        @pl.when(last)
        def _():
            mean_rows(r, s)[...] = mean
            lp_fin[r, pl.ds(s, 1), :] = col_to_row(logw)
            fin(r, s, 0).start()
            mx(s).wait()
            br(s).wait()
            bcol[s, ry] = jnp.broadcast_to(row_to_col(brow[s, ry]), (n_own, 128))
            acc_zero()

            mr_all(s, ry, t)
            mean2, logw2 = acc_result()
            mean_rows(ry, s)[...] = mean2
            lp_fin[ry, pl.ds(s, 1), :] = col_to_row(logw2)
            fin(ry, s, 1).start()

            @pl.when(s == 0)
            def _():
                p3(i + 1)

        return 0

    lax.fori_loop(2, 2 * sweeps, sweep, 0)
    lpf(r, 0).start()
    lpf(ry, 1).start()

    ones = jnp.ones((8, half_dim), jnp.bfloat16)

    def sq_norms(s, _):
        for u in range(bt):
            x = x_tile(s, r * bt + u).astype(jnp.float32)
            sq = x * x
            hi = sq.astype(jnp.bfloat16)
            lo = (sq - hi.astype(jnp.float32)).astype(jnp.bfloat16)
            sq_buf[s, u:u + 1, :] = (dot_t(ones, hi) + dot_t(ones, lo))[0:1]
        return 0

    lax.fori_loop(0, 2, sq_norms, 0)
    for s in range(2):
        gather_sends_wait(s)

    t = sweeps - 1
    for s in range(2):
        for j in range(bt):
            lse_out[s:s + 1, j * TP:(j + 1) * TP] = (
                tot_buf[2 * t + s, r, j:j + 1, :] * LN2 - temp_ref[t] * sq_buf[s, j:j + 1, :])

    for k in range(2):
        for s in range(2):
            fin((r, ry)[k], s, k).wait()
    lpf(r, 0).wait()
    lpf(ry, 1).wait()
    for q in range(row_size):
        lp_out[:, q * n_own:(q + 1) * n_own] = lp_fin[q]


def solution(mesh):
    comp_size = mesh.shape["comp"]
    row_size = mesh.shape["row"]

    def local_fit(x_local, mu_init, logpi_init, inv_temp):
        block, dim = x_local.shape
        half_dim = dim // 2
        n_local = mu_init.shape[1]
        n_own = n_local // row_size
        total_pts = block * row_size
        tiles = total_pts // TP
        sweeps = inv_temp.shape[0]
        n_chips = comp_size * row_size // CORES
        ni = 2 * sweeps
        bt = block // TP
        f32, bf16 = jnp.float32, jnp.bfloat16
        dma = pltpu.SemaphoreType.DMA
        vm = pltpu.VMEM
        scratch = [
            pltpu.SMEM((sweeps,), f32), vm((2, n_local), f32),
            vm((2, total_pts, half_dim), bf16),
            vm((2, n_local, half_dim), f32),
            vm((2, row_size, n_own, half_dim), bf16),
            vm((2, row_size, n_own, 128), f32),
            vm((2, row_size, 1, n_own), f32),
            vm((2, tiles, n_own, TP), f32),
            vm((2, row_size, bt, TP), f32),
            vm((2, row_size, bt, TP), f32),
            vm((row_size, bt, TP), f32),
            vm((n_own, half_dim), f32),
            vm((n_own, 128), f32),
            vm((row_size, 2, n_own), f32),
            vm((2, bt, TP), f32),
            vm((2, bt, TP), f32),
            vm((2, comp_size - 1, bt, TP), f32),
            vm((ni, 2, bt, TP), f32),
            vm((ni, 2, bt, TP), f32),
            vm((ni, n_chips, 2, bt, TP), f32),
            vm((ni, row_size, bt, TP), f32),
            dma((6,)), pltpu.SemaphoreType.REGULAR, pltpu.SemaphoreType.REGULAR,
            dma((1,)), dma((2 * ND,)), dma((2 * ND,)), dma((2,)), dma((2,)), dma((2,)),
            dma((2,)), dma((2,)), dma((2,)), dma((2,)),
            dma((ni - 2,)), dma((ni - 2,)), dma((ni - 2,)), dma((ni - 2,)), dma((ni - 2,)), dma((ni - 2,)),
            dma((2,)), dma((2,)), dma((2,)), dma((2,)),
            dma((2, 2)), dma((2, 2)), dma((2,)), dma((2,)),
        ]
        outs = pl.pallas_call(
            functools.partial(em_kernel, comp_size, row_size, sweeps),
            out_shape=(vm((2, n_local, half_dim), f32), vm((2, n_local), f32), vm((2, block), f32)),
            in_specs=[
                pl.BlockSpec(memory_space=pl.ANY),
            ] * 4,
            out_specs=(pl.BlockSpec(memory_space=pltpu.VMEM),) * 3,
            scratch_shapes=scratch,
            compiler_params=pltpu.CompilerParams(
                collective_id=0, has_side_effects=True, vmem_limit_bytes=56 * 1024 * 1024),
        )(inv_temp, logpi_init, x_local, mu_init)
        return pl.pallas_call(
            write_kernel,
            out_shape=tuple(jax.ShapeDtypeStruct(o.shape, o.dtype) for o in outs),
            in_specs=[pl.BlockSpec(memory_space=pltpu.VMEM)] * 3,
            out_specs=(pl.BlockSpec(memory_space=pl.ANY),) * 3,
            scratch_shapes=[dma((3,))],
        )(*[pltpu.with_memory_space_constraint(o, pltpu.VMEM) for o in outs])

    return jax.shard_map(
        local_fit,
        mesh=mesh,
        in_specs=(P(("grp", "row"), None), P(None, ("grp", "comp"), None), P(None, ("grp", "comp")), P()),
        out_specs=(P(None, ("grp", "comp"), None), P(None, ("grp", "comp")), P(None, ("grp", "row"))),
        check_vma=False,
    )
```

```python
import functools

import jax
import jax.numpy as jnp
from jax import lax
from jax.experimental import pallas as pl
from jax.experimental.pallas import tpu as pltpu
from jax.sharding import PartitionSpec as P

EPS_COUNT = 1e-6
PRIOR_ALPHA = 1e-3
LOG2E = 1.4426950408889634
LN2 = 0.6931471805599453
MESH = pl.DeviceIdType.MESH

CORES = 2
TP = 256
NCK = 16
ND = 9
NR = NCK - ND


def lse2_parts(parts):
    top = functools.reduce(jnp.maximum, parts)
    total = functools.reduce(jnp.add, [jnp.exp2(p - top) for p in parts])
    return top + jnp.log(total) * LOG2E


def dot_t(a, b):
    return lax.dot_general(a, b, (((1,), (1,)), ((), ())), preferred_element_type=jnp.float32)


def eye_mask(n):
    return lax.broadcasted_iota(jnp.int32, (n, n), 0) == lax.broadcasted_iota(jnp.int32, (n, n), 1)


def col_to_row(col):
    return jnp.sum(jnp.where(eye_mask(col.shape[0]), col, 0.0), axis=0, keepdims=True)


def row_to_col(row):
    return jnp.sum(jnp.where(eye_mask(row.shape[1]), row, 0.0), axis=1, keepdims=True)


def twice(b):
    return jnp.concatenate([b, b], axis=1)


def write_kernel(a, b, c, a_out, b_out, c_out, sems):
    copies = [pltpu.make_async_copy(v, o, sems.at[k]) for k, (v, o) in enumerate(((a, a_out), (b, b_out), (c, c_out)))]
    for cp in copies:
        cp.start()
    for cp in copies:
        cp.wait()


def em_kernel(
    comp_size, row_size, sweeps,
    temp_hbm, lp_hbm, x_hbm, mu_hbm,
    mu_out, lp_out, lse_out,
    temp_ref, lp_ref, xg, mu_all, mub, bcol, brow, e_buf, m_buf, l_buf, lq_buf, s_acc, n_acc, lp_fin, sq_buf,
    zl_src, zl_buf, pre_buf, bc_src, bc_buf, tot_buf,
    load_sem, near_sem, far_sem, g_send, y_recv, z_recv, sy_recv, sz_recv, own_recv,
    zl_send, zl_recv, ag_send, ag_recv,
    pre_send, pre_recv, bc_send, bc_recv, post_send, post_recv,
    mx_send, mx_recv, br_send, br_recv, fin_send, fin_recv, lpf_send, lpf_recv,
):
    z = lax.axis_index("comp")
    r = lax.axis_index("row")
    y, c = r // CORES, r % CORES
    n_chips = comp_size * row_size // CORES
    y_size = row_size // CORES
    chip = z * y_size + y
    block = x_hbm.shape[0]
    half_dim = x_hbm.shape[1] // 2
    total_pts = block * row_size
    n_own = mub.shape[2]
    total_comp = mu_hbm.shape[1] * comp_size
    bt = block // TP
    ch = block // NCK
    rs = y * CORES + (1 - c)
    ry = (1 - y) * CORES + c
    sib = {"row": rs}
    yn = {"row": ry}
    rx = (1 - y) * CORES + (1 - c)
    yd = {"row": rx}
    zx = {"comp": z + 1 - 2 * (z % 2), "row": rs}
    hz = z % 2

    def remote(src, dst, send, recv, dev):
        return pltpu.make_async_remote_copy(
            src_ref=src, dst_ref=dst, send_sem=send, recv_sem=recv, device_id=dev, device_id_type=MESH)

    def same(v, send, recv, dev):
        return remote(v, v, send, recv, dev)

    x_loads = [pltpu.make_async_copy(
        x_hbm.at[:, pl.ds(s * half_dim, half_dim)], xg.at[s, pl.ds(r * block, block), :], load_sem.at[s])
        for s in range(2)]
    mu_loads = [pltpu.make_async_copy(mu_hbm.at[s], mu_all.at[s], load_sem.at[2 + s]) for s in range(2)]
    small_loads = [pltpu.make_async_copy(temp_hbm, temp_ref, load_sem.at[4]),
                   pltpu.make_async_copy(lp_hbm, lp_ref, load_sem.at[5])]
    for cp in x_loads + small_loads:
        cp.start()

    n_z = (z > 0).astype(jnp.int32) + (z < comp_size - 1).astype(jnp.int32)

    def signal_z(sem):
        @pl.when(z > 0)
        def _():
            pl.semaphore_signal(sem, inc=1, device_id={"comp": z - 1}, device_id_type=MESH)

        @pl.when(z < comp_size - 1)
        def _():
            pl.semaphore_signal(sem, inc=1, device_id={"comp": z + 1}, device_id_type=MESH)

    def signal_near(sem):
        for dev in (sib, yn, yd):
            pl.semaphore_signal(sem, inc=1, device_id=dev, device_id_type=MESH)
        signal_z(sem)

    barrier = pltpu.get_barrier_semaphore()
    signal_near(barrier)
    pl.semaphore_wait(barrier, 3 + n_z)
    signal_near(near_sem)
    for cp in mu_loads:
        cp.start()

    def xrows(s, blk, cid):
        return xg.at[s, pl.ds(pl.multiple_of(blk * block + cid * ch, ch), ch), :]

    def cid_y(k):
        return k + hz * (NCK - 1 - 2 * k)

    def cid_z(k):
        return k + (1 - hz) * (NCK - 1 - 2 * k)

    def y_out(j):
        return same(xrows(j // ND, r, cid_y(j % ND)), g_send.at[0], y_recv.at[j], yd)

    def z_fwd(m):
        return same(xrows(m // NR, rx, cid_y(m % NR)), g_send.at[0], z_recv.at[m], zx)

    def sy_fwd(j):
        return same(xrows(j // ND, rx, cid_y(j % ND)), g_send.at[0], sy_recv.at[j // ND], sib)

    def sz_fwd(m):
        return same(xrows(m // NR, ry, cid_z(m % NR)), g_send.at[0], sz_recv.at[m // NR], sib)

    def own_out(s):
        return same(xg.at[s, pl.ds(r * block, block), :], g_send.at[0], own_recv.at[s], sib)

    def y_steps(a, b):
        def body(j, _):
            y_out(j).wait_recv()

            @pl.when(j % ND < NR)
            def _():
                z_fwd(j // ND * NR + j % ND).start()

            sy_fwd(j).start()
            return 0

        lax.fori_loop(a, b, body, 0)

    def z_steps(a, b):
        def body(m, _):
            z_fwd(m).wait_recv()
            sz_fwd(m).start()
            return 0

        lax.fori_loop(a, b, body, 0)

    def rows_of(s, chunks):
        return xg.at[s, pl.ds(0, chunks * ch), :]

    def sib_waits(s):
        same(rows_of(s, ND), g_send.at[0], sy_recv.at[s], sib).wait_recv()
        same(rows_of(s, NR), g_send.at[0], sz_recv.at[s], sib).wait_recv()

    def gather_sends_wait(s):
        for chunks in (ND, NR, ND, NR):
            same(rows_of(s, chunks), g_send.at[0], sy_recv.at[s], sib).wait_send()
        own_out(s).wait_send()

    x_loads[0].wait()
    for j in range(ND):
        y_out(j).start()
    own_out(0).start()
    x_loads[1].wait()
    own_out(1).start()
    for cp in mu_loads + small_loads:
        cp.wait()

    def set_params(s, slot, mean, logw, t):
        mub[s, slot] = mean.astype(jnp.bfloat16)
        mu_sq = jnp.sum(mean * mean, axis=1, keepdims=True)
        col = (logw - temp_ref[t] * mu_sq) * LOG2E
        bcol[s, slot] = jnp.broadcast_to(col, (n_own, 128))
        return col

    def x_tile(s, tile):
        return xg[s, pl.ds(pl.multiple_of(tile * TP, TP), TP), :]

    def e_tile(s, slot, t, tile):
        a = dot_t(mub[s, slot], x_tile(s, tile))
        l2 = a * (temp_ref[t] * (2.0 * LOG2E)) + twice(bcol[s, slot])
        m = jnp.max(l2, axis=0, keepdims=True)
        e = jnp.exp2(l2 - m)
        return e, m, m + jnp.log(jnp.sum(e, axis=0, keepdims=True)) * LOG2E

    def tiles_of(half_id):
        return [(2 * half_id + k // bt, k % bt) for k in range(2 * bt)]

    def e_step(s, t, idx, hook=None, early=None):
        def body(i, _):
            h = (1 - c) + i * (2 * c - 1)
            for b, u in tiles_of(h):
                e, m, l = e_tile(s, r, t, b * bt + u)
                e_buf[s, b * bt + u] = e
                m_buf[s, b, u:u + 1, :] = m
                l_buf[s, b, u:u + 1, :] = l

            @pl.when(i == 0)
            def _():
                pre(idx).start()

            if hook is not None:
                hook(i)
            return 0

        lax.fori_loop(0, 2, body, 0)
        if early is not None:
            early()
        p2(idx)

    def acc_zero():
        s_acc[...] = jnp.zeros_like(s_acc)
        n_acc[...] = jnp.zeros_like(n_acc)

    def acc_tiles(s, tiles, resp_of):
        dots, ns = [], []
        for b, u in tiles:
            resp = resp_of(b, u)
            ns.append(resp[:, :128] + resp[:, 128:])
            dots.append(jnp.dot(resp.astype(jnp.bfloat16), x_tile(s, b * bt + u), preferred_element_type=jnp.float32))
        s_acc[...] += functools.reduce(jnp.add, dots)
        n_acc[...] += functools.reduce(jnp.add, ns)

    def m_step(s, t):
        idx = 2 * t + s
        acc_zero()

        def body(i, _):
            @pl.when(i == 1)
            def _():
                post(idx).wait()

            def resp_of(b, u):
                f = jnp.exp2(m_buf[s, b, u:u + 1, :] - tot_buf[idx, b, u:u + 1, :])
                return e_buf[s, b * bt + u] * f

            acc_tiles(s, tiles_of((1 - c) + i * (2 * c - 1)), resp_of)
            return 0

        lax.fori_loop(0, 2, body, 0)

    def mr_half(s, slot, t, half_id):
        idx = 2 * t + s

        def resp_of(b, u):
            a = dot_t(mub[s, slot], x_tile(s, b * bt + u))
            return jnp.exp2(a * (temp_ref[t] * (2.0 * LOG2E)) + twice(bcol[s, slot]) - tot_buf[idx, b, u:u + 1, :])

        acc_tiles(s, tiles_of(half_id), resp_of)

    def mr_all(s, slot, t):
        for h in range(2):
            mr_half(s, slot, t, h)

    def acc_result():
        cnt = jnp.sum(n_acc[...], axis=1, keepdims=True)
        mean = s_acc[...] * (1.0 / (cnt + EPS_COUNT))
        logw = jnp.log((cnt + PRIOR_ALPHA) / (total_pts + total_comp * PRIOR_ALPHA))
        return mean, logw

    def half(ref, k):
        return ref.at[pl.ds(2 * k, 2)]

    def pre(idx):
        return remote(half(l_buf.at[idx % 2], 1 - c), pre_buf.at[idx], pre_send.at[idx - 2], pre_recv.at[idx - 2], sib)

    def bcast(idx, j):
        k = lax.rem(jnp.where(z < comp_size // 2, n_chips - j, j), n_chips)
        q = lax.rem(chip + k, n_chips)
        return remote(bc_src.at[idx], bc_buf.at[idx, k], bc_send.at[idx - 2], bc_recv.at[idx - 2],
                      {"comp": q // y_size, "row": (q % y_size) * CORES + (1 - c)})

    def post(idx):
        return same(half(tot_buf.at[idx], 1 - c), post_send.at[idx - 2], post_recv.at[idx - 2], sib)

    def p2(idx):
        pre(idx).wait()
        bc_src[idx] = lse2_parts([l_buf[idx % 2, pl.ds(2 * c, 2)], pre_buf[idx]])
        for j in range(1, n_chips + 1):
            bcast(idx, j).start()

    def p3(idx):
        same(bc_buf.at[idx], bc_send.at[idx - 2], bc_recv.at[idx - 2], sib).wait()
        tot_buf[idx, pl.ds(2 * (1 - c), 2)] = lse2_parts([bc_buf[idx, k] for k in range(n_chips)])
        post(idx).start()

    def zl(s, k):
        return remote(zl_src.at[s], zl_buf.at[s, k - 1], zl_send.at[s], zl_recv.at[s],
                      {"comp": lax.rem(z + k, comp_size)})

    def ag(s, k):
        return same(tot_buf.at[s, r], ag_send.at[s], ag_recv.at[s], (sib, yn, yd)[k])

    def orig_fit(s, _):
        def orig_slots(p, _):
            for k in range(2):
                q = 2 * p + k
                off = pl.multiple_of(q * n_own, n_own)
                set_params(s, q, mu_all[s, pl.ds(off, n_own), :], row_to_col(lp_ref[pl.ds(s, 1), pl.ds(off, n_own)]), 0)
                for u in range(bt):
                    _, _, l = e_tile(s, q, 0, r * bt + u)
                    lq_buf[q, u:u + 1, :] = l

            @pl.when(jnp.logical_and(s == 0, p == 0))
            def _():
                pl.semaphore_wait(near_sem, 3 + n_z)
                signal_z(far_sem)

            @pl.when(s == 1)
            def _():
                y_steps(1 + 2 * p, 3 + 2 * p)

            return 0

        lax.fori_loop(0, row_size // 2, orig_slots, 0)
        zl_src[s] = lse2_parts([lq_buf[q] for q in range(row_size)])

        @pl.when(s == 0)
        def _():
            pl.semaphore_wait(far_sem, n_z)

        for k in range(1, comp_size):
            zl(s, k).start()

        @pl.when(s == 0)
        def _():
            y_steps(0, 1)

        return 0

    lax.fori_loop(0, 2, orig_fit, 0)

    def y_sends(a, b):
        def send(j, _):
            y_out(j).start()
            return 0

        lax.fori_loop(a, b, send, 0)

    def comb(s):
        same(zl_buf.at[s], zl_send.at[s], zl_recv.at[s], sib).wait()
        tot_buf[s, r] = lse2_parts([zl_src[s]] + [zl_buf[s, k] for k in range(comp_size - 1)])
        for k in range(3):
            ag(s, k).start()

    early = ND + 3
    y_sends(ND, early)
    y_steps(5, 6)
    comb(0)
    y_sends(early, 2 * ND)
    y_steps(6, 8)
    z_steps(0, 4)
    y_steps(8, 9)
    z_steps(4, 5)
    y_steps(9, 10)
    z_steps(5, 6)
    comb(1)
    y_steps(10, 11)
    z_steps(6, 7)
    y_steps(11, 12)

    def sweep0(s, _):
        same(tot_buf.at[s, pl.ds(0, 3)], ag_send.at[s], ag_recv.at[s], sib).wait()
        own_out(s).wait_recv()
        acc_zero()

        def body(k, _):
            @pl.when(jnp.logical_and(s == 0, k == 1))
            def _():
                y_steps(12, 14)
                sib_waits(0)
                y_steps(14, 15)

            @pl.when(jnp.logical_and(s == 1, k == 1))
            def _():
                z_steps(12, 14)
                sib_waits(1)

            mr_half(s, r, 0, y + k * (1 - 2 * y))

            @pl.when(jnp.logical_and(s == 0, k == 1))
            def _():
                y_steps(15, 16)
                z_steps(7, 10)

            return 0

        lax.fori_loop(0, 2, body, 0)
        mean, logw = acc_result()
        set_params(s, r, mean, logw, 1)

        def hook(i):
            @pl.when(jnp.logical_and(s == 0, i == 0))
            def _():
                y_steps(16, 17)

        def first_p3():
            @pl.when(s == 1)
            def _():
                p3(2)

        e_step(s, 1, 2 + s, hook, first_p3)

        @pl.when(s == 0)
        def _():
            y_steps(17, 18)
            z_steps(10, 12)

        return 0

    lax.fori_loop(0, 2, sweep0, 0)

    def mx(s):
        return same(mub.at[s, r], mx_send.at[s], mx_recv.at[s], yn)

    def br(s):
        return same(brow.at[s, r], br_send.at[s], br_recv.at[s], yn)

    def mean_rows(slot, s):
        return mu_out.at[s, pl.ds(pl.multiple_of(slot * n_own, n_own), n_own), :]

    def fin(slot, s, k):
        return same(mean_rows(slot, s), fin_send.at[s, k], fin_recv.at[s, k], sib)

    def lpf(slot, k):
        return same(lp_fin.at[slot], lpf_send.at[k], lpf_recv.at[k], sib)

    def sweep(i, _):
        t, s = i // 2, i % 2
        last = t == sweeps - 1
        m_step(s, t)
        mean, logw = acc_result()

        @pl.when(t < sweeps - 1)
        def _():
            col = set_params(s, r, mean, logw, t + 1)

            @pl.when(t == sweeps - 2)
            def _():
                brow[s, r] = col_to_row(col)

            e_step(s, t + 1, i + 2, early=lambda: p3(i + 1))

            @pl.when(t == sweeps - 2)
            def _():
                mx(s).start()
                br(s).start()

        @pl.when(last)
        def _():
            mean_rows(r, s)[...] = mean
            lp_fin[r, pl.ds(s, 1), :] = col_to_row(logw)
            fin(r, s, 0).start()
            mx(s).wait()
            br(s).wait()
            bcol[s, ry] = jnp.broadcast_to(row_to_col(brow[s, ry]), (n_own, 128))
            acc_zero()

            mr_all(s, ry, t)
            mean2, logw2 = acc_result()
            mean_rows(ry, s)[...] = mean2
            lp_fin[ry, pl.ds(s, 1), :] = col_to_row(logw2)
            fin(ry, s, 1).start()

            @pl.when(s == 0)
            def _():
                p3(i + 1)

        return 0

    lax.fori_loop(2, 2 * sweeps, sweep, 0)
    lpf(r, 0).start()
    lpf(ry, 1).start()

    ones = jnp.ones((8, half_dim), jnp.bfloat16)

    def sq_norms(s, _):
        for u in range(bt):
            x = x_tile(s, r * bt + u).astype(jnp.float32)
            sq = x * x
            hi = sq.astype(jnp.bfloat16)
            lo = (sq - hi.astype(jnp.float32)).astype(jnp.bfloat16)
            sq_buf[s, u:u + 1, :] = (dot_t(ones, hi) + dot_t(ones, lo))[0:1]
        return 0

    lax.fori_loop(0, 2, sq_norms, 0)
    for s in range(2):
        gather_sends_wait(s)

    t = sweeps - 1
    for s in range(2):
        for j in range(bt):
            lse_out[s:s + 1, j * TP:(j + 1) * TP] = (
                tot_buf[2 * t + s, r, j:j + 1, :] * LN2 - temp_ref[t] * sq_buf[s, j:j + 1, :])

    for k in range(2):
        for s in range(2):
            fin((r, ry)[k], s, k).wait()
    lpf(r, 0).wait()
    lpf(ry, 1).wait()
    for q in range(row_size):
        lp_out[:, q * n_own:(q + 1) * n_own] = lp_fin[q]


def solution(mesh):
    comp_size = mesh.shape["comp"]
    row_size = mesh.shape["row"]

    def local_fit(x_local, mu_init, logpi_init, inv_temp):
        block, dim = x_local.shape
        half_dim = dim // 2
        n_local = mu_init.shape[1]
        n_own = n_local // row_size
        total_pts = block * row_size
        tiles = total_pts // TP
        sweeps = inv_temp.shape[0]
        n_chips = comp_size * row_size // CORES
        ni = 2 * sweeps
        bt = block // TP
        f32, bf16 = jnp.float32, jnp.bfloat16
        dma = pltpu.SemaphoreType.DMA
        vm = pltpu.VMEM
        scratch = [
            pltpu.SMEM((sweeps,), f32), vm((2, n_local), f32),
            vm((2, total_pts, half_dim), bf16),
            vm((2, n_local, half_dim), f32),
            vm((2, row_size, n_own, half_dim), bf16),
            vm((2, row_size, n_own, 128), f32),
            vm((2, row_size, 1, n_own), f32),
            vm((2, tiles, n_own, TP), f32),
            vm((2, row_size, bt, TP), f32),
            vm((2, row_size, bt, TP), f32),
            vm((row_size, bt, TP), f32),
            vm((n_own, half_dim), f32),
            vm((n_own, 128), f32),
            vm((row_size, 2, n_own), f32),
            vm((2, bt, TP), f32),
            vm((2, bt, TP), f32),
            vm((2, comp_size - 1, bt, TP), f32),
            vm((ni, 2, bt, TP), f32),
            vm((ni, 2, bt, TP), f32),
            vm((ni, n_chips, 2, bt, TP), f32),
            vm((ni, row_size, bt, TP), f32),
            dma((6,)), pltpu.SemaphoreType.REGULAR, pltpu.SemaphoreType.REGULAR,
            dma((1,)), dma((2 * ND,)), dma((2 * NR,)), dma((2,)), dma((2,)), dma((2,)),
            dma((2,)), dma((2,)), dma((2,)), dma((2,)),
            dma((ni - 2,)), dma((ni - 2,)), dma((ni - 2,)), dma((ni - 2,)), dma((ni - 2,)), dma((ni - 2,)),
            dma((2,)), dma((2,)), dma((2,)), dma((2,)),
            dma((2, 2)), dma((2, 2)), dma((2,)), dma((2,)),
        ]
        outs = pl.pallas_call(
            functools.partial(em_kernel, comp_size, row_size, sweeps),
            out_shape=(vm((2, n_local, half_dim), f32), vm((2, n_local), f32), vm((2, block), f32)),
            in_specs=[
                pl.BlockSpec(memory_space=pl.ANY),
            ] * 4,
            out_specs=(pl.BlockSpec(memory_space=pltpu.VMEM),) * 3,
            scratch_shapes=scratch,
            compiler_params=pltpu.CompilerParams(
                collective_id=0, has_side_effects=True, vmem_limit_bytes=56 * 1024 * 1024),
        )(inv_temp, logpi_init, x_local, mu_init)
        return pl.pallas_call(
            write_kernel,
            out_shape=tuple(jax.ShapeDtypeStruct(o.shape, o.dtype) for o in outs),
            in_specs=[pl.BlockSpec(memory_space=pltpu.VMEM)] * 3,
            out_specs=(pl.BlockSpec(memory_space=pl.ANY),) * 3,
            scratch_shapes=[dma((3,))],
        )(*[pltpu.with_memory_space_constraint(o, pltpu.VMEM) for o in outs])

    return jax.shard_map(
        local_fit,
        mesh=mesh,
        in_specs=(P(("grp", "row"), None), P(None, ("grp", "comp"), None), P(None, ("grp", "comp")), P()),
        out_specs=(P(None, ("grp", "comp"), None), P(None, ("grp", "comp")), P(None, ("grp", "row"))),
        check_vma=False,
    )
```

```python
import functools

import jax
import jax.numpy as jnp
from jax import lax
from jax.experimental import pallas as pl
from jax.experimental.pallas import tpu as pltpu
from jax.sharding import PartitionSpec as P

EPS_COUNT = 1e-6
PRIOR_ALPHA = 1e-3
LOG2E = 1.4426950408889634
LN2 = 0.6931471805599453
MESH = pl.DeviceIdType.MESH

CORES = 2
TP = 256
NCK = 16
ND = 10
NR = NCK - ND


def lse2_parts(parts):
    top = functools.reduce(jnp.maximum, parts)
    total = functools.reduce(jnp.add, [jnp.exp2(p - top) for p in parts])
    return top + jnp.log(total) * LOG2E


def dot_t(a, b):
    return lax.dot_general(a, b, (((1,), (1,)), ((), ())), preferred_element_type=jnp.float32)


def eye_mask(n):
    return lax.broadcasted_iota(jnp.int32, (n, n), 0) == lax.broadcasted_iota(jnp.int32, (n, n), 1)


def col_to_row(col):
    return jnp.sum(jnp.where(eye_mask(col.shape[0]), col, 0.0), axis=0, keepdims=True)


def row_to_col(row):
    return jnp.sum(jnp.where(eye_mask(row.shape[1]), row, 0.0), axis=1, keepdims=True)


def twice(b):
    return jnp.concatenate([b, b], axis=1)


def write_kernel(a, b, c, a_out, b_out, c_out, sems):
    n = a.shape[1] // 4
    pairs = [(a.at[s, pl.ds(q * n, n), :], a_out.at[s, pl.ds(q * n, n), :]) for s in range(2) for q in range(4)]
    pairs += [(b, b_out), (c, c_out)]
    copies = [pltpu.make_async_copy(v, o, sems.at[k]) for k, (v, o) in enumerate(pairs)]
    for cp in copies:
        cp.start()
    for cp in copies:
        cp.wait()


def em_kernel(
    comp_size, row_size, sweeps,
    temp_hbm, lp_hbm, x_hbm, mu_hbm,
    mu_out, lp_out, lse_out,
    temp_ref, lp_ref, xg, mu_all, mub, bcol, brow, e_buf, m_buf, l_buf, lq_buf, s_acc, n_acc, lp_fin, sq_buf,
    zl_src, zl_buf, pre_buf, bc_src, bc_buf, tot_buf,
    load_sem, near_sem, far_sem, g_send, y_recv, z_recv, sy_recv, sz_recv, own_recv,
    zl_send, zl_recv, ag_send, ag_recv,
    pre_send, pre_recv, bc_send, bc_recv, post_send, post_recv,
    mx_send, mx_recv, br_send, br_recv, fin_send, fin_recv, lpf_send, lpf_recv,
):
    z = lax.axis_index("comp")
    r = lax.axis_index("row")
    y, c = r // CORES, r % CORES
    n_chips = comp_size * row_size // CORES
    y_size = row_size // CORES
    chip = z * y_size + y
    block = x_hbm.shape[0]
    half_dim = x_hbm.shape[1] // 2
    total_pts = block * row_size
    n_own = mub.shape[2]
    total_comp = mu_hbm.shape[1] * comp_size
    bt = block // TP
    ch = block // NCK
    rs = y * CORES + (1 - c)
    ry = (1 - y) * CORES + c
    sib = {"row": rs}
    yn = {"row": ry}
    rx = (1 - y) * CORES + (1 - c)
    yd = {"row": rx}
    zx = {"comp": z + 1 - 2 * (z % 2), "row": rs}
    hz = z % 2

    def remote(src, dst, send, recv, dev):
        return pltpu.make_async_remote_copy(
            src_ref=src, dst_ref=dst, send_sem=send, recv_sem=recv, device_id=dev, device_id_type=MESH)

    def same(v, send, recv, dev):
        return remote(v, v, send, recv, dev)

    x_loads = [pltpu.make_async_copy(
        x_hbm.at[:, pl.ds(s * half_dim, half_dim)], xg.at[s, pl.ds(r * block, block), :], load_sem.at[s])
        for s in range(2)]
    mu_loads = [pltpu.make_async_copy(mu_hbm.at[s], mu_all.at[s], load_sem.at[2 + s]) for s in range(2)]
    small_loads = [pltpu.make_async_copy(temp_hbm, temp_ref, load_sem.at[4]),
                   pltpu.make_async_copy(lp_hbm, lp_ref, load_sem.at[5])]
    for cp in x_loads + small_loads:
        cp.start()

    n_z = (z > 0).astype(jnp.int32) + (z < comp_size - 1).astype(jnp.int32)

    def signal_z(sem):
        @pl.when(z > 0)
        def _():
            pl.semaphore_signal(sem, inc=1, device_id={"comp": z - 1}, device_id_type=MESH)

        @pl.when(z < comp_size - 1)
        def _():
            pl.semaphore_signal(sem, inc=1, device_id={"comp": z + 1}, device_id_type=MESH)

    def signal_near(sem):
        for dev in (sib, yn, yd):
            pl.semaphore_signal(sem, inc=1, device_id=dev, device_id_type=MESH)
        signal_z(sem)

    barrier = pltpu.get_barrier_semaphore()
    signal_near(barrier)
    pl.semaphore_wait(barrier, 3 + n_z)
    signal_near(near_sem)
    for cp in mu_loads:
        cp.start()

    def xrows(s, blk, cid):
        return xg.at[s, pl.ds(pl.multiple_of(blk * block + cid * ch, ch), ch), :]

    def cid_y(k):
        return k + hz * (NCK - 1 - 2 * k)

    def cid_z(k):
        return k + (1 - hz) * (NCK - 1 - 2 * k)

    def y_out(j):
        return same(xrows(j // ND, r, cid_y(j % ND)), g_send.at[0], y_recv.at[j], yd)

    def z_fwd(m):
        return same(xrows(m // NR, rx, cid_y(m % NR)), g_send.at[0], z_recv.at[m], zx)

    def sy_fwd(j):
        return same(xrows(j // ND, rx, cid_y(j % ND)), g_send.at[0], sy_recv.at[j // ND], sib)

    def sz_fwd(m):
        return same(xrows(m // NR, ry, cid_z(m % NR)), g_send.at[0], sz_recv.at[m // NR], sib)

    def own_out(s):
        return same(xg.at[s, pl.ds(r * block, block), :], g_send.at[0], own_recv.at[s], sib)

    def y_steps(a, b):
        def body(j, _):
            y_out(j).wait_recv()

            @pl.when(j % ND < NR)
            def _():
                z_fwd(j // ND * NR + j % ND).start()

            sy_fwd(j).start()
            return 0

        lax.fori_loop(a, b, body, 0)

    def z_steps(a, b):
        def body(m, _):
            z_fwd(m).wait_recv()
            sz_fwd(m).start()
            return 0

        lax.fori_loop(a, b, body, 0)

    def rows_of(s, chunks):
        return xg.at[s, pl.ds(0, chunks * ch), :]

    def sib_waits(s):
        same(rows_of(s, ND), g_send.at[0], sy_recv.at[s], sib).wait_recv()
        same(rows_of(s, NR), g_send.at[0], sz_recv.at[s], sib).wait_recv()

    def gather_sends_wait(s):
        for chunks in (ND, NR, ND, NR):
            same(rows_of(s, chunks), g_send.at[0], sy_recv.at[s], sib).wait_send()
        own_out(s).wait_send()

    x_loads[0].wait()
    for j in range(ND):
        y_out(j).start()
    own_out(0).start()
    x_loads[1].wait()
    own_out(1).start()
    for cp in mu_loads + small_loads:
        cp.wait()

    def set_params(s, slot, mean, logw, t):
        mub[s, slot] = mean.astype(jnp.bfloat16)
        mu_sq = jnp.sum(mean * mean, axis=1, keepdims=True)
        col = (logw - temp_ref[t] * mu_sq) * LOG2E
        bcol[s, slot] = jnp.broadcast_to(col, (n_own, 128))
        return col

    def x_tile(s, tile):
        return xg[s, pl.ds(pl.multiple_of(tile * TP, TP), TP), :]

    def e_tile(s, slot, t, tile):
        a = dot_t(mub[s, slot], x_tile(s, tile))
        l2 = a * (temp_ref[t] * (2.0 * LOG2E)) + twice(bcol[s, slot])
        m = jnp.max(l2, axis=0, keepdims=True)
        e = jnp.exp2(l2 - m)
        return e, m, m + jnp.log(jnp.sum(e, axis=0, keepdims=True)) * LOG2E

    def tiles_of(half_id):
        return [(2 * half_id + k // bt, k % bt) for k in range(2 * bt)]

    def e_step(s, t, idx, hook=None, early=None):
        def body(i, _):
            h = (1 - c) + i * (2 * c - 1)
            for b, u in tiles_of(h):
                e, m, l = e_tile(s, r, t, b * bt + u)
                e_buf[s, b * bt + u] = e
                m_buf[s, b, u:u + 1, :] = m
                l_buf[s, b, u:u + 1, :] = l

            @pl.when(i == 0)
            def _():
                pre(idx).start()

            if hook is not None:
                hook(i)
            return 0

        lax.fori_loop(0, 2, body, 0)
        if early is not None:
            early()
        p2(idx)

    def acc_zero():
        s_acc[...] = jnp.zeros_like(s_acc)
        n_acc[...] = jnp.zeros_like(n_acc)

    def acc_tiles(s, tiles, resp_of):
        dots, ns = [], []
        for b, u in tiles:
            resp = resp_of(b, u)
            ns.append(resp[:, :128] + resp[:, 128:])
            dots.append(jnp.dot(resp.astype(jnp.bfloat16), x_tile(s, b * bt + u), preferred_element_type=jnp.float32))
        s_acc[...] += functools.reduce(jnp.add, dots)
        n_acc[...] += functools.reduce(jnp.add, ns)

    def m_step(s, t):
        idx = 2 * t + s
        acc_zero()

        def body(i, _):
            @pl.when(i == 1)
            def _():
                post(idx).wait()

            def resp_of(b, u):
                f = jnp.exp2(m_buf[s, b, u:u + 1, :] - tot_buf[idx, b, u:u + 1, :])
                return e_buf[s, b * bt + u] * f

            acc_tiles(s, tiles_of((1 - c) + i * (2 * c - 1)), resp_of)
            return 0

        lax.fori_loop(0, 2, body, 0)

    def mr_half(s, slot, t, half_id):
        idx = 2 * t + s

        def resp_of(b, u):
            a = dot_t(mub[s, slot], x_tile(s, b * bt + u))
            return jnp.exp2(a * (temp_ref[t] * (2.0 * LOG2E)) + twice(bcol[s, slot]) - tot_buf[idx, b, u:u + 1, :])

        acc_tiles(s, tiles_of(half_id), resp_of)

    def mr_all(s, slot, t):
        for h in range(2):
            mr_half(s, slot, t, h)

    def acc_result():
        cnt = jnp.sum(n_acc[...], axis=1, keepdims=True)
        mean = s_acc[...] * (1.0 / (cnt + EPS_COUNT))
        logw = jnp.log((cnt + PRIOR_ALPHA) / (total_pts + total_comp * PRIOR_ALPHA))
        return mean, logw

    def half(ref, k):
        return ref.at[pl.ds(2 * k, 2)]

    def pre(idx):
        return remote(half(l_buf.at[idx % 2], 1 - c), pre_buf.at[idx], pre_send.at[idx - 2], pre_recv.at[idx - 2], sib)

    def bcast(idx, j):
        k = lax.rem(jnp.where(z < comp_size // 2, n_chips - j, j), n_chips)
        q = lax.rem(chip + k, n_chips)
        return remote(bc_src.at[idx], bc_buf.at[idx, k], bc_send.at[idx - 2], bc_recv.at[idx - 2],
                      {"comp": q // y_size, "row": (q % y_size) * CORES + (1 - c)})

    def post(idx):
        return same(half(tot_buf.at[idx], 1 - c), post_send.at[idx - 2], post_recv.at[idx - 2], sib)

    def p2(idx):
        pre(idx).wait()
        bc_src[idx] = lse2_parts([l_buf[idx % 2, pl.ds(2 * c, 2)], pre_buf[idx]])
        for j in range(1, n_chips + 1):
            bcast(idx, j).start()

    def p3(idx):
        same(bc_buf.at[idx], bc_send.at[idx - 2], bc_recv.at[idx - 2], sib).wait()
        tot_buf[idx, pl.ds(2 * (1 - c), 2)] = lse2_parts([bc_buf[idx, k] for k in range(n_chips)])
        post(idx).start()

    def zl(s, k):
        return remote(zl_src.at[s], zl_buf.at[s, k - 1], zl_send.at[s], zl_recv.at[s],
                      {"comp": lax.rem(z + k, comp_size)})

    def ag(s, k):
        return same(tot_buf.at[s, r], ag_send.at[s], ag_recv.at[s], (sib, yn, yd)[k])

    def orig_fit(s, _):
        def orig_slots(p, _):
            for k in range(2):
                q = 2 * p + k
                off = pl.multiple_of(q * n_own, n_own)
                set_params(s, q, mu_all[s, pl.ds(off, n_own), :], row_to_col(lp_ref[pl.ds(s, 1), pl.ds(off, n_own)]), 0)
                for u in range(bt):
                    _, _, l = e_tile(s, q, 0, r * bt + u)
                    lq_buf[q, u:u + 1, :] = l

            @pl.when(jnp.logical_and(s == 0, p == 0))
            def _():
                pl.semaphore_wait(near_sem, 3 + n_z)
                signal_z(far_sem)

            @pl.when(s == 1)
            def _():
                y_steps(1 + 2 * p, 3 + 2 * p)

            return 0

        lax.fori_loop(0, row_size // 2, orig_slots, 0)
        zl_src[s] = lse2_parts([lq_buf[q] for q in range(row_size)])

        @pl.when(s == 0)
        def _():
            pl.semaphore_wait(far_sem, n_z)

        for k in range(1, comp_size):
            zl(s, k).start()

        @pl.when(s == 0)
        def _():
            y_steps(0, 1)

        return 0

    lax.fori_loop(0, 2, orig_fit, 0)

    def y_sends(a, b):
        def send(j, _):
            y_out(j).start()
            return 0

        lax.fori_loop(a, b, send, 0)

    def comb(s):
        same(zl_buf.at[s], zl_send.at[s], zl_recv.at[s], sib).wait()
        tot_buf[s, r] = lse2_parts([zl_src[s]] + [zl_buf[s, k] for k in range(comp_size - 1)])
        for k in range(3):
            ag(s, k).start()

    early = ND + 3
    y_sends(ND, early)
    y_steps(5, 6)
    comb(0)
    y_sends(early, 2 * ND)
    y_steps(6, 8)
    z_steps(0, 4)
    y_steps(8, 9)
    z_steps(4, 5)
    y_steps(9, 10)
    z_steps(5, 6)
    comb(1)
    y_steps(10, 12)

    def sweep0(s, _):
        same(tot_buf.at[s, pl.ds(0, 3)], ag_send.at[s], ag_recv.at[s], sib).wait()
        own_out(s).wait_recv()
        acc_zero()

        def body(k, _):
            @pl.when(jnp.logical_and(s == 0, k == 1))
            def _():
                y_steps(12, 14)
                sib_waits(0)
                y_steps(14, 15)

            @pl.when(jnp.logical_and(s == 1, k == 1))
            def _():
                z_steps(11, 12)
                y_steps(19, 20)
                sib_waits(1)

            mr_half(s, r, 0, y + k * (1 - 2 * y))

            @pl.when(jnp.logical_and(s == 0, k == 1))
            def _():
                y_steps(15, 16)
                z_steps(6, 9)

            return 0

        lax.fori_loop(0, 2, body, 0)
        mean, logw = acc_result()
        set_params(s, r, mean, logw, 1)

        def hook(i):
            @pl.when(jnp.logical_and(s == 0, i == 0))
            def _():
                y_steps(16, 17)

        def first_p3():
            @pl.when(s == 1)
            def _():
                p3(2)

        e_step(s, 1, 2 + s, hook, first_p3)

        @pl.when(s == 0)
        def _():
            y_steps(17, 19)
            z_steps(9, 11)

        return 0

    lax.fori_loop(0, 2, sweep0, 0)

    def mx(s):
        return same(mub.at[s, r], mx_send.at[s], mx_recv.at[s], yn)

    def br(s):
        return same(brow.at[s, r], br_send.at[s], br_recv.at[s], yn)

    def mean_rows(slot, s):
        return mu_out.at[s, pl.ds(pl.multiple_of(slot * n_own, n_own), n_own), :]

    def fin(slot, s, k):
        return same(mean_rows(slot, s), fin_send.at[s, k], fin_recv.at[s, k], sib)

    def lpf(slot, k):
        return same(lp_fin.at[slot], lpf_send.at[k], lpf_recv.at[k], sib)

    def sweep(i, _):
        t, s = i // 2, i % 2
        last = t == sweeps - 1
        m_step(s, t)
        mean, logw = acc_result()

        @pl.when(t < sweeps - 1)
        def _():
            col = set_params(s, r, mean, logw, t + 1)

            @pl.when(t == sweeps - 2)
            def _():
                brow[s, r] = col_to_row(col)

            e_step(s, t + 1, i + 2, early=lambda: p3(i + 1))

            @pl.when(t == sweeps - 2)
            def _():
                mx(s).start()
                br(s).start()

        @pl.when(last)
        def _():
            mean_rows(r, s)[...] = mean
            lp_fin[r, pl.ds(s, 1), :] = col_to_row(logw)
            fin(r, s, 0).start()
            mx(s).wait()
            br(s).wait()
            bcol[s, ry] = jnp.broadcast_to(row_to_col(brow[s, ry]), (n_own, 128))
            acc_zero()

            mr_all(s, ry, t)
            mean2, logw2 = acc_result()
            mean_rows(ry, s)[...] = mean2
            lp_fin[ry, pl.ds(s, 1), :] = col_to_row(logw2)
            fin(ry, s, 1).start()

            @pl.when(s == 0)
            def _():
                p3(i + 1)

        return 0

    lax.fori_loop(2, 2 * sweeps, sweep, 0)
    lpf(r, 0).start()
    lpf(ry, 1).start()

    ones = jnp.ones((8, half_dim), jnp.bfloat16)

    def sq_norms(s, _):
        for u in range(bt):
            x = x_tile(s, r * bt + u).astype(jnp.float32)
            sq = x * x
            hi = sq.astype(jnp.bfloat16)
            lo = (sq - hi.astype(jnp.float32)).astype(jnp.bfloat16)
            sq_buf[s, u:u + 1, :] = (dot_t(ones, hi) + dot_t(ones, lo))[0:1]
        return 0

    lax.fori_loop(0, 2, sq_norms, 0)
    for s in range(2):
        gather_sends_wait(s)

    t = sweeps - 1
    for s in range(2):
        for j in range(bt):
            lse_out[s:s + 1, j * TP:(j + 1) * TP] = (
                tot_buf[2 * t + s, r, j:j + 1, :] * LN2 - temp_ref[t] * sq_buf[s, j:j + 1, :])

    for k in range(2):
        for s in range(2):
            fin((r, ry)[k], s, k).wait()
    lpf(r, 0).wait()
    lpf(ry, 1).wait()
    for q in range(row_size):
        lp_out[:, q * n_own:(q + 1) * n_own] = lp_fin[q]


def solution(mesh):
    comp_size = mesh.shape["comp"]
    row_size = mesh.shape["row"]

    def local_fit(x_local, mu_init, logpi_init, inv_temp):
        block, dim = x_local.shape
        half_dim = dim // 2
        n_local = mu_init.shape[1]
        n_own = n_local // row_size
        total_pts = block * row_size
        tiles = total_pts // TP
        sweeps = inv_temp.shape[0]
        n_chips = comp_size * row_size // CORES
        ni = 2 * sweeps
        bt = block // TP
        f32, bf16 = jnp.float32, jnp.bfloat16
        dma = pltpu.SemaphoreType.DMA
        vm = pltpu.VMEM
        scratch = [
            pltpu.SMEM((sweeps,), f32), vm((2, n_local), f32),
            vm((2, total_pts, half_dim), bf16),
            vm((2, n_local, half_dim), f32),
            vm((2, row_size, n_own, half_dim), bf16),
            vm((2, row_size, n_own, 128), f32),
            vm((2, row_size, 1, n_own), f32),
            vm((2, tiles, n_own, TP), f32),
            vm((2, row_size, bt, TP), f32),
            vm((2, row_size, bt, TP), f32),
            vm((row_size, bt, TP), f32),
            vm((n_own, half_dim), f32),
            vm((n_own, 128), f32),
            vm((row_size, 2, n_own), f32),
            vm((2, bt, TP), f32),
            vm((2, bt, TP), f32),
            vm((2, comp_size - 1, bt, TP), f32),
            vm((ni, 2, bt, TP), f32),
            vm((ni, 2, bt, TP), f32),
            vm((ni, n_chips, 2, bt, TP), f32),
            vm((ni, row_size, bt, TP), f32),
            dma((6,)), pltpu.SemaphoreType.REGULAR, pltpu.SemaphoreType.REGULAR,
            dma((1,)), dma((2 * ND,)), dma((2 * NR,)), dma((2,)), dma((2,)), dma((2,)),
            dma((2,)), dma((2,)), dma((2,)), dma((2,)),
            dma((ni - 2,)), dma((ni - 2,)), dma((ni - 2,)), dma((ni - 2,)), dma((ni - 2,)), dma((ni - 2,)),
            dma((2,)), dma((2,)), dma((2,)), dma((2,)),
            dma((2, 2)), dma((2, 2)), dma((2,)), dma((2,)),
        ]
        outs = pl.pallas_call(
            functools.partial(em_kernel, comp_size, row_size, sweeps),
            out_shape=(vm((2, n_local, half_dim), f32), vm((2, n_local), f32), vm((2, block), f32)),
            in_specs=[
                pl.BlockSpec(memory_space=pl.ANY),
            ] * 4,
            out_specs=(pl.BlockSpec(memory_space=pltpu.VMEM),) * 3,
            scratch_shapes=scratch,
            compiler_params=pltpu.CompilerParams(
                collective_id=0, has_side_effects=True, vmem_limit_bytes=56 * 1024 * 1024),
        )(inv_temp, logpi_init, x_local, mu_init)
        return pl.pallas_call(
            write_kernel,
            out_shape=tuple(jax.ShapeDtypeStruct(o.shape, o.dtype) for o in outs),
            in_specs=[pl.BlockSpec(memory_space=pltpu.VMEM)] * 3,
            out_specs=(pl.BlockSpec(memory_space=pl.ANY),) * 3,
            scratch_shapes=[dma((10,))],
        )(*[pltpu.with_memory_space_constraint(o, pltpu.VMEM) for o in outs])

    return jax.shard_map(
        local_fit,
        mesh=mesh,
        in_specs=(P(("grp", "row"), None), P(None, ("grp", "comp"), None), P(None, ("grp", "comp")), P()),
        out_specs=(P(None, ("grp", "comp"), None), P(None, ("grp", "comp")), P(None, ("grp", "row"))),
        check_vma=False,
    )
```

```python
import functools

import jax
import jax.numpy as jnp
from jax import lax
from jax.experimental import pallas as pl
from jax.experimental.pallas import tpu as pltpu
from jax.sharding import PartitionSpec as P

EPS_COUNT = 1e-6
PRIOR_ALPHA = 1e-3
LOG2E = 1.4426950408889634
LN2 = 0.6931471805599453
MESH = pl.DeviceIdType.MESH

CORES = 2
TP = 256
NCK = 16
ND = 9
NR = NCK - ND


def lse2_parts(parts):
    top = functools.reduce(jnp.maximum, parts)
    total = functools.reduce(jnp.add, [jnp.exp2(p - top) for p in parts])
    return top + jnp.log(total) * LOG2E


def dot_t(a, b):
    return lax.dot_general(a, b, (((1,), (1,)), ((), ())), preferred_element_type=jnp.float32)


def eye_mask(n):
    return lax.broadcasted_iota(jnp.int32, (n, n), 0) == lax.broadcasted_iota(jnp.int32, (n, n), 1)


def col_to_row(col):
    return jnp.sum(jnp.where(eye_mask(col.shape[0]), col, 0.0), axis=0, keepdims=True)


def row_to_col(row):
    return jnp.sum(jnp.where(eye_mask(row.shape[1]), row, 0.0), axis=1, keepdims=True)


def twice(b):
    return jnp.concatenate([b, b], axis=1)


def write_kernel(a, b, c, a_out, b_out, c_out, sems):
    copies = [pltpu.make_async_copy(v, o, sems.at[k]) for k, (v, o) in enumerate(((a, a_out), (b, b_out), (c, c_out)))]
    for cp in copies:
        cp.start()
    for cp in copies:
        cp.wait()


def em_kernel(
    comp_size, row_size, sweeps,
    temp_hbm, lp_hbm, x_hbm, mu_hbm,
    mu_out, lp_out, lse_out,
    temp_ref, lp_ref, xg, mu_all, mub, bcol, brow, e_buf, m_buf, l_buf, lq_buf, s_acc, n_acc, lp_fin, sq_buf,
    zl_src, zl_buf, pre_buf, bc_src, bc_buf, tot_buf,
    load_sem, near_sem, far_sem, g_send, y_recv, z_recv, sy_recv, sz_recv, own_recv,
    zl_send, zl_recv, ag_send, ag_recv,
    pre_send, pre_recv, bc_send, bc_recv, post_send, post_recv,
    mx_send, mx_recv, br_send, br_recv, fin_send, fin_recv, lpf_send, lpf_recv,
):
    z = lax.axis_index("comp")
    r = lax.axis_index("row")
    y, c = r // CORES, r % CORES
    n_chips = comp_size * row_size // CORES
    y_size = row_size // CORES
    chip = z * y_size + y
    block = x_hbm.shape[0]
    half_dim = x_hbm.shape[1] // 2
    total_pts = block * row_size
    n_own = mub.shape[2]
    total_comp = mu_hbm.shape[1] * comp_size
    bt = block // TP
    ch = block // NCK
    rs = y * CORES + (1 - c)
    ry = (1 - y) * CORES + c
    sib = {"row": rs}
    yn = {"row": ry}
    rx = (1 - y) * CORES + (1 - c)
    yd = {"row": rx}
    zx = {"comp": z + 1 - 2 * (z % 2), "row": rs}
    hz = z % 2

    def remote(src, dst, send, recv, dev):
        return pltpu.make_async_remote_copy(
            src_ref=src, dst_ref=dst, send_sem=send, recv_sem=recv, device_id=dev, device_id_type=MESH)

    def same(v, send, recv, dev):
        return remote(v, v, send, recv, dev)

    x_loads = [pltpu.make_async_copy(
        x_hbm.at[:, pl.ds(s * half_dim, half_dim)], xg.at[s, pl.ds(r * block, block), :], load_sem.at[s])
        for s in range(2)]
    mu_loads = [pltpu.make_async_copy(mu_hbm.at[s], mu_all.at[s], load_sem.at[2 + s]) for s in range(2)]
    small_loads = [pltpu.make_async_copy(temp_hbm, temp_ref, load_sem.at[4]),
                   pltpu.make_async_copy(lp_hbm, lp_ref, load_sem.at[5])]
    for cp in x_loads + small_loads:
        cp.start()

    n_z = (z > 0).astype(jnp.int32) + (z < comp_size - 1).astype(jnp.int32)

    def signal_z(sem):
        @pl.when(z > 0)
        def _():
            pl.semaphore_signal(sem, inc=1, device_id={"comp": z - 1}, device_id_type=MESH)

        @pl.when(z < comp_size - 1)
        def _():
            pl.semaphore_signal(sem, inc=1, device_id={"comp": z + 1}, device_id_type=MESH)

    def signal_near(sem):
        for dev in (sib, yn, yd):
            pl.semaphore_signal(sem, inc=1, device_id=dev, device_id_type=MESH)
        signal_z(sem)

    barrier = pltpu.get_barrier_semaphore()
    signal_near(barrier)
    pl.semaphore_wait(barrier, 3 + n_z)
    signal_near(near_sem)
    for cp in mu_loads:
        cp.start()

    def xrows(s, blk, cid):
        return xg.at[s, pl.ds(pl.multiple_of(blk * block + cid * ch, ch), ch), :]

    def cid_y(k):
        return k + hz * (NCK - 1 - 2 * k)

    def cid_z(k):
        return k + (1 - hz) * (NCK - 1 - 2 * k)

    def y_out(j):
        return same(xrows(j // ND, r, cid_y(j % ND)), g_send.at[0], y_recv.at[j], yd)

    def z_fwd(m):
        return same(xrows(m // NR, rx, cid_y(m % NR)), g_send.at[0], z_recv.at[m], zx)

    def sy_fwd(j):
        return same(xrows(j // ND, rx, cid_y(j % ND)), g_send.at[0], sy_recv.at[j // ND], sib)

    def sz_fwd(m):
        return same(xrows(m // NR, ry, cid_z(m % NR)), g_send.at[0], sz_recv.at[m // NR], sib)

    def own_out(s):
        return same(xg.at[s, pl.ds(r * block, block), :], g_send.at[0], own_recv.at[s], sib)

    def y_steps(a, b):
        def body(j, _):
            y_out(j).wait_recv()

            @pl.when(j % ND < NR)
            def _():
                z_fwd(j // ND * NR + j % ND).start()

            sy_fwd(j).start()
            return 0

        lax.fori_loop(a, b, body, 0)

    def z_steps(a, b):
        def body(m, _):
            z_fwd(m).wait_recv()
            sz_fwd(m).start()
            return 0

        lax.fori_loop(a, b, body, 0)

    def rows_of(s, chunks):
        return xg.at[s, pl.ds(0, chunks * ch), :]

    def sib_waits(s):
        same(rows_of(s, ND), g_send.at[0], sy_recv.at[s], sib).wait_recv()
        same(rows_of(s, NR), g_send.at[0], sz_recv.at[s], sib).wait_recv()

    def gather_sends_wait(s):
        for chunks in (ND, NR, ND, NR):
            same(rows_of(s, chunks), g_send.at[0], sy_recv.at[s], sib).wait_send()
        own_out(s).wait_send()

    x_loads[0].wait()
    for j in range(ND):
        y_out(j).start()
    own_out(0).start()
    x_loads[1].wait()
    own_out(1).start()
    for cp in mu_loads + small_loads:
        cp.wait()

    def set_params(s, slot, mean, logw, t):
        mub[s, slot] = mean.astype(jnp.bfloat16)
        mu_sq = jnp.sum(mean * mean, axis=1, keepdims=True)
        col = (logw - temp_ref[t] * mu_sq) * LOG2E
        bcol[s, slot] = jnp.broadcast_to(col, (n_own, 128))
        return col

    def x_tile(s, tile):
        return xg[s, pl.ds(pl.multiple_of(tile * TP, TP), TP), :]

    def e_tile(s, slot, t, tile):
        a = dot_t(mub[s, slot], x_tile(s, tile))
        l2 = a * (temp_ref[t] * (2.0 * LOG2E)) + twice(bcol[s, slot])
        m = jnp.max(l2, axis=0, keepdims=True)
        e = jnp.exp2(l2 - m)
        return e, m, m + jnp.log(jnp.sum(e, axis=0, keepdims=True)) * LOG2E

    def tiles_of(half_id):
        return [(2 * half_id + k // bt, k % bt) for k in range(2 * bt)]

    def e_step(s, t, idx, hook=None, early=None):
        def body(i, _):
            h = (1 - c) + i * (2 * c - 1)
            for b, u in tiles_of(h):
                e, m, l = e_tile(s, r, t, b * bt + u)
                e_buf[s, b * bt + u] = e
                m_buf[s, b, u:u + 1, :] = m
                l_buf[s, b, u:u + 1, :] = l

            @pl.when(i == 0)
            def _():
                pre(idx).start()

            if hook is not None:
                hook(i)
            return 0

        lax.fori_loop(0, 2, body, 0)
        p2(idx)
        if early is not None:
            early()

    def acc_zero():
        s_acc[...] = jnp.zeros_like(s_acc)
        n_acc[...] = jnp.zeros_like(n_acc)

    def acc_tiles(s, tiles, resp_of):
        dots, ns = [], []
        for b, u in tiles:
            resp = resp_of(b, u)
            ns.append(resp[:, :128] + resp[:, 128:])
            dots.append(jnp.dot(resp.astype(jnp.bfloat16), x_tile(s, b * bt + u), preferred_element_type=jnp.float32))
        s_acc[...] += functools.reduce(jnp.add, dots)
        n_acc[...] += functools.reduce(jnp.add, ns)

    def m_step(s, t):
        idx = 2 * t + s
        acc_zero()

        def body(i, _):
            @pl.when(i == 1)
            def _():
                post(idx).wait()

            def resp_of(b, u):
                f = jnp.exp2(m_buf[s, b, u:u + 1, :] - tot_buf[idx, b, u:u + 1, :])
                return e_buf[s, b * bt + u] * f

            acc_tiles(s, tiles_of((1 - c) + i * (2 * c - 1)), resp_of)
            return 0

        lax.fori_loop(0, 2, body, 0)

    def mr_half(s, slot, t, half_id):
        idx = 2 * t + s

        def resp_of(b, u):
            a = dot_t(mub[s, slot], x_tile(s, b * bt + u))
            return jnp.exp2(a * (temp_ref[t] * (2.0 * LOG2E)) + twice(bcol[s, slot]) - tot_buf[idx, b, u:u + 1, :])

        acc_tiles(s, tiles_of(half_id), resp_of)

    def mr_all(s, slot, t):
        for h in range(2):
            mr_half(s, slot, t, h)

    def acc_result():
        cnt = jnp.sum(n_acc[...], axis=1, keepdims=True)
        mean = s_acc[...] * (1.0 / (cnt + EPS_COUNT))
        logw = jnp.log((cnt + PRIOR_ALPHA) / (total_pts + total_comp * PRIOR_ALPHA))
        return mean, logw

    def half(ref, k):
        return ref.at[pl.ds(2 * k, 2)]

    def pre(idx):
        return remote(half(l_buf.at[idx % 2], 1 - c), pre_buf.at[idx], pre_send.at[idx - 2], pre_recv.at[idx - 2], sib)

    def bcast(idx, j):
        k = lax.rem(jnp.where(z < comp_size // 2, n_chips - j, j), n_chips)
        q = lax.rem(chip + k, n_chips)
        return remote(bc_src.at[idx], bc_buf.at[idx, k], bc_send.at[idx - 2], bc_recv.at[idx - 2],
                      {"comp": q // y_size, "row": (q % y_size) * CORES + (1 - c)})

    def post(idx):
        return same(half(tot_buf.at[idx], 1 - c), post_send.at[idx - 2], post_recv.at[idx - 2], sib)

    def p2(idx):
        pre(idx).wait()
        bc_src[idx] = lse2_parts([l_buf[idx % 2, pl.ds(2 * c, 2)], pre_buf[idx]])
        for j in range(1, n_chips + 1):
            bcast(idx, j).start()

    def p3(idx):
        same(bc_buf.at[idx], bc_send.at[idx - 2], bc_recv.at[idx - 2], sib).wait()
        tot_buf[idx, pl.ds(2 * (1 - c), 2)] = lse2_parts([bc_buf[idx, k] for k in range(n_chips)])
        post(idx).start()

    def zl(s, k):
        return remote(zl_src.at[s], zl_buf.at[s, k - 1], zl_send.at[s], zl_recv.at[s],
                      {"comp": lax.rem(z + k, comp_size)})

    def ag(s, k):
        return same(tot_buf.at[s, r], ag_send.at[s], ag_recv.at[s], (sib, yn, yd)[k])

    def orig_fit(s, _):
        def orig_slots(p, _):
            for k in range(2):
                q = 2 * p + k
                off = pl.multiple_of(q * n_own, n_own)
                set_params(s, q, mu_all[s, pl.ds(off, n_own), :], row_to_col(lp_ref[pl.ds(s, 1), pl.ds(off, n_own)]), 0)
                for u in range(bt):
                    _, _, l = e_tile(s, q, 0, r * bt + u)
                    lq_buf[q, u:u + 1, :] = l

            @pl.when(jnp.logical_and(s == 0, p == 0))
            def _():
                pl.semaphore_wait(near_sem, 3 + n_z)
                signal_z(far_sem)

            @pl.when(s == 1)
            def _():
                y_steps(1 + 2 * p, 3 + 2 * p)

            return 0

        lax.fori_loop(0, row_size // 2, orig_slots, 0)
        zl_src[s] = lse2_parts([lq_buf[q] for q in range(row_size)])

        @pl.when(s == 0)
        def _():
            pl.semaphore_wait(far_sem, n_z)

        for k in range(1, comp_size):
            zl(s, k).start()

        @pl.when(s == 0)
        def _():
            y_steps(0, 1)

        return 0

    lax.fori_loop(0, 2, orig_fit, 0)

    def y_sends(a, b):
        def send(j, _):
            y_out(j).start()
            return 0

        lax.fori_loop(a, b, send, 0)

    def comb(s):
        same(zl_buf.at[s], zl_send.at[s], zl_recv.at[s], sib).wait()
        tot_buf[s, r] = lse2_parts([zl_src[s]] + [zl_buf[s, k] for k in range(comp_size - 1)])
        for k in range(3):
            ag(s, k).start()

    early = ND + 3
    y_sends(ND, early)
    y_steps(5, 6)
    comb(0)
    y_sends(early, 2 * ND)
    y_steps(6, 8)
    z_steps(0, 4)
    y_steps(8, 9)
    z_steps(4, 5)
    y_steps(9, 10)
    z_steps(5, 6)
    comb(1)
    y_steps(10, 11)
    z_steps(6, 7)
    y_steps(11, 12)

    def sweep0(s, _):
        same(tot_buf.at[s, pl.ds(0, 3)], ag_send.at[s], ag_recv.at[s], sib).wait()
        own_out(s).wait_recv()
        acc_zero()

        def body(k, _):
            @pl.when(jnp.logical_and(s == 0, k == 1))
            def _():
                y_steps(12, 14)
                sib_waits(0)
                y_steps(14, 15)

            @pl.when(jnp.logical_and(s == 1, k == 1))
            def _():
                z_steps(12, 14)
                sib_waits(1)

            mr_half(s, r, 0, y + k * (1 - 2 * y))

            @pl.when(jnp.logical_and(s == 0, k == 1))
            def _():
                y_steps(15, 16)
                z_steps(7, 10)

            return 0

        lax.fori_loop(0, 2, body, 0)
        mean, logw = acc_result()
        set_params(s, r, mean, logw, 1)

        def hook(i):
            @pl.when(jnp.logical_and(s == 0, i == 0))
            def _():
                y_steps(16, 17)

        def first_p3():
            @pl.when(s == 1)
            def _():
                p3(2)

        e_step(s, 1, 2 + s, hook, first_p3)

        @pl.when(s == 0)
        def _():
            y_steps(17, 18)
            z_steps(10, 12)

        return 0

    lax.fori_loop(0, 2, sweep0, 0)

    def mx(s):
        return same(mub.at[s, r], mx_send.at[s], mx_recv.at[s], yn)

    def br(s):
        return same(brow.at[s, r], br_send.at[s], br_recv.at[s], yn)

    def mean_rows(slot, s):
        return mu_out.at[s, pl.ds(pl.multiple_of(slot * n_own, n_own), n_own), :]

    def fin(slot, s, k):
        return same(mean_rows(slot, s), fin_send.at[s, k], fin_recv.at[s, k], sib)

    def lpf(slot, k):
        return same(lp_fin.at[slot], lpf_send.at[k], lpf_recv.at[k], sib)

    def sweep(i, _):
        t, s = i // 2, i % 2
        last = t == sweeps - 1
        m_step(s, t)
        mean, logw = acc_result()

        @pl.when(t < sweeps - 1)
        def _():
            col = set_params(s, r, mean, logw, t + 1)

            @pl.when(t == sweeps - 2)
            def _():
                brow[s, r] = col_to_row(col)

            e_step(s, t + 1, i + 2, early=lambda: p3(i + 1))

            @pl.when(t == sweeps - 2)
            def _():
                mx(s).start()
                br(s).start()

        @pl.when(last)
        def _():
            mean_rows(r, s)[...] = mean
            lp_fin[r, pl.ds(s, 1), :] = col_to_row(logw)
            fin(r, s, 0).start()
            mx(s).wait()
            br(s).wait()
            bcol[s, ry] = jnp.broadcast_to(row_to_col(brow[s, ry]), (n_own, 128))
            acc_zero()

            mr_all(s, ry, t)
            mean2, logw2 = acc_result()
            mean_rows(ry, s)[...] = mean2
            lp_fin[ry, pl.ds(s, 1), :] = col_to_row(logw2)
            fin(ry, s, 1).start()

            @pl.when(s == 0)
            def _():
                p3(i + 1)

        return 0

    lax.fori_loop(2, 2 * sweeps, sweep, 0)
    lpf(r, 0).start()
    lpf(ry, 1).start()

    ones = jnp.ones((8, half_dim), jnp.bfloat16)

    def sq_norms(s, _):
        for u in range(bt):
            x = x_tile(s, r * bt + u).astype(jnp.float32)
            sq = x * x
            hi = sq.astype(jnp.bfloat16)
            lo = (sq - hi.astype(jnp.float32)).astype(jnp.bfloat16)
            sq_buf[s, u:u + 1, :] = (dot_t(ones, hi) + dot_t(ones, lo))[0:1]
        return 0

    lax.fori_loop(0, 2, sq_norms, 0)
    for s in range(2):
        gather_sends_wait(s)

    t = sweeps - 1
    for s in range(2):
        for j in range(bt):
            lse_out[s:s + 1, j * TP:(j + 1) * TP] = (
                tot_buf[2 * t + s, r, j:j + 1, :] * LN2 - temp_ref[t] * sq_buf[s, j:j + 1, :])

    for k in range(2):
        for s in range(2):
            fin((r, ry)[k], s, k).wait()
    lpf(r, 0).wait()
    lpf(ry, 1).wait()
    for q in range(row_size):
        lp_out[:, q * n_own:(q + 1) * n_own] = lp_fin[q]


def solution(mesh):
    comp_size = mesh.shape["comp"]
    row_size = mesh.shape["row"]

    def local_fit(x_local, mu_init, logpi_init, inv_temp):
        block, dim = x_local.shape
        half_dim = dim // 2
        n_local = mu_init.shape[1]
        n_own = n_local // row_size
        total_pts = block * row_size
        tiles = total_pts // TP
        sweeps = inv_temp.shape[0]
        n_chips = comp_size * row_size // CORES
        ni = 2 * sweeps
        bt = block // TP
        f32, bf16 = jnp.float32, jnp.bfloat16
        dma = pltpu.SemaphoreType.DMA
        vm = pltpu.VMEM
        scratch = [
            pltpu.SMEM((sweeps,), f32), vm((2, n_local), f32),
            vm((2, total_pts, half_dim), bf16),
            vm((2, n_local, half_dim), f32),
            vm((2, row_size, n_own, half_dim), bf16),
            vm((2, row_size, n_own, 128), f32),
            vm((2, row_size, 1, n_own), f32),
            vm((2, tiles, n_own, TP), f32),
            vm((2, row_size, bt, TP), f32),
            vm((2, row_size, bt, TP), f32),
            vm((row_size, bt, TP), f32),
            vm((n_own, half_dim), f32),
            vm((n_own, 128), f32),
            vm((row_size, 2, n_own), f32),
            vm((2, bt, TP), f32),
            vm((2, bt, TP), f32),
            vm((2, comp_size - 1, bt, TP), f32),
            vm((ni, 2, bt, TP), f32),
            vm((ni, 2, bt, TP), f32),
            vm((ni, n_chips, 2, bt, TP), f32),
            vm((ni, row_size, bt, TP), f32),
            dma((6,)), pltpu.SemaphoreType.REGULAR, pltpu.SemaphoreType.REGULAR,
            dma((1,)), dma((2 * ND,)), dma((2 * NR,)), dma((2,)), dma((2,)), dma((2,)),
            dma((2,)), dma((2,)), dma((2,)), dma((2,)),
            dma((ni - 2,)), dma((ni - 2,)), dma((ni - 2,)), dma((ni - 2,)), dma((ni - 2,)), dma((ni - 2,)),
            dma((2,)), dma((2,)), dma((2,)), dma((2,)),
            dma((2, 2)), dma((2, 2)), dma((2,)), dma((2,)),
        ]
        outs = pl.pallas_call(
            functools.partial(em_kernel, comp_size, row_size, sweeps),
            out_shape=(vm((2, n_local, half_dim), f32), vm((2, n_local), f32), vm((2, block), f32)),
            in_specs=[
                pl.BlockSpec(memory_space=pl.ANY),
            ] * 4,
            out_specs=(pl.BlockSpec(memory_space=pltpu.VMEM),) * 3,
            scratch_shapes=scratch,
            compiler_params=pltpu.CompilerParams(
                collective_id=0, has_side_effects=True, vmem_limit_bytes=56 * 1024 * 1024),
        )(inv_temp, logpi_init, x_local, mu_init)
        return pl.pallas_call(
            write_kernel,
            out_shape=tuple(jax.ShapeDtypeStruct(o.shape, o.dtype) for o in outs),
            in_specs=[pl.BlockSpec(memory_space=pltpu.VMEM)] * 3,
            out_specs=(pl.BlockSpec(memory_space=pl.ANY),) * 3,
            scratch_shapes=[dma((3,))],
        )(*[pltpu.with_memory_space_constraint(o, pltpu.VMEM) for o in outs])

    return jax.shard_map(
        local_fit,
        mesh=mesh,
        in_specs=(P(("grp", "row"), None), P(None, ("grp", "comp"), None), P(None, ("grp", "comp")), P()),
        out_specs=(P(None, ("grp", "comp"), None), P(None, ("grp", "comp")), P(None, ("grp", "row"))),
        check_vma=False,
    )
```

```python
import functools

import jax
import jax.numpy as jnp
from jax import lax
from jax.experimental import pallas as pl
from jax.experimental.pallas import tpu as pltpu
from jax.sharding import PartitionSpec as P

EPS_COUNT = 1e-6
PRIOR_ALPHA = 1e-3
LOG2E = 1.4426950408889634
LN2 = 0.6931471805599453
MESH = pl.DeviceIdType.MESH

CORES = 2
TP = 256
NCK = 16
ND = 9
NR = NCK - ND


def lse2_parts(parts):
    top = functools.reduce(jnp.maximum, parts)
    total = functools.reduce(jnp.add, [jnp.exp2(p - top) for p in parts])
    return top + jnp.log(total) * LOG2E


def dot_t(a, b):
    return lax.dot_general(a, b, (((1,), (1,)), ((), ())), preferred_element_type=jnp.float32)


def eye_mask(n):
    return lax.broadcasted_iota(jnp.int32, (n, n), 0) == lax.broadcasted_iota(jnp.int32, (n, n), 1)


def col_to_row(col):
    return jnp.sum(jnp.where(eye_mask(col.shape[0]), col, 0.0), axis=0, keepdims=True)


def row_to_col(row):
    return jnp.sum(jnp.where(eye_mask(row.shape[1]), row, 0.0), axis=1, keepdims=True)


def twice(b):
    return jnp.concatenate([b, b], axis=1)


def write_kernel(a, b, c, a_out, b_out, c_out, sems):
    copies = [pltpu.make_async_copy(v, o, sems.at[k]) for k, (v, o) in enumerate(((a, a_out), (b, b_out), (c, c_out)))]
    for cp in copies:
        cp.start()
    for cp in copies:
        cp.wait()


def em_kernel(
    comp_size, row_size, sweeps,
    temp_hbm, lp_hbm, x_hbm, mu_hbm,
    mu_out, lp_out, lse_out,
    temp_ref, lp_ref, xg, mu_all, mub, bcol, brow, e_buf, m_buf, l_buf, lq_buf, s_acc, n_acc, lp_fin, sq_buf,
    zl_src, zl_buf, pre_buf, bc_src, bc_buf, tot_buf,
    load_sem, near_sem, far_sem, g_send, y_recv, z_recv, sy_recv, sz_recv, own_recv,
    l_send, zl_recv, ag_recv, pre_send, pre_recv, bc_recv, post_recv, mx_recv, br_recv, fin_recv, lpf_recv,
):
    z = lax.axis_index("comp")
    r = lax.axis_index("row")
    y, c = r // CORES, r % CORES
    n_chips = comp_size * row_size // CORES
    y_size = row_size // CORES
    chip = z * y_size + y
    block = x_hbm.shape[0]
    half_dim = x_hbm.shape[1] // 2
    total_pts = block * row_size
    n_own = mub.shape[2]
    total_comp = mu_hbm.shape[1] * comp_size
    bt = block // TP
    ch = block // NCK
    rs = y * CORES + (1 - c)
    ry = (1 - y) * CORES + c
    sib = {"row": rs}
    yn = {"row": ry}
    rx = (1 - y) * CORES + (1 - c)
    yd = {"row": rx}
    zx = {"comp": z + 1 - 2 * (z % 2), "row": rs}
    hz = z % 2

    def remote(src, dst, send, recv, dev):
        return pltpu.make_async_remote_copy(
            src_ref=src, dst_ref=dst, send_sem=send, recv_sem=recv, device_id=dev, device_id_type=MESH)

    def same(v, send, recv, dev):
        return remote(v, v, send, recv, dev)

    x_loads = [pltpu.make_async_copy(
        x_hbm.at[:, pl.ds(s * half_dim, half_dim)], xg.at[s, pl.ds(r * block, block), :], load_sem.at[s])
        for s in range(2)]
    mu_loads = [pltpu.make_async_copy(mu_hbm.at[s], mu_all.at[s], load_sem.at[2 + s]) for s in range(2)]
    small_loads = [pltpu.make_async_copy(temp_hbm, temp_ref, load_sem.at[4]),
                   pltpu.make_async_copy(lp_hbm, lp_ref, load_sem.at[5])]
    for cp in x_loads + small_loads:
        cp.start()

    n_z = (z > 0).astype(jnp.int32) + (z < comp_size - 1).astype(jnp.int32)

    def signal_z(sem):
        @pl.when(z > 0)
        def _():
            pl.semaphore_signal(sem, inc=1, device_id={"comp": z - 1}, device_id_type=MESH)

        @pl.when(z < comp_size - 1)
        def _():
            pl.semaphore_signal(sem, inc=1, device_id={"comp": z + 1}, device_id_type=MESH)

    def signal_near(sem):
        for dev in (sib, yn, yd):
            pl.semaphore_signal(sem, inc=1, device_id=dev, device_id_type=MESH)
        signal_z(sem)

    barrier = pltpu.get_barrier_semaphore()
    signal_near(barrier)
    pl.semaphore_wait(barrier, 3 + n_z)
    signal_near(near_sem)
    for cp in mu_loads:
        cp.start()

    def xrows(s, blk, cid):
        return xg.at[s, pl.ds(pl.multiple_of(blk * block + cid * ch, ch), ch), :]

    def cid_y(k):
        return k + hz * (NCK - 1 - 2 * k)

    def cid_z(k):
        return k + (1 - hz) * (NCK - 1 - 2 * k)

    def y_out(j):
        return same(xrows(j // ND, r, cid_y(j % ND)), g_send.at[0], y_recv.at[j], yd)

    def z_fwd(m):
        return same(xrows(m // NR, rx, cid_y(m % NR)), g_send.at[0], z_recv.at[m], zx)

    def sy_fwd(j):
        return same(xrows(j // ND, rx, cid_y(j % ND)), g_send.at[0], sy_recv.at[j // ND], sib)

    def sz_fwd(m):
        return same(xrows(m // NR, ry, cid_z(m % NR)), g_send.at[0], sz_recv.at[m // NR], sib)

    def own_out(s):
        return same(xg.at[s, pl.ds(r * block, block), :], g_send.at[0], own_recv.at[s], sib)

    def y_steps(a, b):
        def body(j, _):
            y_out(j).wait_recv()

            @pl.when(j % ND < NR)
            def _():
                z_fwd(j // ND * NR + j % ND).start()

            sy_fwd(j).start()
            return 0

        lax.fori_loop(a, b, body, 0)

    def z_steps(a, b):
        def body(m, _):
            z_fwd(m).wait_recv()
            sz_fwd(m).start()
            return 0

        lax.fori_loop(a, b, body, 0)

    def rows_of(s, chunks):
        return xg.at[s, pl.ds(0, chunks * ch), :]

    def sib_waits(s):
        same(rows_of(s, ND), g_send.at[0], sy_recv.at[s], sib).wait_recv()
        same(rows_of(s, NR), g_send.at[0], sz_recv.at[s], sib).wait_recv()

    def gather_sends_wait(s):
        for chunks in (ND, NR, ND, NR):
            same(rows_of(s, chunks), g_send.at[0], sy_recv.at[s], sib).wait_send()
        own_out(s).wait_send()

    x_loads[0].wait()
    for j in range(ND):
        y_out(j).start()
    own_out(0).start()
    x_loads[1].wait()
    own_out(1).start()
    for cp in mu_loads + small_loads:
        cp.wait()

    def set_params(s, slot, mean, logw, t):
        mub[s, slot] = mean.astype(jnp.bfloat16)
        mu_sq = jnp.sum(mean * mean, axis=1, keepdims=True)
        col = (logw - temp_ref[t] * mu_sq) * LOG2E
        bcol[s, slot] = jnp.broadcast_to(col, (n_own, 128))
        return col

    def x_tile(s, tile):
        return xg[s, pl.ds(pl.multiple_of(tile * TP, TP), TP), :]

    def e_tile(s, slot, t, tile):
        a = dot_t(mub[s, slot], x_tile(s, tile))
        l2 = a * (temp_ref[t] * (2.0 * LOG2E)) + twice(bcol[s, slot])
        m = jnp.max(l2, axis=0, keepdims=True)
        e = jnp.exp2(l2 - m)
        return e, m, m + jnp.log(jnp.sum(e, axis=0, keepdims=True)) * LOG2E

    def tiles_of(half_id):
        return [(2 * half_id + k // bt, k % bt) for k in range(2 * bt)]

    def e_step(s, t, idx, hook=None, early=None):
        def body(i, _):
            h = (1 - c) + i * (2 * c - 1)
            for b, u in tiles_of(h):
                e, m, l = e_tile(s, r, t, b * bt + u)
                e_buf[s, b * bt + u] = e
                m_buf[s, b, u:u + 1, :] = m
                l_buf[s, b, u:u + 1, :] = l

            @pl.when(i == 0)
            def _():
                pre(idx).start()

            if hook is not None:
                hook(i)
            return 0

        lax.fori_loop(0, 2, body, 0)
        p2(idx)
        if early is not None:
            early()

    def acc_zero():
        s_acc[...] = jnp.zeros_like(s_acc)
        n_acc[...] = jnp.zeros_like(n_acc)

    def acc_tiles(s, tiles, resp_of):
        dots, ns = [], []
        for b, u in tiles:
            resp = resp_of(b, u)
            ns.append(resp[:, :128] + resp[:, 128:])
            dots.append(jnp.dot(resp.astype(jnp.bfloat16), x_tile(s, b * bt + u), preferred_element_type=jnp.float32))
        s_acc[...] += functools.reduce(jnp.add, dots)
        n_acc[...] += functools.reduce(jnp.add, ns)

    def m_step(s, t):
        idx = 2 * t + s
        acc_zero()

        def body(i, _):
            @pl.when(i == 1)
            def _():
                post(idx).wait_recv()

            def resp_of(b, u):
                f = jnp.exp2(m_buf[s, b, u:u + 1, :] - tot_buf[idx, b, u:u + 1, :])
                return e_buf[s, b * bt + u] * f

            acc_tiles(s, tiles_of((1 - c) + i * (2 * c - 1)), resp_of)
            return 0

        lax.fori_loop(0, 2, body, 0)

    def mr_half(s, slot, t, half_id):
        idx = 2 * t + s

        def resp_of(b, u):
            a = dot_t(mub[s, slot], x_tile(s, b * bt + u))
            return jnp.exp2(a * (temp_ref[t] * (2.0 * LOG2E)) + twice(bcol[s, slot]) - tot_buf[idx, b, u:u + 1, :])

        acc_tiles(s, tiles_of(half_id), resp_of)

    def mr_all(s, slot, t):
        for h in range(2):
            mr_half(s, slot, t, h)

    def acc_result():
        cnt = jnp.sum(n_acc[...], axis=1, keepdims=True)
        mean = s_acc[...] * (1.0 / (cnt + EPS_COUNT))
        logw = jnp.log((cnt + PRIOR_ALPHA) / (total_pts + total_comp * PRIOR_ALPHA))
        return mean, logw

    def half(ref, k):
        return ref.at[pl.ds(2 * k, 2)]

    def pre(idx):
        return remote(half(l_buf.at[idx % 2], 1 - c), pre_buf.at[idx], pre_send.at[idx - 2], pre_recv.at[idx - 2], sib)

    def bcast(idx, j):
        k = lax.rem(jnp.where(z < comp_size // 2, n_chips - j, j), n_chips)
        q = lax.rem(chip + k, n_chips)
        return remote(bc_src.at[idx], bc_buf.at[idx, k], l_send.at[0], bc_recv.at[idx - 2],
                      {"comp": q // y_size, "row": (q % y_size) * CORES + (1 - c)})

    def post(idx):
        return same(half(tot_buf.at[idx], 1 - c), l_send.at[0], post_recv.at[idx - 2], sib)

    def p2(idx):
        pre(idx).wait()
        bc_src[idx] = lse2_parts([l_buf[idx % 2, pl.ds(2 * c, 2)], pre_buf[idx]])
        for j in range(1, n_chips + 1):
            bcast(idx, j).start()

    def p3(idx):
        same(bc_buf.at[idx], l_send.at[0], bc_recv.at[idx - 2], sib).wait_recv()
        tot_buf[idx, pl.ds(2 * (1 - c), 2)] = lse2_parts([bc_buf[idx, k] for k in range(n_chips)])
        post(idx).start()

    def zl(s, k):
        return remote(zl_src.at[s], zl_buf.at[s, k - 1], l_send.at[0], zl_recv.at[s],
                      {"comp": lax.rem(z + k, comp_size)})

    def ag(s, k):
        return same(tot_buf.at[s, r], l_send.at[0], ag_recv.at[s], (sib, yn, yd)[k])

    def orig_fit(s, _):
        def orig_slots(p, _):
            for k in range(2):
                q = 2 * p + k
                off = pl.multiple_of(q * n_own, n_own)
                set_params(s, q, mu_all[s, pl.ds(off, n_own), :], row_to_col(lp_ref[pl.ds(s, 1), pl.ds(off, n_own)]), 0)
                for u in range(bt):
                    _, _, l = e_tile(s, q, 0, r * bt + u)
                    lq_buf[q, u:u + 1, :] = l

            @pl.when(jnp.logical_and(s == 0, p == 0))
            def _():
                pl.semaphore_wait(near_sem, 3 + n_z)
                signal_z(far_sem)

            @pl.when(s == 1)
            def _():
                y_steps(1 + 2 * p, 3 + 2 * p)

            return 0

        lax.fori_loop(0, row_size // 2, orig_slots, 0)
        zl_src[s] = lse2_parts([lq_buf[q] for q in range(row_size)])

        @pl.when(s == 0)
        def _():
            pl.semaphore_wait(far_sem, n_z)

        for k in range(1, comp_size):
            zl(s, k).start()

        @pl.when(s == 0)
        def _():
            y_steps(0, 1)

        return 0

    lax.fori_loop(0, 2, orig_fit, 0)

    def y_sends(a, b):
        def send(j, _):
            y_out(j).start()
            return 0

        lax.fori_loop(a, b, send, 0)

    def comb(s):
        same(zl_buf.at[s], l_send.at[0], zl_recv.at[s], sib).wait_recv()
        tot_buf[s, r] = lse2_parts([zl_src[s]] + [zl_buf[s, k] for k in range(comp_size - 1)])
        for k in range(3):
            ag(s, k).start()

    early = ND + 3
    y_sends(ND, early)
    y_steps(5, 6)
    comb(0)
    y_sends(early, 2 * ND)
    y_steps(6, 8)
    z_steps(0, 4)
    y_steps(8, 9)
    z_steps(4, 5)
    y_steps(9, 10)
    z_steps(5, 6)
    comb(1)
    y_steps(10, 11)
    z_steps(6, 7)
    y_steps(11, 12)

    def sweep0(s, _):
        same(tot_buf.at[s, pl.ds(0, 3)], l_send.at[0], ag_recv.at[s], sib).wait_recv()
        own_out(s).wait_recv()
        acc_zero()

        def body(k, _):
            @pl.when(jnp.logical_and(s == 0, k == 1))
            def _():
                y_steps(12, 14)
                sib_waits(0)
                y_steps(14, 15)

            @pl.when(jnp.logical_and(s == 1, k == 1))
            def _():
                z_steps(12, 14)
                sib_waits(1)

            mr_half(s, r, 0, y + k * (1 - 2 * y))

            @pl.when(jnp.logical_and(s == 0, k == 1))
            def _():
                y_steps(15, 16)
                z_steps(7, 10)

            return 0

        lax.fori_loop(0, 2, body, 0)
        mean, logw = acc_result()
        set_params(s, r, mean, logw, 1)

        def hook(i):
            @pl.when(jnp.logical_and(s == 0, i == 0))
            def _():
                y_steps(16, 17)

        def first_p3():
            @pl.when(s == 1)
            def _():
                p3(2)

        e_step(s, 1, 2 + s, hook, first_p3)

        @pl.when(s == 0)
        def _():
            y_steps(17, 18)
            z_steps(10, 12)

        return 0

    lax.fori_loop(0, 2, sweep0, 0)

    def mx(s):
        return same(mub.at[s, r], l_send.at[0], mx_recv.at[s], yn)

    def br(s):
        return same(brow.at[s, r], l_send.at[0], br_recv.at[s], yn)

    def mean_rows(slot, s):
        return mu_out.at[s, pl.ds(pl.multiple_of(slot * n_own, n_own), n_own), :]

    def fin(slot, s, k):
        return same(mean_rows(slot, s), l_send.at[0], fin_recv.at[s, k], sib)

    def lpf(slot, k):
        return same(lp_fin.at[slot], l_send.at[0], lpf_recv.at[k], sib)

    def sweep(i, _):
        t, s = i // 2, i % 2
        last = t == sweeps - 1
        m_step(s, t)
        mean, logw = acc_result()

        @pl.when(t < sweeps - 1)
        def _():
            col = set_params(s, r, mean, logw, t + 1)

            @pl.when(t == sweeps - 2)
            def _():
                brow[s, r] = col_to_row(col)

            def early():
                @pl.when(t == sweeps - 2)
                def _():
                    mx(s).start()
                    br(s).start()

                p3(i + 1)

            e_step(s, t + 1, i + 2, early=early)

        @pl.when(last)
        def _():
            mean_rows(r, s)[...] = mean
            lp_fin[r, pl.ds(s, 1), :] = col_to_row(logw)
            fin(r, s, 0).start()
            mx(s).wait_recv()
            br(s).wait_recv()
            bcol[s, ry] = jnp.broadcast_to(row_to_col(brow[s, ry]), (n_own, 128))
            acc_zero()

            mr_all(s, ry, t)
            mean2, logw2 = acc_result()
            mean_rows(ry, s)[...] = mean2
            lp_fin[ry, pl.ds(s, 1), :] = col_to_row(logw2)
            fin(ry, s, 1).start()

            @pl.when(s == 0)
            def _():
                p3(i + 1)

        return 0

    lax.fori_loop(2, 2 * sweeps, sweep, 0)
    lpf(r, 0).start()
    lpf(ry, 1).start()

    ones = jnp.ones((8, half_dim), jnp.bfloat16)

    def sq_norms(s, _):
        for u in range(bt):
            x = x_tile(s, r * bt + u).astype(jnp.float32)
            sq = x * x
            hi = sq.astype(jnp.bfloat16)
            lo = (sq - hi.astype(jnp.float32)).astype(jnp.bfloat16)
            sq_buf[s, u:u + 1, :] = (dot_t(ones, hi) + dot_t(ones, lo))[0:1]
        return 0

    lax.fori_loop(0, 2, sq_norms, 0)
    for s in range(2):
        gather_sends_wait(s)
        same(zl_buf.at[s], l_send.at[0], zl_recv.at[s], sib).wait_send()
        same(tot_buf.at[s, pl.ds(0, 3)], l_send.at[0], ag_recv.at[s], sib).wait_send()
        mx(s).wait_send()
        br(s).wait_send()
        for t in range(1, sweeps):
            same(bc_buf.at[2 * t + s], l_send.at[0], zl_recv.at[s], sib).wait_send()
            post(2 * t + s).wait_send()


    t = sweeps - 1
    for s in range(2):
        for j in range(bt):
            lse_out[s:s + 1, j * TP:(j + 1) * TP] = (
                tot_buf[2 * t + s, r, j:j + 1, :] * LN2 - temp_ref[t] * sq_buf[s, j:j + 1, :])

    for k in range(2):
        for s in range(2):
            fin((r, ry)[k], s, k).wait_recv()
    lpf(r, 0).wait_recv()
    lpf(ry, 1).wait_recv()
    for k in range(2):
        for s in range(2):
            fin((r, ry)[k], s, k).wait_send()
        lpf((r, ry)[k], k).wait_send()
    for q in range(row_size):
        lp_out[:, q * n_own:(q + 1) * n_own] = lp_fin[q]


def solution(mesh):
    comp_size = mesh.shape["comp"]
    row_size = mesh.shape["row"]

    def local_fit(x_local, mu_init, logpi_init, inv_temp):
        block, dim = x_local.shape
        half_dim = dim // 2
        n_local = mu_init.shape[1]
        n_own = n_local // row_size
        total_pts = block * row_size
        tiles = total_pts // TP
        sweeps = inv_temp.shape[0]
        n_chips = comp_size * row_size // CORES
        ni = 2 * sweeps
        bt = block // TP
        f32, bf16 = jnp.float32, jnp.bfloat16
        dma = pltpu.SemaphoreType.DMA
        vm = pltpu.VMEM
        scratch = [
            pltpu.SMEM((sweeps,), f32), vm((2, n_local), f32),
            vm((2, total_pts, half_dim), bf16),
            vm((2, n_local, half_dim), f32),
            vm((2, row_size, n_own, half_dim), bf16),
            vm((2, row_size, n_own, 128), f32),
            vm((2, row_size, 1, n_own), f32),
            vm((2, tiles, n_own, TP), f32),
            vm((2, row_size, bt, TP), f32),
            vm((2, row_size, bt, TP), f32),
            vm((row_size, bt, TP), f32),
            vm((n_own, half_dim), f32),
            vm((n_own, 128), f32),
            vm((row_size, 2, n_own), f32),
            vm((2, bt, TP), f32),
            vm((2, bt, TP), f32),
            vm((2, comp_size - 1, bt, TP), f32),
            vm((ni, 2, bt, TP), f32),
            vm((ni, 2, bt, TP), f32),
            vm((ni, n_chips, 2, bt, TP), f32),
            vm((ni, row_size, bt, TP), f32),
            dma((6,)), pltpu.SemaphoreType.REGULAR, pltpu.SemaphoreType.REGULAR,
            dma((1,)), dma((2 * ND,)), dma((2 * NR,)), dma((2,)), dma((2,)), dma((2,)),
            dma((1,)), dma((2,)), dma((2,)), dma((ni - 2,)), dma((ni - 2,)), dma((ni - 2,)), dma((ni - 2,)),
            dma((2,)), dma((2,)), dma((2, 2)), dma((2,)),
        ]
        outs = pl.pallas_call(
            functools.partial(em_kernel, comp_size, row_size, sweeps),
            out_shape=(vm((2, n_local, half_dim), f32), vm((2, n_local), f32), vm((2, block), f32)),
            in_specs=[
                pl.BlockSpec(memory_space=pl.ANY),
            ] * 4,
            out_specs=(pl.BlockSpec(memory_space=pltpu.VMEM),) * 3,
            scratch_shapes=scratch,
            compiler_params=pltpu.CompilerParams(
                collective_id=0, has_side_effects=True, vmem_limit_bytes=56 * 1024 * 1024),
        )(inv_temp, logpi_init, x_local, mu_init)
        return pl.pallas_call(
            write_kernel,
            out_shape=tuple(jax.ShapeDtypeStruct(o.shape, o.dtype) for o in outs),
            in_specs=[pl.BlockSpec(memory_space=pltpu.VMEM)] * 3,
            out_specs=(pl.BlockSpec(memory_space=pl.ANY),) * 3,
            scratch_shapes=[dma((3,))],
        )(*[pltpu.with_memory_space_constraint(o, pltpu.VMEM) for o in outs])

    return jax.shard_map(
        local_fit,
        mesh=mesh,
        in_specs=(P(("grp", "row"), None), P(None, ("grp", "comp"), None), P(None, ("grp", "comp")), P()),
        out_specs=(P(None, ("grp", "comp"), None), P(None, ("grp", "comp")), P(None, ("grp", "row"))),
        check_vma=False,
    )
```

```python
import functools

import jax
import jax.numpy as jnp
from jax import lax
from jax.experimental import pallas as pl
from jax.experimental.pallas import tpu as pltpu
from jax.sharding import PartitionSpec as P

EPS_COUNT = 1e-6
PRIOR_ALPHA = 1e-3
LOG2E = 1.4426950408889634
LN2 = 0.6931471805599453
MESH = pl.DeviceIdType.MESH

CORES = 2
TP = 256
NCK = 16
ND = 9
NR = NCK - ND


def lse2_parts(parts):
    top = functools.reduce(jnp.maximum, parts)
    total = functools.reduce(jnp.add, [jnp.exp2(p - top) for p in parts])
    return top + jnp.log(total) * LOG2E


def dot_t(a, b):
    return lax.dot_general(a, b, (((1,), (1,)), ((), ())), preferred_element_type=jnp.float32)


def eye_mask(n):
    return lax.broadcasted_iota(jnp.int32, (n, n), 0) == lax.broadcasted_iota(jnp.int32, (n, n), 1)


def col_to_row(col):
    return jnp.sum(jnp.where(eye_mask(col.shape[0]), col, 0.0), axis=0, keepdims=True)


def row_to_col(row):
    return jnp.sum(jnp.where(eye_mask(row.shape[1]), row, 0.0), axis=1, keepdims=True)


def twice(b):
    return jnp.concatenate([b, b], axis=1)


def write_kernel(a, b, c, a_out, b_out, c_out, sems):
    copies = [pltpu.make_async_copy(v, o, sems.at[k]) for k, (v, o) in enumerate(((a, a_out), (b, b_out), (c, c_out)))]
    for cp in copies:
        cp.start()
    for cp in copies:
        cp.wait()


def em_kernel(
    comp_size, row_size, sweeps,
    temp_hbm, lp_hbm, x_hbm, mu_hbm,
    mu_out, lp_out, lse_out,
    temp_ref, lp_ref, xg, mu_all, mub, bcol, brow, e_buf, m_buf, l_buf, lq_buf, s_acc, n_acc, lp_fin, sq_buf,
    zl_src, zl_buf, pre_buf, bc_src, bc_buf, tot_buf,
    load_sem, near_sem, far_sem, g_send, y_recv, z_recv, sy_recv, sz_recv, own_recv,
    l_send, zl_recv, ag_recv, pre_send, pre_recv, bc_recv, post_recv, mx_recv, br_recv, fin_recv, lpf_recv,
):
    z = lax.axis_index("comp")
    r = lax.axis_index("row")
    y, c = r // CORES, r % CORES
    n_chips = comp_size * row_size // CORES
    y_size = row_size // CORES
    chip = z * y_size + y
    block = x_hbm.shape[0]
    half_dim = x_hbm.shape[1] // 2
    total_pts = block * row_size
    n_own = mub.shape[2]
    total_comp = mu_hbm.shape[1] * comp_size
    bt = block // TP
    ch = block // NCK
    rs = y * CORES + (1 - c)
    ry = (1 - y) * CORES + c
    sib = {"row": rs}
    yn = {"row": ry}
    rx = (1 - y) * CORES + (1 - c)
    yd = {"row": rx}
    zx = {"comp": z + 1 - 2 * (z % 2), "row": rs}
    hz = z % 2

    def remote(src, dst, send, recv, dev):
        return pltpu.make_async_remote_copy(
            src_ref=src, dst_ref=dst, send_sem=send, recv_sem=recv, device_id=dev, device_id_type=MESH)

    def same(v, send, recv, dev):
        return remote(v, v, send, recv, dev)

    x_loads = [pltpu.make_async_copy(
        x_hbm.at[:, pl.ds(s * half_dim, half_dim)], xg.at[s, pl.ds(r * block, block), :], load_sem.at[s])
        for s in range(2)]
    mu_loads = [pltpu.make_async_copy(mu_hbm.at[s], mu_all.at[s], load_sem.at[2 + s]) for s in range(2)]
    small_loads = [pltpu.make_async_copy(temp_hbm, temp_ref, load_sem.at[4]),
                   pltpu.make_async_copy(lp_hbm, lp_ref, load_sem.at[5])]
    for cp in x_loads + small_loads:
        cp.start()

    n_z = (z > 0).astype(jnp.int32) + (z < comp_size - 1).astype(jnp.int32)

    def signal_z(sem):
        @pl.when(z > 0)
        def _():
            pl.semaphore_signal(sem, inc=1, device_id={"comp": z - 1}, device_id_type=MESH)

        @pl.when(z < comp_size - 1)
        def _():
            pl.semaphore_signal(sem, inc=1, device_id={"comp": z + 1}, device_id_type=MESH)

    def signal_near(sem):
        for dev in (sib, yn, yd):
            pl.semaphore_signal(sem, inc=1, device_id=dev, device_id_type=MESH)
        signal_z(sem)

    barrier = pltpu.get_barrier_semaphore()
    signal_near(barrier)
    pl.semaphore_wait(barrier, 3 + n_z)
    signal_near(near_sem)
    for cp in mu_loads:
        cp.start()

    def xrows(s, blk, cid):
        return xg.at[s, pl.ds(pl.multiple_of(blk * block + cid * ch, ch), ch), :]

    def cid_y(k):
        return k + hz * (NCK - 1 - 2 * k)

    def cid_z(k):
        return k + (1 - hz) * (NCK - 1 - 2 * k)

    def y_out(j):
        return same(xrows(j // ND, r, cid_y(j % ND)), g_send.at[0], y_recv.at[j], yd)

    def z_fwd(m):
        return same(xrows(m // NR, rx, cid_y(m % NR)), g_send.at[0], z_recv.at[m], zx)

    def sy_fwd(j):
        return same(xrows(j // ND, rx, cid_y(j % ND)), g_send.at[0], sy_recv.at[j // ND], sib)

    def sz_fwd(m):
        return same(xrows(m // NR, ry, cid_z(m % NR)), g_send.at[0], sz_recv.at[m // NR], sib)

    def own_out(s):
        return same(xg.at[s, pl.ds(r * block, block), :], g_send.at[0], own_recv.at[s], sib)

    def y_steps(a, b):
        def body(j, _):
            y_out(j).wait_recv()

            @pl.when(j % ND < NR)
            def _():
                z_fwd(j // ND * NR + j % ND).start()

            sy_fwd(j).start()
            return 0

        lax.fori_loop(a, b, body, 0)

    def z_steps(a, b):
        def body(m, _):
            z_fwd(m).wait_recv()
            sz_fwd(m).start()
            return 0

        lax.fori_loop(a, b, body, 0)

    def rows_of(s, chunks):
        return xg.at[s, pl.ds(0, chunks * ch), :]

    def sib_waits(s):
        same(rows_of(s, ND), g_send.at[0], sy_recv.at[s], sib).wait_recv()
        same(rows_of(s, NR), g_send.at[0], sz_recv.at[s], sib).wait_recv()

    def gather_sends_wait(s):
        for chunks in (ND, NR, ND, NR):
            same(rows_of(s, chunks), g_send.at[0], sy_recv.at[s], sib).wait_send()
        own_out(s).wait_send()

    x_loads[0].wait()
    for j in range(ND):
        y_out(j).start()
    own_out(0).start()
    x_loads[1].wait()
    own_out(1).start()
    for cp in mu_loads + small_loads:
        cp.wait()

    def set_params(s, slot, mean, logw, t):
        mub[s, slot] = mean.astype(jnp.bfloat16)
        mu_sq = jnp.sum(mean * mean, axis=1, keepdims=True)
        col = (logw - temp_ref[t] * mu_sq) * LOG2E
        bcol[s, slot] = jnp.broadcast_to(col, (n_own, 128))
        return col

    def x_tile(s, tile):
        return xg[s, pl.ds(pl.multiple_of(tile * TP, TP), TP), :]

    def e_tile(s, slot, t, tile):
        a = dot_t(mub[s, slot], x_tile(s, tile))
        l2 = a * (temp_ref[t] * (2.0 * LOG2E)) + twice(bcol[s, slot])
        m = jnp.max(l2, axis=0, keepdims=True)
        e = jnp.exp2(l2 - m)
        return e, m, m + jnp.log(jnp.sum(e, axis=0, keepdims=True)) * LOG2E

    def tiles_of(half_id):
        return [(2 * half_id + k // bt, k % bt) for k in range(2 * bt)]

    def e_step(s, t, idx, hook=None, early=None):
        def body(i, _):
            h = (1 - c) + i * (2 * c - 1)
            for b, u in tiles_of(h):
                e, m, l = e_tile(s, r, t, b * bt + u)
                e_buf[s, b * bt + u] = e
                m_buf[s, b, u:u + 1, :] = m
                l_buf[s, b, u:u + 1, :] = l

            @pl.when(i == 0)
            def _():
                pre(idx).start()

            if hook is not None:
                hook(i)
            return 0

        lax.fori_loop(0, 2, body, 0)
        p2(idx)
        if early is not None:
            early()

    def acc_zero():
        s_acc[...] = jnp.zeros_like(s_acc)
        n_acc[...] = jnp.zeros_like(n_acc)

    def acc_tiles(s, tiles, resp_of):
        dots, ns = [], []
        for b, u in tiles:
            resp = resp_of(b, u)
            ns.append(resp[:, :128] + resp[:, 128:])
            dots.append(jnp.dot(resp.astype(jnp.bfloat16), x_tile(s, b * bt + u), preferred_element_type=jnp.float32))
        s_acc[...] += functools.reduce(jnp.add, dots)
        n_acc[...] += functools.reduce(jnp.add, ns)

    def m_step(s, t):
        idx = 2 * t + s
        acc_zero()

        def body(i, _):
            @pl.when(i == 1)
            def _():
                post(idx).wait_recv()

            def resp_of(b, u):
                f = jnp.exp2(m_buf[s, b, u:u + 1, :] - tot_buf[idx, b, u:u + 1, :])
                return e_buf[s, b * bt + u] * f

            acc_tiles(s, tiles_of((1 - c) + i * (2 * c - 1)), resp_of)
            return 0

        lax.fori_loop(0, 2, body, 0)

    def mr_half(s, slot, t, half_id):
        idx = 2 * t + s

        def resp_of(b, u):
            a = dot_t(mub[s, slot], x_tile(s, b * bt + u))
            return jnp.exp2(a * (temp_ref[t] * (2.0 * LOG2E)) + twice(bcol[s, slot]) - tot_buf[idx, b, u:u + 1, :])

        acc_tiles(s, tiles_of(half_id), resp_of)

    def mr_all(s, slot, t):
        for h in range(2):
            mr_half(s, slot, t, h)

    def acc_result():
        cnt = jnp.sum(n_acc[...], axis=1, keepdims=True)
        mean = s_acc[...] * (1.0 / (cnt + EPS_COUNT))
        logw = jnp.log((cnt + PRIOR_ALPHA) / (total_pts + total_comp * PRIOR_ALPHA))
        return mean, logw

    def half(ref, k):
        return ref.at[pl.ds(2 * k, 2)]

    def pre(idx):
        return remote(half(l_buf.at[idx % 2], 1 - c), pre_buf.at[idx], pre_send.at[idx - 2], pre_recv.at[idx - 2], sib)

    def bcast(idx, j):
        k = lax.rem(jnp.where(z < comp_size // 2, n_chips - j, j), n_chips)
        q = lax.rem(chip + k, n_chips)
        return remote(bc_src.at[idx], bc_buf.at[idx, k], l_send.at[0], bc_recv.at[idx - 2],
                      {"comp": q // y_size, "row": (q % y_size) * CORES + (1 - c)})

    def post(idx):
        return same(half(tot_buf.at[idx], 1 - c), l_send.at[0], post_recv.at[idx - 2], sib)

    def p2(idx):
        pre(idx).wait()
        bc_src[idx] = lse2_parts([l_buf[idx % 2, pl.ds(2 * c, 2)], pre_buf[idx]])
        for j in range(1, n_chips + 1):
            bcast(idx, j).start()

    def p3(idx):
        same(bc_buf.at[idx], l_send.at[0], bc_recv.at[idx - 2], sib).wait_recv()
        tot_buf[idx, pl.ds(2 * (1 - c), 2)] = lse2_parts([bc_buf[idx, k] for k in range(n_chips)])
        post(idx).start()

    def zl(s, k):
        return remote(zl_src.at[s], zl_buf.at[s, k - 1], l_send.at[0], zl_recv.at[s],
                      {"comp": lax.rem(z + k, comp_size)})

    def ag(s, k):
        return same(tot_buf.at[s, r], l_send.at[0], ag_recv.at[s], (sib, yn, yd)[k])

    def orig_fit(s, _):
        def orig_slots(p, _):
            for k in range(2):
                q = 2 * p + k
                off = pl.multiple_of(q * n_own, n_own)
                set_params(s, q, mu_all[s, pl.ds(off, n_own), :], row_to_col(lp_ref[pl.ds(s, 1), pl.ds(off, n_own)]), 0)
                for u in range(bt):
                    _, _, l = e_tile(s, q, 0, r * bt + u)
                    lq_buf[q, u:u + 1, :] = l

            @pl.when(jnp.logical_and(s == 0, p == 0))
            def _():
                pl.semaphore_wait(near_sem, 3 + n_z)
                signal_z(far_sem)

            @pl.when(s == 1)
            def _():
                y_steps(1 + 2 * p, 3 + 2 * p)

            return 0

        lax.fori_loop(0, row_size // 2, orig_slots, 0)
        zl_src[s] = lse2_parts([lq_buf[q] for q in range(row_size)])

        @pl.when(s == 0)
        def _():
            pl.semaphore_wait(far_sem, n_z)

        for k in range(1, comp_size):
            zl(s, k).start()

        @pl.when(s == 0)
        def _():
            y_steps(0, 1)

        return 0

    lax.fori_loop(0, 2, orig_fit, 0)

    def y_sends(a, b):
        def send(j, _):
            y_out(j).start()
            return 0

        lax.fori_loop(a, b, send, 0)

    def comb(s):
        same(zl_buf.at[s], l_send.at[0], zl_recv.at[s], sib).wait_recv()
        tot_buf[s, r] = lse2_parts([zl_src[s]] + [zl_buf[s, k] for k in range(comp_size - 1)])
        for k in range(3):
            ag(s, k).start()

    early = ND + 3
    y_sends(ND, early)
    y_steps(5, 6)
    comb(0)
    y_sends(early, 2 * ND)
    y_steps(6, 8)
    z_steps(0, 4)
    y_steps(8, 9)
    z_steps(4, 5)
    y_steps(9, 10)
    z_steps(5, 6)
    comb(1)
    y_steps(10, 11)
    z_steps(6, 7)
    y_steps(11, 12)

    def sweep0(s, _):
        same(tot_buf.at[s, pl.ds(0, 3)], l_send.at[0], ag_recv.at[s], sib).wait_recv()
        own_out(s).wait_recv()
        acc_zero()

        def body(k, _):
            @pl.when(jnp.logical_and(s == 0, k == 1))
            def _():
                y_steps(12, 14)
                sib_waits(0)

            @pl.when(jnp.logical_and(s == 1, k == 1))
            def _():
                z_steps(13, 14)
                sib_waits(1)

            mr_half(s, r, 0, y + k * (1 - 2 * y))

            @pl.when(jnp.logical_and(s == 0, k == 1))
            def _():
                y_steps(14, 16)
                z_steps(7, 10)

            return 0

        lax.fori_loop(0, 2, body, 0)
        mean, logw = acc_result()
        set_params(s, r, mean, logw, 1)

        def hook(i):
            @pl.when(jnp.logical_and(s == 0, i == 0))
            def _():
                y_steps(16, 17)

        def first_p3():
            @pl.when(s == 1)
            def _():
                p3(2)

        e_step(s, 1, 2 + s, hook, first_p3)

        @pl.when(s == 0)
        def _():
            y_steps(17, 18)
            z_steps(10, 13)

        return 0

    lax.fori_loop(0, 2, sweep0, 0)

    def mx(s):
        return same(mub.at[s, r], l_send.at[0], mx_recv.at[s], yn)

    def br(s):
        return same(brow.at[s, r], l_send.at[0], br_recv.at[s], yn)

    def mean_rows(slot, s):
        return mu_out.at[s, pl.ds(pl.multiple_of(slot * n_own, n_own), n_own), :]

    def fin(slot, s, k):
        return same(mean_rows(slot, s), l_send.at[0], fin_recv.at[s, k], sib)

    def lpf(slot, k):
        return same(lp_fin.at[slot], l_send.at[0], lpf_recv.at[k], sib)

    def sweep(i, _):
        t, s = i // 2, i % 2
        last = t == sweeps - 1
        m_step(s, t)
        mean, logw = acc_result()

        @pl.when(t < sweeps - 1)
        def _():
            col = set_params(s, r, mean, logw, t + 1)

            @pl.when(t == sweeps - 2)
            def _():
                brow[s, r] = col_to_row(col)

            def early():
                @pl.when(t == sweeps - 2)
                def _():
                    mx(s).start()
                    br(s).start()

                p3(i + 1)

            e_step(s, t + 1, i + 2, early=early)

        @pl.when(last)
        def _():
            mean_rows(r, s)[...] = mean
            lp_fin[r, pl.ds(s, 1), :] = col_to_row(logw)
            fin(r, s, 0).start()
            mx(s).wait_recv()
            br(s).wait_recv()
            bcol[s, ry] = jnp.broadcast_to(row_to_col(brow[s, ry]), (n_own, 128))
            acc_zero()

            mr_all(s, ry, t)
            mean2, logw2 = acc_result()
            mean_rows(ry, s)[...] = mean2
            lp_fin[ry, pl.ds(s, 1), :] = col_to_row(logw2)
            fin(ry, s, 1).start()

            @pl.when(s == 0)
            def _():
                p3(i + 1)

        return 0

    lax.fori_loop(2, 2 * sweeps, sweep, 0)
    lpf(r, 0).start()
    lpf(ry, 1).start()

    ones = jnp.ones((8, half_dim), jnp.bfloat16)

    def sq_norms(s, _):
        for u in range(bt):
            x = x_tile(s, r * bt + u).astype(jnp.float32)
            sq = x * x
            hi = sq.astype(jnp.bfloat16)
            lo = (sq - hi.astype(jnp.float32)).astype(jnp.bfloat16)
            sq_buf[s, u:u + 1, :] = (dot_t(ones, hi) + dot_t(ones, lo))[0:1]
        return 0

    lax.fori_loop(0, 2, sq_norms, 0)
    for s in range(2):
        gather_sends_wait(s)
        same(zl_buf.at[s], l_send.at[0], zl_recv.at[s], sib).wait_send()
        same(tot_buf.at[s, pl.ds(0, 3)], l_send.at[0], ag_recv.at[s], sib).wait_send()
        mx(s).wait_send()
        br(s).wait_send()
        for t in range(1, sweeps):
            same(bc_buf.at[2 * t + s], l_send.at[0], zl_recv.at[s], sib).wait_send()
            post(2 * t + s).wait_send()


    t = sweeps - 1
    for s in range(2):
        for j in range(bt):
            lse_out[s:s + 1, j * TP:(j + 1) * TP] = (
                tot_buf[2 * t + s, r, j:j + 1, :] * LN2 - temp_ref[t] * sq_buf[s, j:j + 1, :])

    for k in range(2):
        for s in range(2):
            fin((r, ry)[k], s, k).wait_recv()
    lpf(r, 0).wait_recv()
    lpf(ry, 1).wait_recv()
    for k in range(2):
        for s in range(2):
            fin((r, ry)[k], s, k).wait_send()
        lpf((r, ry)[k], k).wait_send()
    for q in range(row_size):
        lp_out[:, q * n_own:(q + 1) * n_own] = lp_fin[q]


def solution(mesh):
    comp_size = mesh.shape["comp"]
    row_size = mesh.shape["row"]

    def local_fit(x_local, mu_init, logpi_init, inv_temp):
        block, dim = x_local.shape
        half_dim = dim // 2
        n_local = mu_init.shape[1]
        n_own = n_local // row_size
        total_pts = block * row_size
        tiles = total_pts // TP
        sweeps = inv_temp.shape[0]
        n_chips = comp_size * row_size // CORES
        ni = 2 * sweeps
        bt = block // TP
        f32, bf16 = jnp.float32, jnp.bfloat16
        dma = pltpu.SemaphoreType.DMA
        vm = pltpu.VMEM
        scratch = [
            pltpu.SMEM((sweeps,), f32), vm((2, n_local), f32),
            vm((2, total_pts, half_dim), bf16),
            vm((2, n_local, half_dim), f32),
            vm((2, row_size, n_own, half_dim), bf16),
            vm((2, row_size, n_own, 128), f32),
            vm((2, row_size, 1, n_own), f32),
            vm((2, tiles, n_own, TP), f32),
            vm((2, row_size, bt, TP), f32),
            vm((2, row_size, bt, TP), f32),
            vm((row_size, bt, TP), f32),
            vm((n_own, half_dim), f32),
            vm((n_own, 128), f32),
            vm((row_size, 2, n_own), f32),
            vm((2, bt, TP), f32),
            vm((2, bt, TP), f32),
            vm((2, comp_size - 1, bt, TP), f32),
            vm((ni, 2, bt, TP), f32),
            vm((ni, 2, bt, TP), f32),
            vm((ni, n_chips, 2, bt, TP), f32),
            vm((ni, row_size, bt, TP), f32),
            dma((6,)), pltpu.SemaphoreType.REGULAR, pltpu.SemaphoreType.REGULAR,
            dma((1,)), dma((2 * ND,)), dma((2 * NR,)), dma((2,)), dma((2,)), dma((2,)),
            dma((1,)), dma((2,)), dma((2,)), dma((ni - 2,)), dma((ni - 2,)), dma((ni - 2,)), dma((ni - 2,)),
            dma((2,)), dma((2,)), dma((2, 2)), dma((2,)),
        ]
        outs = pl.pallas_call(
            functools.partial(em_kernel, comp_size, row_size, sweeps),
            out_shape=(vm((2, n_local, half_dim), f32), vm((2, n_local), f32), vm((2, block), f32)),
            in_specs=[
                pl.BlockSpec(memory_space=pl.ANY),
            ] * 4,
            out_specs=(pl.BlockSpec(memory_space=pltpu.VMEM),) * 3,
            scratch_shapes=scratch,
            compiler_params=pltpu.CompilerParams(
                collective_id=0, has_side_effects=True, vmem_limit_bytes=56 * 1024 * 1024),
        )(inv_temp, logpi_init, x_local, mu_init)
        return pl.pallas_call(
            write_kernel,
            out_shape=tuple(jax.ShapeDtypeStruct(o.shape, o.dtype) for o in outs),
            in_specs=[pl.BlockSpec(memory_space=pltpu.VMEM)] * 3,
            out_specs=(pl.BlockSpec(memory_space=pl.ANY),) * 3,
            scratch_shapes=[dma((3,))],
        )(*[pltpu.with_memory_space_constraint(o, pltpu.VMEM) for o in outs])

    return jax.shard_map(
        local_fit,
        mesh=mesh,
        in_specs=(P(("grp", "row"), None), P(None, ("grp", "comp"), None), P(None, ("grp", "comp")), P()),
        out_specs=(P(None, ("grp", "comp"), None), P(None, ("grp", "comp")), P(None, ("grp", "row"))),
        check_vma=False,
    )
```

```python
import functools

import jax
import jax.numpy as jnp
from jax import lax
from jax.experimental import pallas as pl
from jax.experimental.pallas import tpu as pltpu
from jax.sharding import PartitionSpec as P

EPS_COUNT = 1e-6
PRIOR_ALPHA = 1e-3
LOG2E = 1.4426950408889634
LN2 = 0.6931471805599453
MESH = pl.DeviceIdType.MESH

CORES = 2
TP = 256
NCK = 16
ND = 9
NR = NCK - ND


def lse2_parts(parts):
    top = functools.reduce(jnp.maximum, parts)
    total = functools.reduce(jnp.add, [jnp.exp2(p - top) for p in parts])
    return top + jnp.log(total) * LOG2E


def dot_t(a, b):
    return lax.dot_general(a, b, (((1,), (1,)), ((), ())), preferred_element_type=jnp.float32)


def eye_mask(n):
    return lax.broadcasted_iota(jnp.int32, (n, n), 0) == lax.broadcasted_iota(jnp.int32, (n, n), 1)


def col_to_row(col):
    return jnp.sum(jnp.where(eye_mask(col.shape[0]), col, 0.0), axis=0, keepdims=True)


def row_to_col(row):
    return jnp.sum(jnp.where(eye_mask(row.shape[1]), row, 0.0), axis=1, keepdims=True)


def twice(b):
    return jnp.concatenate([b, b], axis=1)


def write_kernel(a, b, c, a_out, b_out, c_out, sems):
    copies = [pltpu.make_async_copy(v, o, sems.at[k]) for k, (v, o) in enumerate(((a, a_out), (b, b_out), (c, c_out)))]
    for cp in copies:
        cp.start()
    for cp in copies:
        cp.wait()


def em_kernel(
    comp_size, row_size, sweeps,
    temp_hbm, lp_hbm, x_hbm, mu_hbm,
    mu_out, lp_out, lse_out,
    temp_ref, lp_ref, xg, mu_all, mub, bcol, brow, e_buf, m_buf, l_buf, lq_buf, s_acc, n_acc, lp_fin, sq_buf,
    zl_src, zl_buf, pre_buf, bc_src, bc_buf, tot_buf,
    load_sem, near_sem, far_sem, g_send, y_recv, z_recv, sy_recv, sz_recv, own_recv,
    l_send, zl_recv, ag_recv, pre_send, pre_recv, bc_recv, post_recv, mx_recv, br_recv, fin_recv, lpf_recv,
):
    z = lax.axis_index("comp")
    r = lax.axis_index("row")
    y, c = r // CORES, r % CORES
    n_chips = comp_size * row_size // CORES
    y_size = row_size // CORES
    chip = z * y_size + y
    block = x_hbm.shape[0]
    half_dim = x_hbm.shape[1] // 2
    total_pts = block * row_size
    n_own = mub.shape[2]
    total_comp = mu_hbm.shape[1] * comp_size
    bt = block // TP
    ch = block // NCK
    rs = y * CORES + (1 - c)
    ry = (1 - y) * CORES + c
    sib = {"row": rs}
    yn = {"row": ry}
    rx = (1 - y) * CORES + (1 - c)
    yd = {"row": rx}
    zx = {"comp": z + 1 - 2 * (z % 2), "row": rs}
    hz = z % 2

    def remote(src, dst, send, recv, dev):
        return pltpu.make_async_remote_copy(
            src_ref=src, dst_ref=dst, send_sem=send, recv_sem=recv, device_id=dev, device_id_type=MESH)

    def same(v, send, recv, dev):
        return remote(v, v, send, recv, dev)

    x_loads = [pltpu.make_async_copy(
        x_hbm.at[:, pl.ds(s * half_dim, half_dim)], xg.at[s, pl.ds(r * block, block), :], load_sem.at[s])
        for s in range(2)]
    mu_loads = [pltpu.make_async_copy(mu_hbm.at[s], mu_all.at[s], load_sem.at[2 + s]) for s in range(2)]
    small_loads = [pltpu.make_async_copy(temp_hbm, temp_ref, load_sem.at[4]),
                   pltpu.make_async_copy(lp_hbm, lp_ref, load_sem.at[5])]
    for cp in x_loads + small_loads:
        cp.start()

    n_z = (z > 0).astype(jnp.int32) + (z < comp_size - 1).astype(jnp.int32)

    def signal_z(sem):
        @pl.when(z > 0)
        def _():
            pl.semaphore_signal(sem, inc=1, device_id={"comp": z - 1}, device_id_type=MESH)

        @pl.when(z < comp_size - 1)
        def _():
            pl.semaphore_signal(sem, inc=1, device_id={"comp": z + 1}, device_id_type=MESH)

    def signal_near(sem):
        for dev in (sib, yn, yd):
            pl.semaphore_signal(sem, inc=1, device_id=dev, device_id_type=MESH)
        signal_z(sem)

    barrier = pltpu.get_barrier_semaphore()
    signal_near(barrier)
    pl.semaphore_wait(barrier, 3 + n_z)
    signal_near(near_sem)
    for cp in mu_loads:
        cp.start()

    def xrows(s, blk, cid):
        return xg.at[s, pl.ds(pl.multiple_of(blk * block + cid * ch, ch), ch), :]

    def cid_y(k):
        return k + hz * (NCK - 1 - 2 * k)

    def cid_z(k):
        return k + (1 - hz) * (NCK - 1 - 2 * k)

    def y_out(j):
        return same(xrows(j // ND, r, cid_y(j % ND)), g_send.at[0], y_recv.at[j], yd)

    def z_fwd(m):
        return same(xrows(m // NR, rx, cid_y(m % NR)), g_send.at[0], z_recv.at[m], zx)

    def sy_fwd(j):
        return same(xrows(j // ND, rx, cid_y(j % ND)), g_send.at[0], sy_recv.at[j // ND], sib)

    def sz_fwd(m):
        return same(xrows(m // NR, ry, cid_z(m % NR)), g_send.at[0], sz_recv.at[m // NR], sib)

    def own_out(s):
        return same(xg.at[s, pl.ds(r * block, block), :], g_send.at[0], own_recv.at[s], sib)

    def y_steps(a, b):
        def body(j, _):
            y_out(j).wait_recv()

            @pl.when(j % ND < NR)
            def _():
                z_fwd(j // ND * NR + j % ND).start()

            sy_fwd(j).start()
            return 0

        lax.fori_loop(a, b, body, 0)

    def z_steps(a, b):
        def body(m, _):
            z_fwd(m).wait_recv()
            sz_fwd(m).start()
            return 0

        lax.fori_loop(a, b, body, 0)

    def rows_of(s, chunks):
        return xg.at[s, pl.ds(0, chunks * ch), :]

    def sib_waits(s):
        same(rows_of(s, ND), g_send.at[0], sy_recv.at[s], sib).wait_recv()
        same(rows_of(s, NR), g_send.at[0], sz_recv.at[s], sib).wait_recv()

    def gather_sends_wait(s):
        for chunks in (ND, NR, ND, NR):
            same(rows_of(s, chunks), g_send.at[0], sy_recv.at[s], sib).wait_send()
        own_out(s).wait_send()

    x_loads[0].wait()
    for j in range(ND):
        y_out(j).start()
    own_out(0).start()
    x_loads[1].wait()
    own_out(1).start()
    for cp in mu_loads + small_loads:
        cp.wait()

    def set_params(s, slot, mean, logw, t):
        mub[s, slot] = mean.astype(jnp.bfloat16)
        mu_sq = jnp.sum(mean * mean, axis=1, keepdims=True)
        col = (logw - temp_ref[t] * mu_sq) * LOG2E
        bcol[s, slot] = jnp.broadcast_to(col, (n_own, 128))
        return col

    def x_tile(s, tile):
        return xg[s, pl.ds(pl.multiple_of(tile * TP, TP), TP), :]

    def e_tile(s, slot, t, tile):
        a = dot_t(mub[s, slot], x_tile(s, tile))
        l2 = a * (temp_ref[t] * (2.0 * LOG2E)) + twice(bcol[s, slot])
        m = jnp.max(l2, axis=0, keepdims=True)
        e = jnp.exp2(l2 - m)
        return e, m, m + jnp.log(jnp.sum(e, axis=0, keepdims=True)) * LOG2E

    def tiles_of(half_id):
        return [(2 * half_id + k // bt, k % bt) for k in range(2 * bt)]

    def e_step(s, t, idx, hook=None, early=None):
        def body(i, _):
            h = (1 - c) + i * (2 * c - 1)
            for b, u in tiles_of(h):
                e, m, l = e_tile(s, r, t, b * bt + u)
                e_buf[s, b * bt + u] = e
                m_buf[s, b, u:u + 1, :] = m
                l_buf[s, b, u:u + 1, :] = l

            @pl.when(i == 0)
            def _():
                pre(idx).start()

            if hook is not None:
                hook(i)
            return 0

        lax.fori_loop(0, 2, body, 0)
        p2(idx)
        if early is not None:
            early()

    def acc_zero():
        s_acc[...] = jnp.zeros_like(s_acc)
        n_acc[...] = jnp.zeros_like(n_acc)

    def acc_tiles(s, tiles, resp_of):
        dots, ns = [], []
        for b, u in tiles:
            resp = resp_of(b, u)
            ns.append(resp[:, :128] + resp[:, 128:])
            dots.append(jnp.dot(resp.astype(jnp.bfloat16), x_tile(s, b * bt + u), preferred_element_type=jnp.float32))
        s_acc[...] += functools.reduce(jnp.add, dots)
        n_acc[...] += functools.reduce(jnp.add, ns)

    def m_step(s, t):
        idx = 2 * t + s
        acc_zero()

        def body(i, _):
            @pl.when(i == 1)
            def _():
                post(idx).wait_recv()

            def resp_of(b, u):
                f = jnp.exp2(m_buf[s, b, u:u + 1, :] - tot_buf[idx, b, u:u + 1, :])
                return e_buf[s, b * bt + u] * f

            acc_tiles(s, tiles_of((1 - c) + i * (2 * c - 1)), resp_of)
            return 0

        lax.fori_loop(0, 2, body, 0)

    def mr_half(s, slot, t, half_id):
        idx = 2 * t + s

        def resp_of(b, u):
            a = dot_t(mub[s, slot], x_tile(s, b * bt + u))
            return jnp.exp2(a * (temp_ref[t] * (2.0 * LOG2E)) + twice(bcol[s, slot]) - tot_buf[idx, b, u:u + 1, :])

        acc_tiles(s, tiles_of(half_id), resp_of)

    def mr_all(s, slot, t):
        for h in range(2):
            mr_half(s, slot, t, h)

    def acc_result():
        cnt = jnp.sum(n_acc[...], axis=1, keepdims=True)
        mean = s_acc[...] * (1.0 / (cnt + EPS_COUNT))
        logw = jnp.log((cnt + PRIOR_ALPHA) / (total_pts + total_comp * PRIOR_ALPHA))
        return mean, logw

    def half(ref, k):
        return ref.at[pl.ds(2 * k, 2)]

    def pre(idx):
        return remote(half(l_buf.at[idx % 2], 1 - c), pre_buf.at[idx], pre_send.at[idx - 2], pre_recv.at[idx - 2], sib)

    def bcast(idx, j):
        k = lax.rem(jnp.where(z < comp_size // 2, n_chips - j, j), n_chips)
        q = lax.rem(chip + k, n_chips)
        return remote(bc_src.at[idx], bc_buf.at[idx, k], l_send.at[0], bc_recv.at[idx - 2],
                      {"comp": q // y_size, "row": (q % y_size) * CORES + (1 - c)})

    def post(idx):
        return same(half(tot_buf.at[idx], 1 - c), l_send.at[0], post_recv.at[idx - 2], sib)

    def p2(idx):
        pre(idx).wait()
        bc_src[idx] = lse2_parts([l_buf[idx % 2, pl.ds(2 * c, 2)], pre_buf[idx]])
        for j in range(1, n_chips + 1):
            bcast(idx, j).start()

    def p3(idx):
        same(bc_buf.at[idx], l_send.at[0], bc_recv.at[idx - 2], sib).wait_recv()
        tot_buf[idx, pl.ds(2 * (1 - c), 2)] = lse2_parts([bc_buf[idx, k] for k in range(n_chips)])
        post(idx).start()

    def zl(s, k):
        return remote(zl_src.at[s], zl_buf.at[s, k - 1], l_send.at[0], zl_recv.at[s],
                      {"comp": lax.rem(z + k, comp_size)})

    def ag(s, k):
        return same(tot_buf.at[s, r], l_send.at[0], ag_recv.at[s], (sib, yn, yd)[k])

    def orig_fit(s, _):
        def orig_slots(p, _):
            for k in range(2):
                q = 2 * p + k
                off = pl.multiple_of(q * n_own, n_own)
                set_params(s, q, mu_all[s, pl.ds(off, n_own), :], row_to_col(lp_ref[pl.ds(s, 1), pl.ds(off, n_own)]), 0)
                for u in range(bt):
                    _, _, l = e_tile(s, q, 0, r * bt + u)
                    lq_buf[q, u:u + 1, :] = l

            @pl.when(jnp.logical_and(s == 0, p == 0))
            def _():
                pl.semaphore_wait(near_sem, 3 + n_z)
                signal_z(far_sem)

            @pl.when(s == 1)
            def _():
                y_steps(1 + 2 * p, 3 + 2 * p)

            return 0

        lax.fori_loop(0, row_size // 2, orig_slots, 0)
        zl_src[s] = lse2_parts([lq_buf[q] for q in range(row_size)])

        @pl.when(s == 0)
        def _():
            pl.semaphore_wait(far_sem, n_z)

        for k in range(1, comp_size):
            zl(s, k).start()

        @pl.when(s == 0)
        def _():
            y_steps(0, 1)

        return 0

    lax.fori_loop(0, 2, orig_fit, 0)

    def y_sends(a, b):
        def send(j, _):
            y_out(j).start()
            return 0

        lax.fori_loop(a, b, send, 0)

    def comb(s):
        same(zl_buf.at[s], l_send.at[0], zl_recv.at[s], sib).wait_recv()
        tot_buf[s, r] = lse2_parts([zl_src[s]] + [zl_buf[s, k] for k in range(comp_size - 1)])
        for k in range(3):
            ag(s, k).start()

    early = ND + 3
    y_sends(ND, early)
    y_steps(5, 6)
    comb(0)
    y_sends(early, 2 * ND)
    y_steps(6, 8)
    z_steps(0, 4)
    y_steps(8, 9)
    z_steps(4, 5)
    y_steps(9, 10)
    z_steps(5, 6)
    comb(1)
    y_steps(10, 11)
    z_steps(6, 7)
    y_steps(11, 12)

    def sweep0(s, _):
        same(tot_buf.at[s, pl.ds(0, 3)], l_send.at[0], ag_recv.at[s], sib).wait_recv()
        own_out(s).wait_recv()
        acc_zero()

        def body(k, _):
            @pl.when(jnp.logical_and(s == 0, k == 1))
            def _():
                y_steps(12, 14)
                sib_waits(0)

            @pl.when(jnp.logical_and(s == 1, k == 1))
            def _():
                z_steps(13, 14)
                sib_waits(1)

            mr_half(s, r, 0, y + k * (1 - 2 * y))

            @pl.when(jnp.logical_and(s == 0, k == 1))
            def _():
                y_steps(14, 16)
                z_steps(7, 10)

            return 0

        lax.fori_loop(0, 2, body, 0)
        mean, logw = acc_result()
        set_params(s, r, mean, logw, 1)

        def hook(i):
            @pl.when(jnp.logical_and(s == 0, i == 0))
            def _():
                y_steps(16, 17)

        def first_p3():
            @pl.when(s == 1)
            def _():
                p3(2)

        e_step(s, 1, 2 + s, hook, first_p3)

        @pl.when(s == 0)
        def _():
            y_steps(17, 18)
            z_steps(10, 13)

        return 0

    lax.fori_loop(0, 2, sweep0, 0)

    def mx(s):
        return same(mub.at[s, r], l_send.at[0], mx_recv.at[s], yn)

    def br(s):
        return same(brow.at[s, r], l_send.at[0], br_recv.at[s], yn)

    def mean_rows(slot, s):
        return mu_out.at[s, pl.ds(pl.multiple_of(slot * n_own, n_own), n_own), :]

    def fin(slot, s, k):
        return same(mean_rows(slot, s), l_send.at[0], fin_recv.at[s, k], sib)

    def lpf(slot, k):
        return same(lp_fin.at[slot], l_send.at[0], lpf_recv.at[k], sib)

    def sweep(i, _):
        t, s = i // 2, i % 2
        last = t == sweeps - 1
        m_step(s, t)
        mean, logw = acc_result()

        @pl.when(t < sweeps - 1)
        def _():
            set_params(s, r, mean, logw, t + 1)

            def early():
                @pl.when(t == sweeps - 2)
                def _():
                    mx(s).start()
                    brow[s, r] = col_to_row(bcol[s, r][:, :1])
                    br(s).start()

                p3(i + 1)

            e_step(s, t + 1, i + 2, early=early)

        @pl.when(last)
        def _():
            mean_rows(r, s)[...] = mean
            fin(r, s, 0).start()
            lp_fin[r, pl.ds(s, 1), :] = col_to_row(logw)
            mx(s).wait_recv()
            br(s).wait_recv()
            bcol[s, ry] = jnp.broadcast_to(row_to_col(brow[s, ry]), (n_own, 128))
            acc_zero()

            mr_all(s, ry, t)
            mean2, logw2 = acc_result()
            mean_rows(ry, s)[...] = mean2
            fin(ry, s, 1).start()
            lp_fin[ry, pl.ds(s, 1), :] = col_to_row(logw2)

            @pl.when(s == 0)
            def _():
                p3(i + 1)

        return 0

    lax.fori_loop(2, 2 * sweeps, sweep, 0)
    lpf(r, 0).start()
    lpf(ry, 1).start()

    ones = jnp.ones((8, half_dim), jnp.bfloat16)

    def sq_norms(s, _):
        for u in range(bt):
            x = x_tile(s, r * bt + u).astype(jnp.float32)
            sq = x * x
            hi = sq.astype(jnp.bfloat16)
            lo = (sq - hi.astype(jnp.float32)).astype(jnp.bfloat16)
            sq_buf[s, u:u + 1, :] = (dot_t(ones, hi) + dot_t(ones, lo))[0:1]
        return 0

    lax.fori_loop(0, 2, sq_norms, 0)
    for s in range(2):
        gather_sends_wait(s)
        same(zl_buf.at[s], l_send.at[0], zl_recv.at[s], sib).wait_send()
        same(tot_buf.at[s, pl.ds(0, 3)], l_send.at[0], ag_recv.at[s], sib).wait_send()
        mx(s).wait_send()
        br(s).wait_send()
        for t in range(1, sweeps):
            same(bc_buf.at[2 * t + s], l_send.at[0], zl_recv.at[s], sib).wait_send()
            post(2 * t + s).wait_send()


    t = sweeps - 1
    for s in range(2):
        for j in range(bt):
            lse_out[s:s + 1, j * TP:(j + 1) * TP] = (
                tot_buf[2 * t + s, r, j:j + 1, :] * LN2 - temp_ref[t] * sq_buf[s, j:j + 1, :])

    for k in range(2):
        for s in range(2):
            fin((r, ry)[k], s, k).wait_recv()
    lpf(r, 0).wait_recv()
    lpf(ry, 1).wait_recv()
    for k in range(2):
        for s in range(2):
            fin((r, ry)[k], s, k).wait_send()
        lpf((r, ry)[k], k).wait_send()
    for q in range(row_size):
        lp_out[:, q * n_own:(q + 1) * n_own] = lp_fin[q]


def solution(mesh):
    comp_size = mesh.shape["comp"]
    row_size = mesh.shape["row"]

    def local_fit(x_local, mu_init, logpi_init, inv_temp):
        block, dim = x_local.shape
        half_dim = dim // 2
        n_local = mu_init.shape[1]
        n_own = n_local // row_size
        total_pts = block * row_size
        tiles = total_pts // TP
        sweeps = inv_temp.shape[0]
        n_chips = comp_size * row_size // CORES
        ni = 2 * sweeps
        bt = block // TP
        f32, bf16 = jnp.float32, jnp.bfloat16
        dma = pltpu.SemaphoreType.DMA
        vm = pltpu.VMEM
        scratch = [
            pltpu.SMEM((sweeps,), f32), vm((2, n_local), f32),
            vm((2, total_pts, half_dim), bf16),
            vm((2, n_local, half_dim), f32),
            vm((2, row_size, n_own, half_dim), bf16),
            vm((2, row_size, n_own, 128), f32),
            vm((2, row_size, 1, n_own), f32),
            vm((2, tiles, n_own, TP), f32),
            vm((2, row_size, bt, TP), f32),
            vm((2, row_size, bt, TP), f32),
            vm((row_size, bt, TP), f32),
            vm((n_own, half_dim), f32),
            vm((n_own, 128), f32),
            vm((row_size, 2, n_own), f32),
            vm((2, bt, TP), f32),
            vm((2, bt, TP), f32),
            vm((2, comp_size - 1, bt, TP), f32),
            vm((ni, 2, bt, TP), f32),
            vm((ni, 2, bt, TP), f32),
            vm((ni, n_chips, 2, bt, TP), f32),
            vm((ni, row_size, bt, TP), f32),
            dma((6,)), pltpu.SemaphoreType.REGULAR, pltpu.SemaphoreType.REGULAR,
            dma((1,)), dma((2 * ND,)), dma((2 * NR,)), dma((2,)), dma((2,)), dma((2,)),
            dma((1,)), dma((2,)), dma((2,)), dma((ni - 2,)), dma((ni - 2,)), dma((ni - 2,)), dma((ni - 2,)),
            dma((2,)), dma((2,)), dma((2, 2)), dma((2,)),
        ]
        outs = pl.pallas_call(
            functools.partial(em_kernel, comp_size, row_size, sweeps),
            out_shape=(vm((2, n_local, half_dim), f32), vm((2, n_local), f32), vm((2, block), f32)),
            in_specs=[
                pl.BlockSpec(memory_space=pl.ANY),
            ] * 4,
            out_specs=(pl.BlockSpec(memory_space=pltpu.VMEM),) * 3,
            scratch_shapes=scratch,
            compiler_params=pltpu.CompilerParams(
                collective_id=0, has_side_effects=True, vmem_limit_bytes=56 * 1024 * 1024),
        )(inv_temp, logpi_init, x_local, mu_init)
        return pl.pallas_call(
            write_kernel,
            out_shape=tuple(jax.ShapeDtypeStruct(o.shape, o.dtype) for o in outs),
            in_specs=[pl.BlockSpec(memory_space=pltpu.VMEM)] * 3,
            out_specs=(pl.BlockSpec(memory_space=pl.ANY),) * 3,
            scratch_shapes=[dma((3,))],
        )(*[pltpu.with_memory_space_constraint(o, pltpu.VMEM) for o in outs])

    return jax.shard_map(
        local_fit,
        mesh=mesh,
        in_specs=(P(("grp", "row"), None), P(None, ("grp", "comp"), None), P(None, ("grp", "comp")), P()),
        out_specs=(P(None, ("grp", "comp"), None), P(None, ("grp", "comp")), P(None, ("grp", "row"))),
        check_vma=False,
    )
```

```python
import functools

import jax
import jax.numpy as jnp
from jax import lax
from jax.experimental import pallas as pl
from jax.experimental.pallas import tpu as pltpu
from jax.sharding import PartitionSpec as P

EPS_COUNT = 1e-6
PRIOR_ALPHA = 1e-3
LOG2E = 1.4426950408889634
LN2 = 0.6931471805599453
MESH = pl.DeviceIdType.MESH

CORES = 2
TP = 256
NCK = 16
ND = 9
NR = NCK - ND


def lse2_parts(parts):
    top = functools.reduce(jnp.maximum, parts)
    total = functools.reduce(jnp.add, [jnp.exp2(p - top) for p in parts])
    return top + jnp.log(total) * LOG2E


def dot_t(a, b):
    return lax.dot_general(a, b, (((1,), (1,)), ((), ())), preferred_element_type=jnp.float32)


def eye_mask(n):
    return lax.broadcasted_iota(jnp.int32, (n, n), 0) == lax.broadcasted_iota(jnp.int32, (n, n), 1)


def col_to_row(col):
    return jnp.sum(jnp.where(eye_mask(col.shape[0]), col, 0.0), axis=0, keepdims=True)


def row_to_col(row):
    return jnp.sum(jnp.where(eye_mask(row.shape[1]), row, 0.0), axis=1, keepdims=True)


def twice(b):
    return jnp.concatenate([b, b], axis=1)


def write_kernel(a, b, c, a_out, b_out, c_out, sems):
    copies = [pltpu.make_async_copy(v, o, sems.at[k]) for k, (v, o) in enumerate(((a, a_out), (b, b_out), (c, c_out)))]
    for cp in copies:
        cp.start()
    for cp in copies:
        cp.wait()


def em_kernel(
    comp_size, row_size, sweeps,
    temp_hbm, lp_hbm, x_hbm, mu_hbm,
    mu_out, lp_out, lse_out,
    temp_ref, lp_ref, xg, mu_all, mub, bcol, brow, e_buf, m_buf, l_buf, lq_buf, s_acc, n_acc, lp_fin, sq_buf,
    zl_src, zl_buf, pre_buf, bc_src, bc_buf, tot_buf,
    load_sem, near_sem, far_sem, g_send, y_recv, z_recv, sy_recv, sz_recv, own_recv,
    l_send, zl_recv, ag_recv, pre_send, pre_recv, bc_recv, post_recv, mx_recv, br_recv, fin_recv, lpf_recv,
):
    z = lax.axis_index("comp")
    r = lax.axis_index("row")
    y, c = r // CORES, r % CORES
    n_chips = comp_size * row_size // CORES
    y_size = row_size // CORES
    chip = z * y_size + y
    block = x_hbm.shape[0]
    half_dim = x_hbm.shape[1] // 2
    total_pts = block * row_size
    n_own = mub.shape[2]
    total_comp = mu_hbm.shape[1] * comp_size
    bt = block // TP
    ch = block // NCK
    rs = y * CORES + (1 - c)
    ry = (1 - y) * CORES + c
    sib = {"row": rs}
    yn = {"row": ry}
    rx = (1 - y) * CORES + (1 - c)
    yd = {"row": rx}
    zx = {"comp": z + 1 - 2 * (z % 2), "row": rs}
    hz = z % 2

    def remote(src, dst, send, recv, dev):
        return pltpu.make_async_remote_copy(
            src_ref=src, dst_ref=dst, send_sem=send, recv_sem=recv, device_id=dev, device_id_type=MESH)

    def same(v, send, recv, dev):
        return remote(v, v, send, recv, dev)

    x_loads = [pltpu.make_async_copy(
        x_hbm.at[:, pl.ds(s * half_dim, half_dim)], xg.at[s, pl.ds(r * block, block), :], load_sem.at[s])
        for s in range(2)]
    mu_loads = [pltpu.make_async_copy(mu_hbm.at[s], mu_all.at[s], load_sem.at[2 + s]) for s in range(2)]
    small_loads = [pltpu.make_async_copy(temp_hbm, temp_ref, load_sem.at[4]),
                   pltpu.make_async_copy(lp_hbm, lp_ref, load_sem.at[5])]
    for cp in x_loads + small_loads:
        cp.start()

    n_z = (z > 0).astype(jnp.int32) + (z < comp_size - 1).astype(jnp.int32)

    def signal_z(sem):
        @pl.when(z > 0)
        def _():
            pl.semaphore_signal(sem, inc=1, device_id={"comp": z - 1}, device_id_type=MESH)

        @pl.when(z < comp_size - 1)
        def _():
            pl.semaphore_signal(sem, inc=1, device_id={"comp": z + 1}, device_id_type=MESH)

    def signal_near(sem):
        for dev in (sib, yn, yd):
            pl.semaphore_signal(sem, inc=1, device_id=dev, device_id_type=MESH)
        signal_z(sem)

    barrier = pltpu.get_barrier_semaphore()
    signal_near(barrier)
    pl.semaphore_wait(barrier, 3 + n_z)
    signal_near(near_sem)
    for cp in mu_loads:
        cp.start()

    def xrows(s, blk, cid):
        return xg.at[s, pl.ds(pl.multiple_of(blk * block + cid * ch, ch), ch), :]

    def cid_y(k):
        return k + hz * (NCK - 1 - 2 * k)

    def cid_z(k):
        return k + (1 - hz) * (NCK - 1 - 2 * k)

    def y_out(j):
        return same(xrows(j // ND, r, cid_y(j % ND)), g_send.at[0], y_recv.at[j], yd)

    def z_fwd(m):
        return same(xrows(m // NR, rx, cid_y(m % NR)), g_send.at[0], z_recv.at[m], zx)

    def sy_fwd(j):
        return same(xrows(j // ND, rx, cid_y(j % ND)), g_send.at[0], sy_recv.at[j // ND], sib)

    def sz_fwd(m):
        return same(xrows(m // NR, ry, cid_z(m % NR)), g_send.at[0], sz_recv.at[m // NR], sib)

    def own_out(s):
        return same(xg.at[s, pl.ds(r * block, block), :], g_send.at[0], own_recv.at[s], sib)

    def y_steps(a, b):
        def body(j, _):
            y_out(j).wait_recv()

            @pl.when(j % ND < NR)
            def _():
                z_fwd(j // ND * NR + j % ND).start()

            sy_fwd(j).start()
            return 0

        lax.fori_loop(a, b, body, 0)

    def z_steps(a, b):
        def body(m, _):
            z_fwd(m).wait_recv()
            sz_fwd(m).start()
            return 0

        lax.fori_loop(a, b, body, 0)

    def rows_of(s, chunks):
        return xg.at[s, pl.ds(0, chunks * ch), :]

    def sib_waits(s):
        same(rows_of(s, ND), g_send.at[0], sy_recv.at[s], sib).wait_recv()
        same(rows_of(s, NR), g_send.at[0], sz_recv.at[s], sib).wait_recv()

    def gather_sends_wait(s):
        for chunks in (ND, NR, ND, NR):
            same(rows_of(s, chunks), g_send.at[0], sy_recv.at[s], sib).wait_send()
        own_out(s).wait_send()

    x_loads[0].wait()
    for j in range(ND):
        y_out(j).start()
    own_out(0).start()
    x_loads[1].wait()
    own_out(1).start()
    for cp in mu_loads + small_loads:
        cp.wait()

    def set_params(s, slot, mean, logw, t):
        mub[s, slot] = mean.astype(jnp.bfloat16)
        mu_sq = jnp.sum(mean * mean, axis=1, keepdims=True)
        col = (logw - temp_ref[t] * mu_sq) * LOG2E
        bcol[s, slot] = jnp.broadcast_to(col, (n_own, 128))
        return col

    def x_tile(s, tile):
        return xg[s, pl.ds(pl.multiple_of(tile * TP, TP), TP), :]

    def e_tile(s, slot, t, tile):
        a = dot_t(mub[s, slot], x_tile(s, tile))
        l2 = a * (temp_ref[t] * (2.0 * LOG2E)) + twice(bcol[s, slot])
        m = jnp.max(l2, axis=0, keepdims=True)
        e = jnp.exp2(l2 - m)
        return e, m, m + jnp.log(jnp.sum(e, axis=0, keepdims=True)) * LOG2E

    def tiles_of(half_id):
        return [(2 * half_id + k // bt, k % bt) for k in range(2 * bt)]

    def e_step(s, t, idx, hook=None, early=None):
        def body(i, _):
            h = (1 - c) + i * (2 * c - 1)
            for b, u in tiles_of(h):
                e, m, l = e_tile(s, r, t, b * bt + u)
                e_buf[s, b * bt + u] = e
                m_buf[s, b, u:u + 1, :] = m
                l_buf[s, b, u:u + 1, :] = l

            @pl.when(i == 0)
            def _():
                pre(idx).start()

            if hook is not None:
                hook(i)
            return 0

        lax.fori_loop(0, 2, body, 0)
        p2(idx)
        if early is not None:
            early()

    def acc_zero():
        s_acc[...] = jnp.zeros_like(s_acc)
        n_acc[...] = jnp.zeros_like(n_acc)

    def acc_tiles(s, tiles, resp_of):
        dots, ns = [], []
        for b, u in tiles:
            resp = resp_of(b, u)
            ns.append(resp[:, :128] + resp[:, 128:])
            dots.append(jnp.dot(resp.astype(jnp.bfloat16), x_tile(s, b * bt + u), preferred_element_type=jnp.float32))
        s_acc[...] += functools.reduce(jnp.add, dots)
        n_acc[...] += functools.reduce(jnp.add, ns)

    def m_step(s, t):
        idx = 2 * t + s
        acc_zero()

        def body(i, _):
            @pl.when(i == 1)
            def _():
                post(idx).wait_recv()

            def resp_of(b, u):
                f = jnp.exp2(m_buf[s, b, u:u + 1, :] - tot_buf[idx, b, u:u + 1, :])
                return e_buf[s, b * bt + u] * f

            acc_tiles(s, tiles_of((1 - c) + i * (2 * c - 1)), resp_of)
            return 0

        lax.fori_loop(0, 2, body, 0)

    def mr_half(s, slot, t, half_id):
        idx = 2 * t + s

        def resp_of(b, u):
            a = dot_t(mub[s, slot], x_tile(s, b * bt + u))
            return jnp.exp2(a * (temp_ref[t] * (2.0 * LOG2E)) + twice(bcol[s, slot]) - tot_buf[idx, b, u:u + 1, :])

        acc_tiles(s, tiles_of(half_id), resp_of)

    def mr_all(s, slot, t):
        for h in range(2):
            mr_half(s, slot, t, h)

    def acc_result():
        cnt = jnp.sum(n_acc[...], axis=1, keepdims=True)
        mean = s_acc[...] * (1.0 / (cnt + EPS_COUNT))
        logw = jnp.log((cnt + PRIOR_ALPHA) / (total_pts + total_comp * PRIOR_ALPHA))
        return mean, logw

    def half(ref, k):
        return ref.at[pl.ds(2 * k, 2)]

    def pre(idx):
        return remote(half(l_buf.at[idx % 2], 1 - c), pre_buf.at[idx], pre_send.at[idx - 2], pre_recv.at[idx - 2], sib)

    def bcast(idx, j):
        k = lax.rem(jnp.where(z < comp_size // 2, n_chips - j, j), n_chips)
        q = lax.rem(chip + k, n_chips)
        return remote(bc_src.at[idx], bc_buf.at[idx, k], l_send.at[0], bc_recv.at[idx - 2],
                      {"comp": q // y_size, "row": (q % y_size) * CORES + (1 - c)})

    def post(idx):
        return same(half(tot_buf.at[idx], 1 - c), l_send.at[0], post_recv.at[idx - 2], sib)

    def p2(idx):
        pre(idx).wait()
        bc_src[idx] = lse2_parts([l_buf[idx % 2, pl.ds(2 * c, 2)], pre_buf[idx]])
        for j in range(1, n_chips + 1):
            bcast(idx, j).start()

    def p3(idx):
        same(bc_buf.at[idx], l_send.at[0], bc_recv.at[idx - 2], sib).wait_recv()
        tot_buf[idx, pl.ds(2 * (1 - c), 2)] = lse2_parts([bc_buf[idx, k] for k in range(n_chips)])
        post(idx).start()

    def zl(s, k):
        return remote(zl_src.at[s], zl_buf.at[s, k - 1], l_send.at[0], zl_recv.at[s],
                      {"comp": lax.rem(z + k, comp_size)})

    def ag(s, k):
        return same(tot_buf.at[s, r], l_send.at[0], ag_recv.at[s], (sib, yn, yd)[k])

    def orig_fit(s, _):
        def orig_slots(p, _):
            for k in range(2):
                q = 2 * p + k
                off = pl.multiple_of(q * n_own, n_own)
                set_params(s, q, mu_all[s, pl.ds(off, n_own), :], row_to_col(lp_ref[pl.ds(s, 1), pl.ds(off, n_own)]), 0)
                for u in range(bt):
                    _, _, l = e_tile(s, q, 0, r * bt + u)
                    lq_buf[q, u:u + 1, :] = l

            @pl.when(jnp.logical_and(s == 0, p == 0))
            def _():
                pl.semaphore_wait(near_sem, 3 + n_z)
                signal_z(far_sem)

            @pl.when(s == 1)
            def _():
                y_steps(1 + 2 * p, 3 + 2 * p)

            return 0

        lax.fori_loop(0, row_size // 2, orig_slots, 0)
        zl_src[s] = lse2_parts([lq_buf[q] for q in range(row_size)])

        @pl.when(s == 0)
        def _():
            pl.semaphore_wait(far_sem, n_z)

        for k in range(1, comp_size):
            zl(s, k).start()

        @pl.when(s == 0)
        def _():
            y_steps(0, 1)

        return 0

    lax.fori_loop(0, 2, orig_fit, 0)

    def y_sends(a, b):
        def send(j, _):
            y_out(j).start()
            return 0

        lax.fori_loop(a, b, send, 0)

    def comb(s):
        same(zl_buf.at[s], l_send.at[0], zl_recv.at[s], sib).wait_recv()
        tot_buf[s, r] = lse2_parts([zl_src[s]] + [zl_buf[s, k] for k in range(comp_size - 1)])
        for k in range(3):
            ag(s, k).start()

    early = ND + 4
    y_sends(ND, early)
    y_steps(5, 6)
    comb(0)
    y_sends(early, 2 * ND)
    y_steps(6, 8)
    z_steps(0, 4)
    y_steps(8, 9)
    z_steps(4, 5)
    y_steps(9, 10)
    z_steps(5, 6)
    comb(1)
    y_steps(10, 11)
    z_steps(6, 7)
    y_steps(11, 12)

    def sweep0(s, _):
        same(tot_buf.at[s, pl.ds(0, 3)], l_send.at[0], ag_recv.at[s], sib).wait_recv()
        own_out(s).wait_recv()
        acc_zero()

        def body(k, _):
            @pl.when(jnp.logical_and(s == 0, k == 1))
            def _():
                y_steps(12, 14)
                sib_waits(0)

            @pl.when(jnp.logical_and(s == 1, k == 1))
            def _():
                z_steps(13, 14)
                sib_waits(1)

            mr_half(s, r, 0, y + k * (1 - 2 * y))

            @pl.when(jnp.logical_and(s == 0, k == 1))
            def _():
                y_steps(14, 16)
                z_steps(7, 10)

            return 0

        lax.fori_loop(0, 2, body, 0)
        mean, logw = acc_result()
        set_params(s, r, mean, logw, 1)

        def hook(i):
            @pl.when(jnp.logical_and(s == 0, i == 0))
            def _():
                y_steps(16, 17)

        def first_p3():
            @pl.when(s == 1)
            def _():
                p3(2)

        e_step(s, 1, 2 + s, hook, first_p3)

        @pl.when(s == 0)
        def _():
            y_steps(17, 18)
            z_steps(10, 13)

        return 0

    lax.fori_loop(0, 2, sweep0, 0)

    def mx(s):
        return same(mub.at[s, r], l_send.at[0], mx_recv.at[s], yn)

    def br(s):
        return same(brow.at[s, r], l_send.at[0], br_recv.at[s], yn)

    def mean_rows(slot, s):
        return mu_out.at[s, pl.ds(pl.multiple_of(slot * n_own, n_own), n_own), :]

    def fin(slot, s, k):
        return same(mean_rows(slot, s), l_send.at[0], fin_recv.at[s, k], sib)

    def lpf(slot, k):
        return same(lp_fin.at[slot], l_send.at[0], lpf_recv.at[k], sib)

    def sweep(i, _):
        t, s = i // 2, i % 2
        last = t == sweeps - 1
        m_step(s, t)
        mean, logw = acc_result()

        @pl.when(t < sweeps - 1)
        def _():
            set_params(s, r, mean, logw, t + 1)

            def early():
                @pl.when(t == sweeps - 2)
                def _():
                    mx(s).start()
                    brow[s, r] = col_to_row(bcol[s, r][:, :1])
                    br(s).start()

                p3(i + 1)

            e_step(s, t + 1, i + 2, early=early)

        @pl.when(last)
        def _():
            mean_rows(r, s)[...] = mean
            fin(r, s, 0).start()
            lp_fin[r, pl.ds(s, 1), :] = col_to_row(logw)
            mx(s).wait_recv()
            br(s).wait_recv()
            bcol[s, ry] = jnp.broadcast_to(row_to_col(brow[s, ry]), (n_own, 128))
            acc_zero()

            mr_all(s, ry, t)
            mean2, logw2 = acc_result()
            mean_rows(ry, s)[...] = mean2
            fin(ry, s, 1).start()
            lp_fin[ry, pl.ds(s, 1), :] = col_to_row(logw2)

            @pl.when(s == 0)
            def _():
                p3(i + 1)

        return 0

    lax.fori_loop(2, 2 * sweeps, sweep, 0)
    lpf(r, 0).start()
    lpf(ry, 1).start()

    ones = jnp.ones((8, half_dim), jnp.bfloat16)

    def sq_norms(s, _):
        for u in range(bt):
            x = x_tile(s, r * bt + u).astype(jnp.float32)
            sq = x * x
            hi = sq.astype(jnp.bfloat16)
            lo = (sq - hi.astype(jnp.float32)).astype(jnp.bfloat16)
            sq_buf[s, u:u + 1, :] = (dot_t(ones, hi) + dot_t(ones, lo))[0:1]
        return 0

    lax.fori_loop(0, 2, sq_norms, 0)
    for s in range(2):
        gather_sends_wait(s)
        same(zl_buf.at[s], l_send.at[0], zl_recv.at[s], sib).wait_send()
        same(tot_buf.at[s, pl.ds(0, 3)], l_send.at[0], ag_recv.at[s], sib).wait_send()
        mx(s).wait_send()
        br(s).wait_send()
        for t in range(1, sweeps):
            same(bc_buf.at[2 * t + s], l_send.at[0], zl_recv.at[s], sib).wait_send()
            post(2 * t + s).wait_send()


    t = sweeps - 1
    for s in range(2):
        for j in range(bt):
            lse_out[s:s + 1, j * TP:(j + 1) * TP] = (
                tot_buf[2 * t + s, r, j:j + 1, :] * LN2 - temp_ref[t] * sq_buf[s, j:j + 1, :])

    for k in range(2):
        for s in range(2):
            fin((r, ry)[k], s, k).wait_recv()
    lpf(r, 0).wait_recv()
    lpf(ry, 1).wait_recv()
    for k in range(2):
        for s in range(2):
            fin((r, ry)[k], s, k).wait_send()
        lpf((r, ry)[k], k).wait_send()
    for q in range(row_size):
        lp_out[:, q * n_own:(q + 1) * n_own] = lp_fin[q]


def solution(mesh):
    comp_size = mesh.shape["comp"]
    row_size = mesh.shape["row"]

    def local_fit(x_local, mu_init, logpi_init, inv_temp):
        block, dim = x_local.shape
        half_dim = dim // 2
        n_local = mu_init.shape[1]
        n_own = n_local // row_size
        total_pts = block * row_size
        tiles = total_pts // TP
        sweeps = inv_temp.shape[0]
        n_chips = comp_size * row_size // CORES
        ni = 2 * sweeps
        bt = block // TP
        f32, bf16 = jnp.float32, jnp.bfloat16
        dma = pltpu.SemaphoreType.DMA
        vm = pltpu.VMEM
        scratch = [
            pltpu.SMEM((sweeps,), f32), vm((2, n_local), f32),
            vm((2, total_pts, half_dim), bf16),
            vm((2, n_local, half_dim), f32),
            vm((2, row_size, n_own, half_dim), bf16),
            vm((2, row_size, n_own, 128), f32),
            vm((2, row_size, 1, n_own), f32),
            vm((2, tiles, n_own, TP), f32),
            vm((2, row_size, bt, TP), f32),
            vm((2, row_size, bt, TP), f32),
            vm((row_size, bt, TP), f32),
            vm((n_own, half_dim), f32),
            vm((n_own, 128), f32),
            vm((row_size, 2, n_own), f32),
            vm((2, bt, TP), f32),
            vm((2, bt, TP), f32),
            vm((2, comp_size - 1, bt, TP), f32),
            vm((ni, 2, bt, TP), f32),
            vm((ni, 2, bt, TP), f32),
            vm((ni, n_chips, 2, bt, TP), f32),
            vm((ni, row_size, bt, TP), f32),
            dma((6,)), pltpu.SemaphoreType.REGULAR, pltpu.SemaphoreType.REGULAR,
            dma((1,)), dma((2 * ND,)), dma((2 * NR,)), dma((2,)), dma((2,)), dma((2,)),
            dma((1,)), dma((2,)), dma((2,)), dma((ni - 2,)), dma((ni - 2,)), dma((ni - 2,)), dma((ni - 2,)),
            dma((2,)), dma((2,)), dma((2, 2)), dma((2,)),
        ]
        outs = pl.pallas_call(
            functools.partial(em_kernel, comp_size, row_size, sweeps),
            out_shape=(vm((2, n_local, half_dim), f32), vm((2, n_local), f32), vm((2, block), f32)),
            in_specs=[
                pl.BlockSpec(memory_space=pl.ANY),
            ] * 4,
            out_specs=(pl.BlockSpec(memory_space=pltpu.VMEM),) * 3,
            scratch_shapes=scratch,
            compiler_params=pltpu.CompilerParams(
                collective_id=0, has_side_effects=True, vmem_limit_bytes=56 * 1024 * 1024),
        )(inv_temp, logpi_init, x_local, mu_init)
        return pl.pallas_call(
            write_kernel,
            out_shape=tuple(jax.ShapeDtypeStruct(o.shape, o.dtype) for o in outs),
            in_specs=[pl.BlockSpec(memory_space=pltpu.VMEM)] * 3,
            out_specs=(pl.BlockSpec(memory_space=pl.ANY),) * 3,
            scratch_shapes=[dma((3,))],
        )(*[pltpu.with_memory_space_constraint(o, pltpu.VMEM) for o in outs])

    return jax.shard_map(
        local_fit,
        mesh=mesh,
        in_specs=(P(("grp", "row"), None), P(None, ("grp", "comp"), None), P(None, ("grp", "comp")), P()),
        out_specs=(P(None, ("grp", "comp"), None), P(None, ("grp", "comp")), P(None, ("grp", "row"))),
        check_vma=False,
    )
```
